16 devices in a mesh: tp: 2 (over z), dp: 8 (over y, x, core).
Axes of the slice: x: 2, y: 2, z: 2, core: 2. Of those that a mesh axis runs over, the one named last changes fastest.
Arguments:
- hidden: bfloat16 [32, 512, 3072], P('dp', 'tp')
- norm_gain: bfloat16 [3072], P('dp')
- w_query: bfloat16 [3072, 3072], P('dp', 'tp')
- w_key: bfloat16 [3072, 1024], P('dp', 'tp')
- w_value: bfloat16 [3072, 1024], P('dp', 'tp')
- w_out: bfloat16 [3072, 3072], P('tp', 'dp')
- grad_out: bfloat16 [32, 512, 3072], P('dp', 'tp')
Outputs:
- output 1: bfloat16 [32, 512, 3072], P('dp', 'tp')
- output 2: bfloat16 [32, 512, 3072], P('dp', 'tp')
- output 3: float32 [3072], P('dp')
- output 4: float32 [3072, 3072], P('dp', 'tp')
- output 5: float32 [3072, 1024], P('dp', 'tp')
- output 6: float32 [3072, 1024], P('dp', 'tp')
- output 7: float32 [3072, 3072], P('tp', 'dp')
All inputs are finite; a program needn't handle non-finite values.
Results may differ from the reference program's by a relative error of at most 0.02.
Values are sent between devices in bfloat16 or wider.
A program may use at most 1 GiB of HBM per device.

```python
import jax
import jax.numpy as jnp
from jax import lax

BATCH_SIZE = 32
SEQ_LEN = 512
MODEL_DIM = 3072
NUM_HEADS = 24
NUM_KV = 8
HEAD_DIM = 128
NORM_EPS = 1e-5
ROPE_BASE = 500000.0
GROUP_SIZE = NUM_HEADS // NUM_KV
SCORE_SCALE = HEAD_DIM ** -0.5


def setup_inputs(seed: int = 0) -> dict:
    key_list = jax.random.split(jax.random.key(seed), 7)
    q_width = NUM_HEADS * HEAD_DIM
    kv_width = NUM_KV * HEAD_DIM
    act_shape = (BATCH_SIZE, SEQ_LEN, MODEL_DIM)
    in_scale = MODEL_DIM ** -0.5
    hidden = jax.random.normal(key_list[0], act_shape, jnp.float32)
    norm_gain = 1.0 + 0.3 * jax.random.normal(key_list[1], (MODEL_DIM,), jnp.float32)
    w_query = (1.25 * in_scale) * jax.random.normal(key_list[2], (MODEL_DIM, q_width), jnp.float32)
    w_key = (1.25 * in_scale) * jax.random.normal(key_list[3], (MODEL_DIM, kv_width), jnp.float32)
    w_value = in_scale * jax.random.normal(key_list[4], (MODEL_DIM, kv_width), jnp.float32)
    w_out = (2.0 * q_width ** -0.5) * jax.random.normal(key_list[5], (q_width, MODEL_DIM), jnp.float32)
    grad_out = jax.random.normal(key_list[6], act_shape, jnp.float32)
    return {
        "hidden": hidden.astype(jnp.bfloat16),
        "norm_gain": norm_gain.astype(jnp.bfloat16),
        "w_query": w_query.astype(jnp.bfloat16),
        "w_key": w_key.astype(jnp.bfloat16),
        "w_value": w_value.astype(jnp.bfloat16),
        "w_out": w_out.astype(jnp.bfloat16),
        "grad_out": grad_out.astype(jnp.bfloat16),
    }


def rope_tables():
    half_dim = HEAD_DIM // 2
    inv_freq = ROPE_BASE ** (-jnp.arange(half_dim, dtype=jnp.float32) * 2.0 / HEAD_DIM)
    angles = jnp.arange(SEQ_LEN, dtype=jnp.float32)[:, None] * inv_freq[None, :]
    return jnp.cos(angles), jnp.sin(angles)


def rotate(values, cos_t, sin_t):
    half_dim = values.shape[-1] // 2
    lower_half = values[..., :half_dim]
    upper_half = values[..., half_dim:]
    return jnp.concatenate([lower_half * cos_t - upper_half * sin_t, upper_half * cos_t + lower_half * sin_t], axis=-1)


def to_bf16(values):
    return values.astype(jnp.bfloat16).astype(jnp.float32)


def group_attention(items):
    q_blk, k_blk, v_blk = items
    scores = jnp.einsum("qrd,kd->rqk", q_blk, k_blk) * SCORE_SCALE
    causal = jnp.arange(SEQ_LEN)[:, None] >= jnp.arange(SEQ_LEN)[None, :]
    scores = jnp.where(causal[None], scores, -1e30)
    attn_prob = to_bf16(jax.nn.softmax(scores, axis=-1))
    return to_bf16(jnp.einsum("rqk,kd->qrd", attn_prob, v_blk))


def block_forward(hidden, norm_gain, w_query, w_key, w_value, w_out):
    cos_t, sin_t = rope_tables()
    inv_rms = lax.rsqrt(jnp.mean(hidden * hidden, axis=-1, keepdims=True) + NORM_EPS)
    normed = to_bf16(hidden * inv_rms * norm_gain).reshape(-1, MODEL_DIM)
    q_lin = to_bf16(jnp.dot(normed, w_query, preferred_element_type=jnp.float32))
    k_lin = to_bf16(jnp.dot(normed, w_key, preferred_element_type=jnp.float32))
    v_lin = to_bf16(jnp.dot(normed, w_value, preferred_element_type=jnp.float32))
    q_heads = to_bf16(rotate(q_lin.reshape(BATCH_SIZE, SEQ_LEN, NUM_KV, GROUP_SIZE, HEAD_DIM), cos_t[:, None, None, :], sin_t[:, None, None, :]))
    k_heads = to_bf16(rotate(k_lin.reshape(BATCH_SIZE, SEQ_LEN, NUM_KV, HEAD_DIM), cos_t[:, None, :], sin_t[:, None, :]))
    v_heads = v_lin.reshape(BATCH_SIZE, SEQ_LEN, NUM_KV, HEAD_DIM)
    q_items = jnp.moveaxis(q_heads, 2, 1).reshape(BATCH_SIZE * NUM_KV, SEQ_LEN, GROUP_SIZE, HEAD_DIM)
    k_items = jnp.moveaxis(k_heads, 2, 1).reshape(BATCH_SIZE * NUM_KV, SEQ_LEN, HEAD_DIM)
    v_items = jnp.moveaxis(v_heads, 2, 1).reshape(BATCH_SIZE * NUM_KV, SEQ_LEN, HEAD_DIM)
    attn_items = lax.map(jax.checkpoint(group_attention), (q_items, k_items, v_items))
    attn_out = jnp.moveaxis(attn_items.reshape(BATCH_SIZE, NUM_KV, SEQ_LEN, GROUP_SIZE, HEAD_DIM), 1, 2).reshape(BATCH_SIZE * SEQ_LEN, NUM_HEADS * HEAD_DIM)
    block_out = to_bf16(jnp.dot(attn_out, w_out, preferred_element_type=jnp.float32))
    return hidden + block_out.reshape(BATCH_SIZE, SEQ_LEN, MODEL_DIM)


def reference(hidden, norm_gain, w_query, w_key, w_value, w_out, grad_out):
    out_f32, pullback = jax.vjp(
        block_forward,
        hidden.astype(jnp.float32),
        norm_gain.astype(jnp.float32),
        w_query.astype(jnp.float32),
        w_key.astype(jnp.float32),
        w_value.astype(jnp.float32),
        w_out.astype(jnp.float32),
    )
    grad_list = pullback(grad_out.astype(jnp.float32))
    return (
        out_f32.astype(jnp.bfloat16),
        grad_list[0].astype(jnp.bfloat16),
        grad_list[1],
        grad_list[2],
        grad_list[3],
        grad_list[4],
        grad_list[5],
    )
```

```python
import functools

import jax
import jax.numpy as jnp
from jax import lax
from jax.experimental import pallas as pl
from jax.experimental.pallas import tpu as pltpu
from jax.sharding import PartitionSpec as P


HEAD_DIM = 128
NORM_EPS = 1e-5
ROPE_BASE = 500000.0
SCORE_SCALE = HEAD_DIM ** -0.5
MASK_VALUE = -1e30
F32 = jnp.float32
BF16 = jnp.bfloat16
NT = (((1,), (1,)), ((), ()))
NN = (((1,), (0,)), ((), ()))
TN = (((0,), (0,)), ((), ()))


def rope_tables(seq_len):
    half_dim = HEAD_DIM // 2
    inv_freq = ROPE_BASE ** (-jnp.arange(half_dim, dtype=F32) * 2.0 / HEAD_DIM)
    angles = jnp.arange(seq_len, dtype=F32)[:, None] * inv_freq[None, :]
    cos_t, sin_t = jnp.cos(angles), jnp.sin(angles)
    return jnp.concatenate([cos_t, cos_t], axis=1), jnp.concatenate([-sin_t, sin_t], axis=1)


def dot(lhs, rhs, dims):
    return lax.dot_general(lhs, rhs, dims, preferred_element_type=F32)


def turn(values, cos_t, sin_t):
    return values * cos_t + pltpu.roll(values, HEAD_DIM // 2, 1) * sin_t


def pick_halves(first, own, rec):
    own, rec = own.astype(F32), rec.astype(F32)
    return jnp.where(first, own, rec), jnp.where(first, rec, own)


def heads_of(group_size, block, cos_t, sin_t):
    cut = [block[:, i * HEAD_DIM:(i + 1) * HEAD_DIM] for i in range(group_size + 2)]
    queries = jnp.concatenate([turn(cut[i], cos_t, sin_t).astype(BF16) for i in range(group_size)], axis=0)
    return queries, turn(cut[group_size], cos_t, sin_t).astype(BF16), cut[group_size + 1].astype(BF16)


def store_halves(first, own_ref, rec_ref, columns, lower, upper):
    own_ref[0, :, columns] = jnp.where(first, lower, upper).astype(own_ref.dtype)
    rec_ref[0, :, columns] = jnp.where(first, upper, lower).astype(rec_ref.dtype)


def attention_fwd_kernel(group_size, tp_ref, own_ref, rec_ref, cos_ref, sin_ref, out_own_ref, out_rec_ref):
    half = own_ref.shape[1]
    first = tp_ref[0] == 0
    lower, upper = pick_halves(first, own_ref[0], rec_ref[0])
    q_lo, k_lo, v_lo = heads_of(group_size, lower, cos_ref[:half], sin_ref[:half])
    q_up, k_up, v_up = heads_of(group_size, upper, cos_ref[half:], sin_ref[half:])
    rows = lax.broadcasted_iota(jnp.int32, (group_size, half, half), 1).reshape(group_size * half, half)
    cols = lax.broadcasted_iota(jnp.int32, (group_size * half, half), 1)
    causal = rows >= cols

    s_lo = jnp.where(causal, dot(q_lo, k_lo, NT), MASK_VALUE)
    p_lo = jnp.exp((s_lo - jnp.max(s_lo, axis=1, keepdims=True)) * SCORE_SCALE)
    p_lo = (p_lo * (1.0 / jnp.sum(p_lo, axis=1, keepdims=True))).astype(BF16)
    a_lo = dot(p_lo, v_lo, NN)

    s_a = dot(q_up, k_lo, NT)
    s_b = jnp.where(causal, dot(q_up, k_up, NT), MASK_VALUE)
    top = jnp.maximum(jnp.max(s_a, axis=1, keepdims=True), jnp.max(s_b, axis=1, keepdims=True))
    p_a = jnp.exp((s_a - top) * SCORE_SCALE)
    p_b = jnp.exp((s_b - top) * SCORE_SCALE)
    inv = 1.0 / (jnp.sum(p_a, axis=1, keepdims=True) + jnp.sum(p_b, axis=1, keepdims=True))
    a_up = dot((p_a * inv).astype(BF16), v_lo, NN) + dot((p_b * inv).astype(BF16), v_up, NN)
    for i in range(group_size):
        part = slice(i * half, (i + 1) * half)
        store_halves(first, out_own_ref, out_rec_ref, slice(i * HEAD_DIM, (i + 1) * HEAD_DIM), a_lo[part], a_up[part])


def attention_bwd_kernel(group_size, tp_ref, own_ref, rec_ref, cos_ref, sin_ref, ga_own_ref, ga_rec_ref, *rest):
    out_own_ref, out_rec_ref = rest[-2:]
    half = own_ref.shape[1]
    first = tp_ref[0] == 0
    lower, upper = pick_halves(first, own_ref[0], rec_ref[0])
    cos_lo, sin_lo, cos_up, sin_up = cos_ref[:half], sin_ref[:half], cos_ref[half:], sin_ref[half:]
    q_lo, k_lo, v_lo = heads_of(group_size, lower, cos_lo, sin_lo)
    q_up, k_up, v_up = heads_of(group_size, upper, cos_up, sin_up)
    ga_lower, ga_upper = pick_halves(first, ga_own_ref[0], ga_rec_ref[0])

    def stacked(block):
        return jnp.concatenate([block[:, i * HEAD_DIM:(i + 1) * HEAD_DIM].astype(BF16) for i in range(group_size)], axis=0)

    ga_lo, ga_up = stacked(ga_lower), stacked(ga_upper)
    keys = lax.broadcasted_iota(jnp.int32, (half, half), 0)
    spots = lax.broadcasted_iota(jnp.int32, (half, half), 1)
    causal = jnp.concatenate([spots >= keys] * group_size, axis=1)

    s_lo = jnp.where(causal, dot(k_lo, q_lo, NT), MASK_VALUE)
    p_lo = jnp.exp((s_lo - jnp.max(s_lo, axis=0, keepdims=True)) * SCORE_SCALE)
    p_lo = p_lo * (1.0 / jnp.sum(p_lo, axis=0, keepdims=True))
    gp_lo = dot(v_lo, ga_lo, NT).astype(BF16).astype(F32)
    gs_lo = (p_lo * (gp_lo - jnp.sum(gp_lo * p_lo, axis=0, keepdims=True)) * SCORE_SCALE).astype(BF16)

    s_a = dot(k_lo, q_up, NT)
    s_b = jnp.where(causal, dot(k_up, q_up, NT), MASK_VALUE)
    top = jnp.maximum(jnp.max(s_a, axis=0, keepdims=True), jnp.max(s_b, axis=0, keepdims=True))
    p_a = jnp.exp((s_a - top) * SCORE_SCALE)
    p_b = jnp.exp((s_b - top) * SCORE_SCALE)
    inv = 1.0 / (jnp.sum(p_a, axis=0, keepdims=True) + jnp.sum(p_b, axis=0, keepdims=True))
    p_a = p_a * inv
    p_b = p_b * inv
    gp_a = dot(v_lo, ga_up, NT).astype(BF16).astype(F32)
    gp_b = dot(v_up, ga_up, NT).astype(BF16).astype(F32)
    mean_up = jnp.sum(gp_a * p_a, axis=0, keepdims=True) + jnp.sum(gp_b * p_b, axis=0, keepdims=True)
    gs_a = (p_a * (gp_a - mean_up) * SCORE_SCALE).astype(BF16)
    gs_b = (p_b * (gp_b - mean_up) * SCORE_SCALE).astype(BF16)

    gv_lo = dot(p_lo.astype(BF16), ga_lo, NN) + dot(p_a.astype(BF16), ga_up, NN)
    gv_up = dot(p_b.astype(BF16), ga_up, NN)
    gk_lo = (dot(gs_lo, q_lo, NN) + dot(gs_a, q_up, NN)).astype(BF16).astype(F32)
    gk_up = dot(gs_b, q_up, NN).astype(BF16).astype(F32)
    gq_lo = dot(gs_lo, k_lo, TN).astype(BF16).astype(F32)
    gq_up = (dot(gs_a, k_lo, TN) + dot(gs_b, k_up, TN)).astype(BF16).astype(F32)

    def store(index, lower_part, upper_part):
        store_halves(first, out_own_ref, out_rec_ref, slice(index * HEAD_DIM, (index + 1) * HEAD_DIM), lower_part, upper_part)

    for i in range(group_size):
        part = slice(i * half, (i + 1) * half)
        store(i, turn(gq_lo[part], cos_lo, -sin_lo), turn(gq_up[part], cos_up, -sin_up))
    store(group_size, turn(gk_lo, cos_lo, -sin_lo), turn(gk_up, cos_up, -sin_up))
    store(group_size + 1, gv_lo, gv_up)


def cost(flops, transcendentals, *arrays):
    return pl.CostEstimate(flops=int(flops), transcendentals=int(transcendentals), bytes_accessed=int(sum(a.size * a.dtype.itemsize for a in arrays)))


def attention_fwd(tp_index, qkv_own, qkv_rec, tables, groups, group_size):
    batch, half, width = qkv_own.shape
    block = width // groups
    out_block = group_size * HEAD_DIM
    shape = jax.ShapeDtypeStruct((batch, half, groups * out_block), BF16)
    spec = lambda columns: pl.BlockSpec((1, half, columns), lambda b, g, tp: (b, 0, g))
    table = pl.BlockSpec((2 * half, HEAD_DIM), lambda b, g, tp: (0, 0))
    return pl.pallas_call(
        functools.partial(attention_fwd_kernel, group_size),
        out_shape=(shape, shape),
        grid_spec=pltpu.PrefetchScalarGridSpec(
            num_scalar_prefetch=1,
            grid=(batch, groups),
            in_specs=[spec(block), spec(block), table, table],
            out_specs=(spec(out_block), spec(out_block)),
        ),
        compiler_params=pltpu.CompilerParams(vmem_limit_bytes=48 * 2**20),
        cost_estimate=cost(batch * groups * group_size * half * half * HEAD_DIM * 12, batch * groups * group_size * half * half * 3, qkv_own, qkv_rec, shape, shape),
        name="attention_fwd",
    )(tp_index, qkv_own, qkv_rec, *tables)


def attention_bwd(tp_index, qkv_own, qkv_rec, tables, ga_own, ga_rec, start, held, groups, group_size):
    batch, half, width = qkv_own.shape
    count = ga_rec.shape[0]
    block = width // groups
    ga_block = group_size * HEAD_DIM
    shape = jax.ShapeDtypeStruct((batch, half, width), BF16)
    spec = lambda columns, offset: pl.BlockSpec((1, half, columns), lambda b, g, tp: (b + offset, 0, g))
    table = pl.BlockSpec((2 * half, HEAD_DIM), lambda b, g, tp: (0, 0))
    in_specs = [spec(block, start), spec(block, start), table, table, spec(ga_block, start), spec(ga_block, 0)]
    args = [tp_index, qkv_own, qkv_rec, *tables, ga_own, ga_rec]
    aliases = {}
    if held is not None:
        in_specs += [pl.BlockSpec(memory_space=pl.ANY)] * 2
        aliases = {len(args): 0, len(args) + 1: 1}
        args += list(held)
    work = count * groups * group_size * half * half
    return pl.pallas_call(
        functools.partial(attention_bwd_kernel, group_size),
        out_shape=(shape, shape),
        grid_spec=pltpu.PrefetchScalarGridSpec(
            num_scalar_prefetch=1,
            grid=(count, groups),
            in_specs=in_specs,
            out_specs=(spec(block, start), spec(block, start)),
        ),
        input_output_aliases=aliases,
        compiler_params=pltpu.CompilerParams(vmem_limit_bytes=48 * 2**20),
        cost_estimate=cost(work * HEAD_DIM * 30, work * 3, ga_rec, ga_rec, ga_rec, ga_rec),
        name="attention_bwd",
    )(*args)


def finish_out_kernel(x_ref, near_ref, far_ref, *rest):
    out_sum = (near_ref[0].astype(F32) + far_ref[0].astype(F32)).astype(BF16).astype(F32)
    rest[-1][0] = (x_ref[0].astype(F32) + out_sum).astype(BF16)


def finish_grad_kernel(x_ref, dy_ref, near_ref, gain_ref, far_ref, *rest):
    out_ref, gain_out_ref = rest[-2:]
    values = x_ref[0].astype(F32)
    inv_rms = lax.rsqrt(jnp.mean(values * values, axis=-1, keepdims=True) + NORM_EPS)
    x_hat = values * inv_rms
    grad_normed = (near_ref[0].astype(F32) + far_ref[0].astype(F32)).astype(BF16).astype(F32)
    scaled = grad_normed * gain_ref[...]
    mean = jnp.mean(scaled * x_hat, axis=-1, keepdims=True)
    out_ref[0] = (dy_ref[0].astype(F32) + inv_rms * (scaled - x_hat * mean)).astype(BF16)

    @pl.when((pl.program_id(0) == 0) & (pl.program_id(1) == 0))
    def _():
        gain_out_ref[...] = jnp.zeros_like(gain_out_ref)

    gain_out_ref[...] += jnp.sum((grad_normed * x_hat).reshape(-1, 8, x_hat.shape[-1]), axis=0)


def finish(kernel, full, chunk, start, held, gain=None, row_block=64):
    batch, half, width = full[0].shape
    count = chunk[0].shape[0]
    row_block = min(row_block, half)
    spec = lambda offset: pl.BlockSpec((1, row_block, width), lambda b, r: (b + offset, r, 0))
    in_specs = [spec(start)] * len(full)
    args = list(full)
    out_shape = [jax.ShapeDtypeStruct((batch, half, width), BF16)]
    out_specs = [spec(start)]
    if gain is not None:
        in_specs.append(pl.BlockSpec((1, width), lambda b, r: (0, 0)))
        args.append(gain.reshape(1, width))
        out_shape.append(jax.ShapeDtypeStruct((8, width), F32))
        out_specs.append(pl.BlockSpec((8, width), lambda b, r: (0, 0)))
    in_specs += [spec(0)] * len(chunk)
    args += list(chunk)
    aliases = {}
    if held is not None:
        aliases = {len(args): 0}
        in_specs.append(pl.BlockSpec(memory_space=pl.ANY))
        args.append(held)
    result = pl.pallas_call(
        kernel,
        out_shape=out_shape,
        grid=(count, half // row_block),
        in_specs=in_specs,
        out_specs=out_specs,
        input_output_aliases=aliases,
        compiler_params=pltpu.CompilerParams(vmem_limit_bytes=32 * 2**20),
        cost_estimate=cost(count * half * width * 400, 0, *([chunk[0]] * (len(full) + len(chunk) + 1))),
    )(*args)
    return result if gain is not None else result[0]


DY_CHUNKS = 2
OUT_CHUNKS = 2
DN_CHUNKS = 4


def after(value, *others):
    return lax.optimization_barrier((value, *others))[0]


def solution(mesh):
    swap = [(0, 1), (1, 0)]

    def exchange(values):
        return lax.ppermute(values, "tp", swap)

    def mm(eq, a, b):
        return jnp.einsum(eq, a, b, preferred_element_type=F32)

    def local_block(hidden, norm_gain, w_query, w_key, w_value, w_out, grad_out):
        batch, half, _ = hidden.shape
        rows_loc = w_query.shape[0]
        groups = w_key.shape[1] // HEAD_DIM
        group_size = w_query.shape[1] // w_key.shape[1]
        block = (group_size + 2) * HEAD_DIM
        tp_index = lax.axis_index("tp").astype(jnp.int32).reshape(1)
        tables = rope_tables(2 * half)

        hidden_rec = exchange(hidden)
        step = batch // DY_CHUNKS
        grad_rec = []
        for i in range(DY_CHUNKS):
            grad_rec.append(exchange(grad_out[i * step:(i + 1) * step]))

        w_qkv = jnp.concatenate(
            [w_query.reshape(rows_loc, groups, -1), w_key.reshape(rows_loc, groups, -1), w_value.reshape(rows_loc, groups, -1)], axis=2
        ).reshape(rows_loc, groups * block)
        w_qkv = lax.all_gather(w_qkv, "dp", axis=0, tiled=True)
        w_o = lax.all_gather(w_out, "dp", axis=1, tiled=True)
        gain = lax.all_gather(norm_gain, "dp", axis=0, tiled=True).astype(F32)

        def norm(values):
            values = values.astype(F32)
            inv_rms = lax.rsqrt(jnp.mean(values * values, axis=-1, keepdims=True) + NORM_EPS)
            return (values * inv_rms * gain).astype(BF16)

        normed_own = norm(hidden)
        qkv_own = mm("bsd,de->bse", normed_own, w_qkv).astype(BF16)
        normed_rec = norm(after(hidden_rec, qkv_own))
        qkv_rec = mm("bsd,de->bse", normed_rec, w_qkv).astype(BF16)
        attn_own, attn_rec = attention_fwd(tp_index, qkv_own, qkv_rec, tables, groups, group_size)

        step = batch // OUT_CHUNKS
        out_send = []
        for i in range(OUT_CHUNKS):
            out_send.append(mm("bse,ed->bsd", attn_rec[i * step:(i + 1) * step], w_o).astype(BF16))
        out_far = []
        for i in range(OUT_CHUNKS):
            out_far.append(exchange(out_send[i]))

        ga_own = mm("bsd,ed->bse", after(grad_out, *out_send), w_o).astype(BF16)
        held = None
        step = batch // DY_CHUNKS
        for i in range(DY_CHUNKS):
            if i == DY_CHUNKS - 1:
                grad_wo = mm("bse,bsd->ed", attn_own, after(grad_out, *held)) + mm("bse,bsd->ed", attn_rec, jnp.concatenate(grad_rec, axis=0))
                ga_rec = mm("bsd,ed->bse", after(grad_rec[i], grad_wo), w_o).astype(BF16)
            else:
                ga_rec = mm("bsd,ed->bse", after(grad_rec[i], ga_own), w_o).astype(BF16)
            held = attention_bwd(tp_index, qkv_own, qkv_rec, tables, ga_own, ga_rec, i * step, held, groups, group_size)
        gqkv_own, gqkv_rec = held

        grad_wo = lax.psum_scatter(grad_wo, "dp", scatter_dimension=1, tiled=True)
        grad_wqkv = mm("bsd,bse->de", normed_own, gqkv_own) + mm("bsd,bse->de", normed_rec, gqkv_rec)
        gqkv_own, gqkv_rec = after((gqkv_own, gqkv_rec), grad_wqkv)
        grad_wqkv = lax.psum_scatter(grad_wqkv, "dp", scatter_dimension=0, tiled=True)

        step = batch // DN_CHUNKS
        dn_send = []
        for i in range(DN_CHUNKS):
            dn_send.append(mm("bse,de->bsd", gqkv_rec[i * step:(i + 1) * step], w_qkv).astype(BF16))
        dn_far = []
        for i in range(DN_CHUNKS):
            dn_far.append(exchange(dn_send[i]))

        attn_own, gqkv_own = after((attn_own, gqkv_own), *dn_send)
        out_near = lax.optimization_barrier(mm("bse,ed->bsd", attn_own, w_o).astype(BF16))
        dn_near = lax.optimization_barrier(mm("bse,de->bsd", gqkv_own, w_qkv).astype(BF16))
        hidden_out = None
        step = batch // OUT_CHUNKS
        for i in range(OUT_CHUNKS):
            hidden_out = finish(finish_out_kernel, [hidden, out_near], [out_far[i]], i * step, hidden_out)
        dn_near = after(dn_near, hidden_out)
        grad_hidden = None
        gain_parts = []
        step = batch // DN_CHUNKS
        for i in range(DN_CHUNKS):
            grad_hidden, part = finish(
                finish_grad_kernel, [hidden, grad_out, dn_near], [dn_far[i]], i * step, grad_hidden, gain
            )
            gain_parts.append(part)
        gain_sum = lax.psum(jnp.sum(sum(gain_parts), axis=0), ("dp", "tp"))
        grad_gain = lax.dynamic_slice(gain_sum, (lax.axis_index("dp") * rows_loc,), (rows_loc,))

        grad_wqkv = grad_wqkv.reshape(rows_loc, groups, block)
        split = group_size * HEAD_DIM
        grad_wq = grad_wqkv[:, :, :split].reshape(rows_loc, -1)
        grad_wk = grad_wqkv[:, :, split:split + HEAD_DIM].reshape(rows_loc, -1)
        grad_wv = grad_wqkv[:, :, split + HEAD_DIM:].reshape(rows_loc, -1)
        return hidden_out, grad_hidden, grad_gain, grad_wq, grad_wk, grad_wv, grad_wo

    act_spec = P("dp", "tp", None)
    col_spec = P("dp", "tp")
    row_spec = P("tp", "dp")
    return jax.shard_map(
        local_block,
        mesh=mesh,
        in_specs=(act_spec, P("dp"), col_spec, col_spec, col_spec, row_spec, act_spec),
        out_specs=(act_spec, act_spec, P("dp"), col_spec, col_spec, col_spec, row_spec),
        check_vma=False,
    )
```

```python
import functools

import jax
import jax.numpy as jnp
from jax import lax
from jax.experimental import pallas as pl
from jax.experimental.pallas import tpu as pltpu
from jax.sharding import PartitionSpec as P


HEAD_DIM = 128
NORM_EPS = 1e-5
ROPE_BASE = 500000.0
SCORE_SCALE = HEAD_DIM ** -0.5
MASK_VALUE = -1e30
F32 = jnp.float32
BF16 = jnp.bfloat16
NT = (((1,), (1,)), ((), ()))
NN = (((1,), (0,)), ((), ()))
TN = (((0,), (0,)), ((), ()))


def rope_tables(seq_len):
    half_dim = HEAD_DIM // 2
    inv_freq = ROPE_BASE ** (-jnp.arange(half_dim, dtype=F32) * 2.0 / HEAD_DIM)
    angles = jnp.arange(seq_len, dtype=F32)[:, None] * inv_freq[None, :]
    cos_t, sin_t = jnp.cos(angles), jnp.sin(angles)
    return jnp.concatenate([cos_t, cos_t], axis=1), jnp.concatenate([-sin_t, sin_t], axis=1)


def dot(lhs, rhs, dims):
    return lax.dot_general(lhs, rhs, dims, preferred_element_type=F32)


def turn(values, cos_t, sin_t):
    return values * cos_t + pltpu.roll(values, HEAD_DIM // 2, 1) * sin_t


def pick_halves(first, own, rec):
    own, rec = own.astype(F32), rec.astype(F32)
    return jnp.where(first, own, rec), jnp.where(first, rec, own)


def heads_of(group_size, block, cos_t, sin_t):
    cut = [block[:, i * HEAD_DIM:(i + 1) * HEAD_DIM] for i in range(group_size + 2)]
    queries = jnp.concatenate([turn(cut[i], cos_t, sin_t).astype(BF16) for i in range(group_size)], axis=0)
    return queries, turn(cut[group_size], cos_t, sin_t).astype(BF16), cut[group_size + 1].astype(BF16)


def store_halves(first, own_ref, rec_ref, columns, lower, upper):
    own_ref[0, :, columns] = jnp.where(first, lower, upper).astype(own_ref.dtype)
    rec_ref[0, :, columns] = jnp.where(first, upper, lower).astype(rec_ref.dtype)


def attention_fwd_kernel(group_size, tp_ref, own_ref, rec_ref, cos_ref, sin_ref, *rest):
    out_own_ref, out_rec_ref = rest[-2:]
    half = own_ref.shape[1]
    first = tp_ref[0] == 0
    lower, upper = pick_halves(first, own_ref[0], rec_ref[0])
    q_lo, k_lo, v_lo = heads_of(group_size, lower, cos_ref[:half], sin_ref[:half])
    q_up, k_up, v_up = heads_of(group_size, upper, cos_ref[half:], sin_ref[half:])
    rows = lax.broadcasted_iota(jnp.int32, (group_size, half, half), 1).reshape(group_size * half, half)
    cols = lax.broadcasted_iota(jnp.int32, (group_size * half, half), 1)
    causal = rows >= cols

    s_lo = jnp.where(causal, dot(q_lo, k_lo, NT), MASK_VALUE)
    p_lo = jnp.exp((s_lo - jnp.max(s_lo, axis=1, keepdims=True)) * SCORE_SCALE)
    p_lo = (p_lo * (1.0 / jnp.sum(p_lo, axis=1, keepdims=True))).astype(BF16)
    a_lo = dot(p_lo, v_lo, NN)

    s_a = dot(q_up, k_lo, NT)
    s_b = jnp.where(causal, dot(q_up, k_up, NT), MASK_VALUE)
    top = jnp.maximum(jnp.max(s_a, axis=1, keepdims=True), jnp.max(s_b, axis=1, keepdims=True))
    p_a = jnp.exp((s_a - top) * SCORE_SCALE)
    p_b = jnp.exp((s_b - top) * SCORE_SCALE)
    inv = 1.0 / (jnp.sum(p_a, axis=1, keepdims=True) + jnp.sum(p_b, axis=1, keepdims=True))
    a_up = dot((p_a * inv).astype(BF16), v_lo, NN) + dot((p_b * inv).astype(BF16), v_up, NN)
    for i in range(group_size):
        part = slice(i * half, (i + 1) * half)
        store_halves(first, out_own_ref, out_rec_ref, slice(i * HEAD_DIM, (i + 1) * HEAD_DIM), a_lo[part], a_up[part])


def attention_bwd_kernel(group_size, tp_ref, own_ref, rec_ref, cos_ref, sin_ref, ga_own_ref, ga_rec_ref, *rest):
    out_own_ref, out_rec_ref = rest[-2:]
    half = own_ref.shape[1]
    first = tp_ref[0] == 0
    lower, upper = pick_halves(first, own_ref[0], rec_ref[0])
    cos_lo, sin_lo, cos_up, sin_up = cos_ref[:half], sin_ref[:half], cos_ref[half:], sin_ref[half:]
    q_lo, k_lo, v_lo = heads_of(group_size, lower, cos_lo, sin_lo)
    q_up, k_up, v_up = heads_of(group_size, upper, cos_up, sin_up)
    ga_lower, ga_upper = pick_halves(first, ga_own_ref[0], ga_rec_ref[0])

    def stacked(block):
        return jnp.concatenate([block[:, i * HEAD_DIM:(i + 1) * HEAD_DIM].astype(BF16) for i in range(group_size)], axis=0)

    ga_lo, ga_up = stacked(ga_lower), stacked(ga_upper)
    keys = lax.broadcasted_iota(jnp.int32, (half, half), 0)
    spots = lax.broadcasted_iota(jnp.int32, (half, half), 1)
    causal = jnp.concatenate([spots >= keys] * group_size, axis=1)

    s_lo = jnp.where(causal, dot(k_lo, q_lo, NT), MASK_VALUE)
    p_lo = jnp.exp((s_lo - jnp.max(s_lo, axis=0, keepdims=True)) * SCORE_SCALE)
    p_lo = p_lo * (1.0 / jnp.sum(p_lo, axis=0, keepdims=True))
    gp_lo = dot(v_lo, ga_lo, NT).astype(BF16).astype(F32)
    gs_lo = (p_lo * (gp_lo - jnp.sum(gp_lo * p_lo, axis=0, keepdims=True)) * SCORE_SCALE).astype(BF16)

    s_a = dot(k_lo, q_up, NT)
    s_b = jnp.where(causal, dot(k_up, q_up, NT), MASK_VALUE)
    top = jnp.maximum(jnp.max(s_a, axis=0, keepdims=True), jnp.max(s_b, axis=0, keepdims=True))
    p_a = jnp.exp((s_a - top) * SCORE_SCALE)
    p_b = jnp.exp((s_b - top) * SCORE_SCALE)
    inv = 1.0 / (jnp.sum(p_a, axis=0, keepdims=True) + jnp.sum(p_b, axis=0, keepdims=True))
    p_a = p_a * inv
    p_b = p_b * inv
    gp_a = dot(v_lo, ga_up, NT).astype(BF16).astype(F32)
    gp_b = dot(v_up, ga_up, NT).astype(BF16).astype(F32)
    mean_up = jnp.sum(gp_a * p_a, axis=0, keepdims=True) + jnp.sum(gp_b * p_b, axis=0, keepdims=True)
    gs_a = (p_a * (gp_a - mean_up) * SCORE_SCALE).astype(BF16)
    gs_b = (p_b * (gp_b - mean_up) * SCORE_SCALE).astype(BF16)

    gv_lo = dot(p_lo.astype(BF16), ga_lo, NN) + dot(p_a.astype(BF16), ga_up, NN)
    gv_up = dot(p_b.astype(BF16), ga_up, NN)
    gk_lo = (dot(gs_lo, q_lo, NN) + dot(gs_a, q_up, NN)).astype(BF16).astype(F32)
    gk_up = dot(gs_b, q_up, NN).astype(BF16).astype(F32)
    gq_lo = dot(gs_lo, k_lo, TN).astype(BF16).astype(F32)
    gq_up = (dot(gs_a, k_lo, TN) + dot(gs_b, k_up, TN)).astype(BF16).astype(F32)

    def store(index, lower_part, upper_part):
        store_halves(first, out_own_ref, out_rec_ref, slice(index * HEAD_DIM, (index + 1) * HEAD_DIM), lower_part, upper_part)

    for i in range(group_size):
        part = slice(i * half, (i + 1) * half)
        store(i, turn(gq_lo[part], cos_lo, -sin_lo), turn(gq_up[part], cos_up, -sin_up))
    store(group_size, turn(gk_lo, cos_lo, -sin_lo), turn(gk_up, cos_up, -sin_up))
    store(group_size + 1, gv_lo, gv_up)


def cost(flops, transcendentals, *arrays):
    return pl.CostEstimate(flops=int(flops), transcendentals=int(transcendentals), bytes_accessed=int(sum(a.size * a.dtype.itemsize for a in arrays)))


def attention_fwd(tp_index, qkv_own, qkv_rec, tables, start, held, groups, group_size):
    batch, half, width = qkv_own.shape
    count = qkv_rec.shape[0]
    block = width // groups
    out_block = group_size * HEAD_DIM
    shape = jax.ShapeDtypeStruct((batch, half, groups * out_block), BF16)
    spec = lambda columns, offset: pl.BlockSpec((1, half, columns), lambda b, g, tp: (b + offset, 0, g))
    table = pl.BlockSpec((2 * half, HEAD_DIM), lambda b, g, tp: (0, 0))
    in_specs = [spec(block, start), spec(block, 0), table, table]
    args = [tp_index, qkv_own, qkv_rec, *tables]
    aliases = {}
    if held is not None:
        in_specs += [pl.BlockSpec(memory_space=pl.ANY)] * 2
        aliases = {len(args): 0, len(args) + 1: 1}
        args += list(held)
    work = count * groups * group_size * half * half
    return pl.pallas_call(
        functools.partial(attention_fwd_kernel, group_size),
        out_shape=(shape, shape),
        grid_spec=pltpu.PrefetchScalarGridSpec(
            num_scalar_prefetch=1,
            grid=(count, groups),
            in_specs=in_specs,
            out_specs=(spec(out_block, start), spec(out_block, start)),
        ),
        input_output_aliases=aliases,
        compiler_params=pltpu.CompilerParams(vmem_limit_bytes=48 * 2**20),
        cost_estimate=cost(work * HEAD_DIM * 12, work * 3, qkv_rec, qkv_rec),
        name="attention_fwd",
    )(*args)


def attention_bwd(tp_index, qkv_own, qkv_rec, tables, ga_own, ga_rec, start, held, groups, group_size):
    batch, half, width = qkv_own.shape
    count = ga_rec.shape[0]
    block = width // groups
    ga_block = group_size * HEAD_DIM
    shape = jax.ShapeDtypeStruct((batch, half, width), BF16)
    spec = lambda columns, offset: pl.BlockSpec((1, half, columns), lambda b, g, tp: (b + offset, 0, g))
    table = pl.BlockSpec((2 * half, HEAD_DIM), lambda b, g, tp: (0, 0))
    in_specs = [spec(block, start), spec(block, 0), table, table, spec(ga_block, start), spec(ga_block, 0)]
    args = [tp_index, qkv_own, qkv_rec, *tables, ga_own, ga_rec]
    aliases = {}
    if held is not None:
        in_specs += [pl.BlockSpec(memory_space=pl.ANY)] * 2
        aliases = {len(args): 0, len(args) + 1: 1}
        args += list(held)
    work = count * groups * group_size * half * half
    return pl.pallas_call(
        functools.partial(attention_bwd_kernel, group_size),
        out_shape=(shape, shape),
        grid_spec=pltpu.PrefetchScalarGridSpec(
            num_scalar_prefetch=1,
            grid=(count, groups),
            in_specs=in_specs,
            out_specs=(spec(block, start), spec(block, start)),
        ),
        input_output_aliases=aliases,
        compiler_params=pltpu.CompilerParams(vmem_limit_bytes=48 * 2**20),
        cost_estimate=cost(work * HEAD_DIM * 30, work * 3, ga_rec, ga_rec, ga_rec, ga_rec),
        name="attention_bwd",
    )(*args)


def finish_out_kernel(x_ref, near_ref, far_ref, *rest):
    out_sum = (near_ref[0].astype(F32) + far_ref[0].astype(F32)).astype(BF16).astype(F32)
    rest[-1][0] = (x_ref[0].astype(F32) + out_sum).astype(BF16)


def finish_grad_kernel(x_ref, dy_ref, near_ref, gain_ref, far_ref, *rest):
    out_ref, gain_out_ref = rest[-2:]
    values = x_ref[0].astype(F32)
    inv_rms = lax.rsqrt(jnp.mean(values * values, axis=-1, keepdims=True) + NORM_EPS)
    x_hat = values * inv_rms
    grad_normed = (near_ref[0].astype(F32) + far_ref[0].astype(F32)).astype(BF16).astype(F32)
    scaled = grad_normed * gain_ref[...]
    mean = jnp.mean(scaled * x_hat, axis=-1, keepdims=True)
    out_ref[0] = (dy_ref[0].astype(F32) + inv_rms * (scaled - x_hat * mean)).astype(BF16)

    @pl.when((pl.program_id(0) == 0) & (pl.program_id(1) == 0))
    def _():
        gain_out_ref[...] = jnp.zeros_like(gain_out_ref)

    gain_out_ref[...] += jnp.sum((grad_normed * x_hat).reshape(-1, 8, x_hat.shape[-1]), axis=0)


def finish(kernel, full, chunk, start, held, gain=None, row_block=64):
    batch, half, width = full[0].shape
    count = chunk[0].shape[0]
    row_block = min(row_block, half)
    spec = lambda offset: pl.BlockSpec((1, row_block, width), lambda b, r: (b + offset, r, 0))
    in_specs = [spec(start)] * len(full)
    args = list(full)
    out_shape = [jax.ShapeDtypeStruct((batch, half, width), BF16)]
    out_specs = [spec(start)]
    if gain is not None:
        in_specs.append(pl.BlockSpec((1, width), lambda b, r: (0, 0)))
        args.append(gain.reshape(1, width))
        out_shape.append(jax.ShapeDtypeStruct((8, width), F32))
        out_specs.append(pl.BlockSpec((8, width), lambda b, r: (0, 0)))
    in_specs += [spec(0)] * len(chunk)
    args += list(chunk)
    aliases = {}
    if held is not None:
        aliases = {len(args): 0}
        in_specs.append(pl.BlockSpec(memory_space=pl.ANY))
        args.append(held)
    result = pl.pallas_call(
        kernel,
        out_shape=out_shape,
        grid=(count, half // row_block),
        in_specs=in_specs,
        out_specs=out_specs,
        input_output_aliases=aliases,
        compiler_params=pltpu.CompilerParams(vmem_limit_bytes=32 * 2**20),
        cost_estimate=cost(count * half * width * 400, 0, *([chunk[0]] * (len(full) + len(chunk) + 1))),
    )(*args)
    return result if gain is not None else result[0]


def regroup_kernel(q_ref, k_ref, v_ref, out_ref):
    split = q_ref.shape[1]
    out_ref[:, :split] = q_ref[...]
    out_ref[:, split:split + HEAD_DIM] = k_ref[...]
    out_ref[:, split + HEAD_DIM:] = v_ref[...]


def regroup(w_query, w_key, w_value):
    rows = w_query.shape[0]
    groups = w_key.shape[1] // HEAD_DIM
    split = w_query.shape[1] // groups
    spec = lambda columns: pl.BlockSpec((rows, columns), lambda g: (0, g))
    out = jax.ShapeDtypeStruct((rows, groups * (split + 2 * HEAD_DIM)), w_query.dtype)
    return pl.pallas_call(
        regroup_kernel,
        out_shape=out,
        grid=(groups,),
        in_specs=[spec(split), spec(HEAD_DIM), spec(HEAD_DIM)],
        out_specs=spec(split + 2 * HEAD_DIM),
        cost_estimate=cost(rows * out.shape[1] * 400, 0, out, out),
        name="regroup",
    )(w_query, w_key, w_value)


def ungroup_kernel(first_ref, near_a_ref, far_a_ref, near_b_ref, far_b_ref, q_ref, k_ref, v_ref):
    split = q_ref.shape[1]
    group, last = pl.program_id(0), pl.num_programs(0) - 1

    def put(block):
        q_ref[...] = block[:, :split]
        k_ref[...] = block[:, split:split + HEAD_DIM]
        v_ref[...] = block[:, split + HEAD_DIM:]

    @pl.when(group < last - 1)
    def _():
        put(first_ref[...])

    @pl.when(group == last - 1)
    def _():
        put(near_a_ref[...] + far_a_ref[...])

    @pl.when(group == last)
    def _():
        put(near_b_ref[...] + far_b_ref[...])


def ungroup(first, terms_a, terms_b, groups):
    rows, block = terms_a[0].shape
    split = block - 2 * HEAD_DIM
    row_block = rows // 2
    spec = lambda columns: pl.BlockSpec((row_block, columns), lambda g, r: (r, g))
    late = pl.BlockSpec((row_block, block), lambda g, r: (r, 0))
    shape = lambda columns: jax.ShapeDtypeStruct((rows, groups * columns), F32)
    return pl.pallas_call(
        ungroup_kernel,
        out_shape=(shape(split), shape(HEAD_DIM), shape(HEAD_DIM)),
        grid=(groups, rows // row_block),
        in_specs=[pl.BlockSpec((row_block, block), lambda g, r: (r, jnp.minimum(g, groups - 3))), late, late, late, late],
        out_specs=(spec(split), spec(HEAD_DIM), spec(HEAD_DIM)),
        compiler_params=pltpu.CompilerParams(vmem_limit_bytes=32 * 2**20),
        cost_estimate=cost(rows * block * groups * 400, 0, first, *terms_a, *terms_b, first, first),
        name="ungroup",
    )(first, *terms_a, *terms_b)


CHUNKS = 2


def after(value, *others):
    return lax.optimization_barrier((value, *others))[0]


def solution(mesh):
    swap = [(0, 1), (1, 0)]

    def exchange(values):
        return lax.ppermute(values, "tp", swap)

    def mm(eq, a, b):
        return jnp.einsum(eq, a, b, preferred_element_type=F32)

    def local_block(hidden, norm_gain, w_query, w_key, w_value, w_out, grad_out):
        batch, half, _ = hidden.shape
        rows_loc = w_query.shape[0]
        groups = w_key.shape[1] // HEAD_DIM
        group_size = w_query.shape[1] // w_key.shape[1]
        block = (group_size + 2) * HEAD_DIM
        tp_index = lax.axis_index("tp").astype(jnp.int32).reshape(1)
        tables = rope_tables(2 * half)

        step = batch // CHUNKS
        hidden_rec, grad_rec = [], []
        source = hidden
        for i in range(CHUNKS):
            piece = lax.optimization_barrier(source[i * step:(i + 1) * step])
            source = after(hidden, piece)
            hidden_rec.append(exchange(piece))
        for i in range(CHUNKS):
            grad_rec.append(exchange(grad_out[i * step:(i + 1) * step]))

        w_qkv = regroup(w_query, w_key, w_value)
        w_qkv = lax.all_gather(w_qkv, "dp", axis=0, tiled=True)
        w_o = lax.all_gather(w_out, "dp", axis=1, tiled=True)
        gain = lax.all_gather(norm_gain, "dp", axis=0, tiled=True).astype(F32)

        def norm(values):
            values = values.astype(F32)
            inv_rms = lax.rsqrt(jnp.mean(values * values, axis=-1, keepdims=True) + NORM_EPS)
            return (values * inv_rms * gain).astype(BF16)

        normed_own = norm(hidden)
        qkv_own = mm("bsd,de->bse", normed_own, w_qkv).astype(BF16)
        qkv_rec = []
        attn = None
        before = qkv_own
        for i in range(CHUNKS):
            rec = norm(after(hidden_rec[i], before))
            qkv_rec.append(mm("bsd,de->bse", rec, w_qkv).astype(BF16))
            attn = attention_fwd(tp_index, qkv_own, qkv_rec[i], tables, i * step, attn, groups, group_size)
            before = attn[0]
        attn_own, attn_rec = attn

        out_send = []
        for i in range(CHUNKS):
            out_send.append(lax.optimization_barrier(mm("bse,ed->bsd", attn_rec[i * step:(i + 1) * step], w_o).astype(BF16)))

        ga_own = mm("bsd,ed->bse", after(grad_out, *out_send), w_o).astype(BF16)
        normed_rec = norm(jnp.concatenate([after(piece, ga_own) for piece in hidden_rec], axis=0))
        held = None
        before = ga_own
        for i in range(CHUNKS):
            if i == CHUNKS - 1:
                grad_wo = mm("bse,bsd->ed", attn_own, after(grad_out, *held)) + mm("bse,bsd->ed", attn_rec, jnp.concatenate(grad_rec, axis=0))
                before = grad_wo
            ga_rec = mm("bsd,ed->bse", after(grad_rec[i], before), w_o).astype(BF16)
            held = attention_bwd(tp_index, qkv_own, qkv_rec[i], tables, ga_own, ga_rec, i * step, held, groups, group_size)
        gqkv_own, gqkv_rec = held
        grad_wo = lax.psum_scatter(grad_wo, "dp", scatter_dimension=1, tiled=True)

        dn_send = []
        for i in range(CHUNKS):
            dn_send.append(lax.optimization_barrier(mm("bse,de->bsd", gqkv_rec[i * step:(i + 1) * step], w_qkv).astype(BF16)))

        out_far, dn_far = [], []
        out_far.append(exchange(out_send[0]))
        for i in range(batch):
            dn_far.append(exchange(dn_send[i // step][i % step:i % step + 1]))
        for i in range(step, batch):
            out_far.append(exchange(out_send[1][i - step:i - step + 1]))

        cut = groups // 2 * block
        gqkv_own, gqkv_rec = after((gqkv_own, gqkv_rec), *dn_send)
        late = mm("bsd,bse->de", normed_own, gqkv_own[:, :, cut:]) + mm("bsd,bse->de", normed_rec, gqkv_rec[:, :, cut:])
        place = lax.axis_index("dp").astype(jnp.uint32)
        core, along_x, along_y = place & 1, (place >> 1) & 1, place >> 2

        def halve(values, axis, coordinate, bit):
            theirs = lax.dynamic_index_in_dim(values, coordinate ^ 1, axis, keepdims=False)
            theirs, values = lax.optimization_barrier((theirs, values))
            mine = lax.dynamic_index_in_dim(values, coordinate, axis, keepdims=False)
            return theirs, mine, lax.ppermute(theirs, "dp", [(i, i ^ bit) for i in range(8)])

        late = late.reshape(2, 2, 2, rows_loc, cut)
        sent, mine, far = halve(late, 2, core, 1)
        gqkv_own, gqkv_rec = after((gqkv_own, gqkv_rec), sent)
        early = mm("bsd,bse->de", normed_own, gqkv_own[:, :, :cut]) + mm("bsd,bse->de", normed_rec, gqkv_rec[:, :, :cut])
        early_sum = lax.psum_scatter(early, "dp", scatter_dimension=0, tiled=True)
        late = mine + after(far, early)
        sent_x, mine_x, far_x = halve(late[..., :block], 1, along_x, 2)
        sent_y, mine_y, far_y = halve(late[..., block:], 0, along_y, 4)

        attn_own, gqkv_own = after((attn_own, gqkv_own), sent_x, sent_y)
        out_near = lax.optimization_barrier(mm("bse,ed->bsd", attn_own, w_o).astype(BF16))
        dn_near = lax.optimization_barrier(mm("bse,de->bsd", gqkv_own, w_qkv).astype(BF16))
        hidden_out = finish(finish_out_kernel, [hidden, out_near], [out_far[0]], 0, None)
        sent_xy, mine_xy, far_xy = halve(mine_x + after(far_x, hidden_out), 0, along_y, 4)
        sent_yx, mine_yx, far_yx = halve(mine_y + after(far_y, hidden_out), 0, along_x, 2)
        dn_near = after(dn_near, sent_xy, sent_yx)
        grad_hidden = None
        gain_parts = []
        for i in range(batch):
            grad_hidden, part = finish(
                finish_grad_kernel, [hidden, grad_out, dn_near], [dn_far[i]], i, grad_hidden, gain
            )
            gain_parts.append(part)
        gain_sum = lax.psum(jnp.sum(sum(gain_parts), axis=0), ("dp", "tp"))
        grad_gain = lax.dynamic_slice(gain_sum, (lax.axis_index("dp") * rows_loc,), (rows_loc,))
        for i in range(step, batch):
            hidden_out = finish(finish_out_kernel, [hidden, out_near], [after(out_far[i - step + 1], gain_sum, hidden_out)], i, hidden_out)
        grad_wq, grad_wk, grad_wv = ungroup(early_sum, (mine_xy, far_xy), (mine_yx, far_yx), groups)
        return hidden_out, grad_hidden, grad_gain, grad_wq, grad_wk, grad_wv, grad_wo

    act_spec = P("dp", "tp", None)
    col_spec = P("dp", "tp")
    row_spec = P("tp", "dp")
    return jax.shard_map(
        local_block,
        mesh=mesh,
        in_specs=(act_spec, P("dp"), col_spec, col_spec, col_spec, row_spec, act_spec),
        out_specs=(act_spec, act_spec, P("dp"), col_spec, col_spec, col_spec, row_spec),
        check_vma=False,
    )
```

```python
import functools

import jax
import jax.numpy as jnp
from jax import lax
from jax.experimental import pallas as pl
from jax.experimental.pallas import tpu as pltpu
from jax.sharding import PartitionSpec as P


HEAD_DIM = 128
NORM_EPS = 1e-5
ROPE_BASE = 500000.0
SCORE_SCALE = HEAD_DIM ** -0.5
MASK_VALUE = -1e30
F32 = jnp.float32
BF16 = jnp.bfloat16
NT = (((1,), (1,)), ((), ()))
NN = (((1,), (0,)), ((), ()))
TN = (((0,), (0,)), ((), ()))


def rope_tables(seq_len):
    half_dim = HEAD_DIM // 2
    inv_freq = ROPE_BASE ** (-jnp.arange(half_dim, dtype=F32) * 2.0 / HEAD_DIM)
    angles = jnp.arange(seq_len, dtype=F32)[:, None] * inv_freq[None, :]
    cos_t, sin_t = jnp.cos(angles), jnp.sin(angles)
    return jnp.concatenate([cos_t, cos_t], axis=1), jnp.concatenate([-sin_t, sin_t], axis=1)


def dot(lhs, rhs, dims):
    return lax.dot_general(lhs, rhs, dims, preferred_element_type=F32)


def turn(values, cos_t, sin_t):
    return values * cos_t + pltpu.roll(values, HEAD_DIM // 2, 1) * sin_t


def pick_halves(first, own, rec):
    own, rec = own.astype(F32), rec.astype(F32)
    return jnp.where(first, own, rec), jnp.where(first, rec, own)


def heads_of(group_size, block, cos_t, sin_t):
    cut = [block[:, i * HEAD_DIM:(i + 1) * HEAD_DIM] for i in range(group_size + 2)]
    queries = jnp.concatenate([turn(cut[i], cos_t, sin_t).astype(BF16) for i in range(group_size)], axis=0)
    return queries, turn(cut[group_size], cos_t, sin_t).astype(BF16), cut[group_size + 1].astype(BF16)


def store_halves(first, own_ref, rec_ref, columns, lower, upper):
    own_ref[0, :, columns] = jnp.where(first, lower, upper).astype(own_ref.dtype)
    rec_ref[0, :, columns] = jnp.where(first, upper, lower).astype(rec_ref.dtype)


def attention_fwd_kernel(group_size, tp_ref, own_ref, rec_ref, cos_ref, sin_ref, *rest):
    out_own_ref, out_rec_ref = rest[-2:]
    half = own_ref.shape[1]
    first = tp_ref[0] == 0
    lower, upper = pick_halves(first, own_ref[0], rec_ref[0])
    q_lo, k_lo, v_lo = heads_of(group_size, lower, cos_ref[:half], sin_ref[:half])
    q_up, k_up, v_up = heads_of(group_size, upper, cos_ref[half:], sin_ref[half:])
    rows = lax.broadcasted_iota(jnp.int32, (group_size, half, half), 1).reshape(group_size * half, half)
    cols = lax.broadcasted_iota(jnp.int32, (group_size * half, half), 1)
    causal = rows >= cols

    s_lo = jnp.where(causal, dot(q_lo, k_lo, NT), MASK_VALUE)
    p_lo = jnp.exp((s_lo - jnp.max(s_lo, axis=1, keepdims=True)) * SCORE_SCALE)
    p_lo = (p_lo * (1.0 / jnp.sum(p_lo, axis=1, keepdims=True))).astype(BF16)
    a_lo = dot(p_lo, v_lo, NN)

    s_a = dot(q_up, k_lo, NT)
    s_b = jnp.where(causal, dot(q_up, k_up, NT), MASK_VALUE)
    top = jnp.maximum(jnp.max(s_a, axis=1, keepdims=True), jnp.max(s_b, axis=1, keepdims=True))
    p_a = jnp.exp((s_a - top) * SCORE_SCALE)
    p_b = jnp.exp((s_b - top) * SCORE_SCALE)
    inv = 1.0 / (jnp.sum(p_a, axis=1, keepdims=True) + jnp.sum(p_b, axis=1, keepdims=True))
    a_up = dot((p_a * inv).astype(BF16), v_lo, NN) + dot((p_b * inv).astype(BF16), v_up, NN)
    for i in range(group_size):
        part = slice(i * half, (i + 1) * half)
        store_halves(first, out_own_ref, out_rec_ref, slice(i * HEAD_DIM, (i + 1) * HEAD_DIM), a_lo[part], a_up[part])


def attention_bwd_kernel(group_size, tp_ref, own_ref, rec_ref, cos_ref, sin_ref, ga_own_ref, ga_rec_ref, *rest):
    out_ref = rest[-1]
    half = own_ref.shape[1]
    first = tp_ref[0] == 0
    lower, upper = pick_halves(first, own_ref[0], rec_ref[0])
    cos_lo, sin_lo, cos_up, sin_up = cos_ref[:half], sin_ref[:half], cos_ref[half:], sin_ref[half:]
    q_lo, k_lo, v_lo = heads_of(group_size, lower, cos_lo, sin_lo)
    q_up, k_up, v_up = heads_of(group_size, upper, cos_up, sin_up)
    ga_lower, ga_upper = pick_halves(first, ga_own_ref[0], ga_rec_ref[0])

    def stacked(block):
        return jnp.concatenate([block[:, i * HEAD_DIM:(i + 1) * HEAD_DIM].astype(BF16) for i in range(group_size)], axis=0)

    ga_lo, ga_up = stacked(ga_lower), stacked(ga_upper)
    keys = lax.broadcasted_iota(jnp.int32, (half, half), 0)
    spots = lax.broadcasted_iota(jnp.int32, (half, half), 1)
    causal = jnp.concatenate([spots >= keys] * group_size, axis=1)

    s_lo = jnp.where(causal, dot(k_lo, q_lo, NT), MASK_VALUE)
    p_lo = jnp.exp((s_lo - jnp.max(s_lo, axis=0, keepdims=True)) * SCORE_SCALE)
    p_lo = p_lo * (1.0 / jnp.sum(p_lo, axis=0, keepdims=True))
    gp_lo = dot(v_lo, ga_lo, NT).astype(BF16).astype(F32)
    gs_lo = (p_lo * (gp_lo - jnp.sum(gp_lo * p_lo, axis=0, keepdims=True)) * SCORE_SCALE).astype(BF16)

    s_a = dot(k_lo, q_up, NT)
    s_b = jnp.where(causal, dot(k_up, q_up, NT), MASK_VALUE)
    top = jnp.maximum(jnp.max(s_a, axis=0, keepdims=True), jnp.max(s_b, axis=0, keepdims=True))
    p_a = jnp.exp((s_a - top) * SCORE_SCALE)
    p_b = jnp.exp((s_b - top) * SCORE_SCALE)
    inv = 1.0 / (jnp.sum(p_a, axis=0, keepdims=True) + jnp.sum(p_b, axis=0, keepdims=True))
    p_a = p_a * inv
    p_b = p_b * inv
    gp_a = dot(v_lo, ga_up, NT).astype(BF16).astype(F32)
    gp_b = dot(v_up, ga_up, NT).astype(BF16).astype(F32)
    mean_up = jnp.sum(gp_a * p_a, axis=0, keepdims=True) + jnp.sum(gp_b * p_b, axis=0, keepdims=True)
    gs_a = (p_a * (gp_a - mean_up) * SCORE_SCALE).astype(BF16)
    gs_b = (p_b * (gp_b - mean_up) * SCORE_SCALE).astype(BF16)

    gv_lo = dot(p_lo.astype(BF16), ga_lo, NN) + dot(p_a.astype(BF16), ga_up, NN)
    gv_up = dot(p_b.astype(BF16), ga_up, NN)
    gk_lo = (dot(gs_lo, q_lo, NN) + dot(gs_a, q_up, NN)).astype(BF16).astype(F32)
    gk_up = dot(gs_b, q_up, NN).astype(BF16).astype(F32)
    gq_lo = dot(gs_lo, k_lo, TN).astype(BF16).astype(F32)
    gq_up = (dot(gs_a, k_lo, TN) + dot(gs_b, k_up, TN)).astype(BF16).astype(F32)

    def store(index, lower_part, upper_part):
        store_halves(first, out_ref.at[0], out_ref.at[1], slice(index * HEAD_DIM, (index + 1) * HEAD_DIM), lower_part, upper_part)

    for i in range(group_size):
        part = slice(i * half, (i + 1) * half)
        store(i, turn(gq_lo[part], cos_lo, -sin_lo), turn(gq_up[part], cos_up, -sin_up))
    store(group_size, turn(gk_lo, cos_lo, -sin_lo), turn(gk_up, cos_up, -sin_up))
    store(group_size + 1, gv_lo, gv_up)


def cost(flops, transcendentals, *arrays):
    return pl.CostEstimate(flops=int(flops), transcendentals=int(transcendentals), bytes_accessed=int(sum(a.size * a.dtype.itemsize for a in arrays)))


def attention_fwd(tp_index, qkv_own, qkv_rec, tables, start, held, groups, group_size):
    batch, half, width = qkv_own.shape
    count = qkv_rec.shape[0]
    block = width // groups
    out_block = group_size * HEAD_DIM
    shape = jax.ShapeDtypeStruct((batch, half, groups * out_block), BF16)
    spec = lambda columns, offset: pl.BlockSpec((1, half, columns), lambda b, g, tp: (b + offset, 0, g))
    table = pl.BlockSpec((2 * half, HEAD_DIM), lambda b, g, tp: (0, 0))
    in_specs = [spec(block, start), spec(block, 0), table, table]
    args = [tp_index, qkv_own, qkv_rec, *tables]
    aliases = {}
    if held is not None:
        in_specs += [pl.BlockSpec(memory_space=pl.ANY)] * 2
        aliases = {len(args): 0, len(args) + 1: 1}
        args += list(held)
    work = count * groups * group_size * half * half
    return pl.pallas_call(
        functools.partial(attention_fwd_kernel, group_size),
        out_shape=(shape, shape),
        grid_spec=pltpu.PrefetchScalarGridSpec(
            num_scalar_prefetch=1,
            grid=(count, groups),
            in_specs=in_specs,
            out_specs=(spec(out_block, start), spec(out_block, start)),
        ),
        input_output_aliases=aliases,
        compiler_params=pltpu.CompilerParams(vmem_limit_bytes=48 * 2**20),
        cost_estimate=cost(work * HEAD_DIM * 12, work * 3, qkv_rec, qkv_rec),
        name="attention_fwd",
    )(*args)


def attention_bwd(tp_index, qkv_own, qkv_rec, tables, ga_own, ga_rec, start, rec_start, held, groups, group_size):
    batch, half, width = qkv_own.shape
    count = ga_rec.shape[0]
    block = width // groups
    ga_block = group_size * HEAD_DIM
    shape = jax.ShapeDtypeStruct((2, batch, half, width), BF16)
    spec = lambda columns, offset: pl.BlockSpec((1, half, columns), lambda b, g, tp: (b + offset, 0, g))
    table = pl.BlockSpec((2 * half, HEAD_DIM), lambda b, g, tp: (0, 0))
    in_specs = [spec(block, start), spec(block, rec_start), table, table, spec(ga_block, start), spec(ga_block, 0)]
    args = [tp_index, qkv_own, qkv_rec, *tables, ga_own, ga_rec]
    aliases = {}
    if held is not None:
        in_specs.append(pl.BlockSpec(memory_space=pl.ANY))
        aliases = {len(args): 0}
        args.append(held)
    work = count * groups * group_size * half * half
    return pl.pallas_call(
        functools.partial(attention_bwd_kernel, group_size),
        out_shape=shape,
        grid_spec=pltpu.PrefetchScalarGridSpec(
            num_scalar_prefetch=1,
            grid=(count, groups),
            in_specs=in_specs,
            out_specs=pl.BlockSpec((2, 1, half, block), lambda b, g, tp: (0, b + start, 0, g)),
        ),
        input_output_aliases=aliases,
        compiler_params=pltpu.CompilerParams(vmem_limit_bytes=48 * 2**20),
        cost_estimate=cost(work * HEAD_DIM * 30, work * 3, ga_rec, ga_rec, ga_rec, ga_rec),
        name="attention_bwd",
    )(*args)


def split_norm_kernel(core_ref, gain_ref, own_ref, rec_a_ref, rec_b_ref, mine_ref, sent_ref):
    kind, batch_index = pl.program_id(0), pl.program_id(1)
    half_batch = pl.num_programs(1) // 2
    first = core_ref[0] == 0

    def put(source):
        values = source[0].astype(F32)
        inv_rms = lax.rsqrt(jnp.mean(values * values, axis=-1, keepdims=True) + NORM_EPS)
        normed = values * inv_rms * gain_ref[...]
        rows = normed.shape[1] // 8
        for i in range(4):
            even = normed[:, 2 * i * rows:(2 * i + 1) * rows]
            odd = normed[:, (2 * i + 1) * rows:(2 * i + 2) * rows]
            mine_ref[0, 0, :, i * rows:(i + 1) * rows] = jnp.where(first, even, odd).astype(BF16)
            sent_ref[0, 0, :, i * rows:(i + 1) * rows] = jnp.where(first, odd, even).astype(BF16)

    @pl.when(kind == 0)
    def _():
        put(own_ref)

    @pl.when((kind == 1) & (batch_index < half_batch))
    def _():
        put(rec_a_ref)

    @pl.when((kind == 1) & (batch_index >= half_batch))
    def _():
        put(rec_b_ref)


def split_norm(core_index, gain, own, rec_a, rec_b, row_block=128):
    batch, half, width = own.shape
    part = batch // 2
    row_block = min(row_block, half)
    last = half // row_block - 1
    out = jax.ShapeDtypeStruct((2, batch, half, width // 2), BF16)
    block = (1, row_block, width)
    own_spec = pl.BlockSpec(block, lambda k, b, r, c: (jnp.where(k == 0, b, batch - 1), jnp.where(k == 0, r, last), 0))
    a_spec = pl.BlockSpec(block, lambda k, b, r, c: (jnp.where(k == 0, 0, jnp.minimum(b, part - 1)), jnp.where(k == 0, 0, jnp.where(b < part, r, last)), 0))
    b_spec = pl.BlockSpec(block, lambda k, b, r, c: (jnp.where(k == 0, 0, jnp.maximum(b - part, 0)), jnp.where(k == 0, 0, jnp.where(b < part, 0, r)), 0))
    out_spec = pl.BlockSpec((1, 1, row_block, width // 2), lambda k, b, r, c: (k, b, r, 0))
    return pl.pallas_call(
        split_norm_kernel,
        out_shape=(out, out),
        grid_spec=pltpu.PrefetchScalarGridSpec(
            num_scalar_prefetch=1,
            grid=(2, batch, half // row_block),
            in_specs=[pl.BlockSpec((1, width), lambda k, b, r, c: (0, 0)), own_spec, a_spec, b_spec],
            out_specs=(out_spec, out_spec),
        ),
        compiler_params=pltpu.CompilerParams(vmem_limit_bytes=40 * 2**20),
        cost_estimate=cost(2 * batch * half * width * 400, 0, own, own, own, own),
        name="split_norm",
    )(core_index, gain.reshape(1, width), own, rec_a, rec_b)


def finish_out_kernel(x_ref, near_ref, far_ref, *rest):
    out_sum = (near_ref[0].astype(F32) + far_ref[0].astype(F32)).astype(BF16).astype(F32)
    rest[-1][0] = (x_ref[0].astype(F32) + out_sum).astype(BF16)


def finish_grad_kernel(x_ref, dy_ref, near_ref, gain_ref, far_ref, *rest):
    out_ref, gain_out_ref = rest[-2:]
    values = x_ref[0].astype(F32)
    inv_rms = lax.rsqrt(jnp.mean(values * values, axis=-1, keepdims=True) + NORM_EPS)
    x_hat = values * inv_rms
    grad_normed = (near_ref[0].astype(F32) + far_ref[0].astype(F32)).astype(BF16).astype(F32)
    scaled = grad_normed * gain_ref[...]
    mean = jnp.mean(scaled * x_hat, axis=-1, keepdims=True)
    out_ref[0] = (dy_ref[0].astype(F32) + inv_rms * (scaled - x_hat * mean)).astype(BF16)

    @pl.when((pl.program_id(0) == 0) & (pl.program_id(1) == 0))
    def _():
        gain_out_ref[...] = jnp.zeros_like(gain_out_ref)

    gain_out_ref[...] += jnp.sum((grad_normed * x_hat).reshape(-1, 8, x_hat.shape[-1]), axis=0)


def finish(kernel, full, chunk, start, held, gain=None, row_block=64):
    batch, half, width = full[0].shape
    count = chunk[0].shape[0]
    row_block = min(row_block, half)
    spec = lambda offset: pl.BlockSpec((1, row_block, width), lambda b, r: (b + offset, r, 0))
    in_specs = [spec(start)] * len(full)
    args = list(full)
    out_shape = [jax.ShapeDtypeStruct((batch, half, width), BF16)]
    out_specs = [spec(start)]
    if gain is not None:
        in_specs.append(pl.BlockSpec((1, width), lambda b, r: (0, 0)))
        args.append(gain.reshape(1, width))
        out_shape.append(jax.ShapeDtypeStruct((8, width), F32))
        out_specs.append(pl.BlockSpec((8, width), lambda b, r: (0, 0)))
    in_specs += [spec(0)] * len(chunk)
    args += list(chunk)
    aliases = {}
    if held is not None:
        aliases = {len(args): 0}
        in_specs.append(pl.BlockSpec(memory_space=pl.ANY))
        args.append(held)
    result = pl.pallas_call(
        kernel,
        out_shape=out_shape,
        grid=(count, half // row_block),
        in_specs=in_specs,
        out_specs=out_specs,
        input_output_aliases=aliases,
        compiler_params=pltpu.CompilerParams(vmem_limit_bytes=32 * 2**20),
        cost_estimate=cost(count * half * width * 400, 0, *([chunk[0]] * (len(full) + len(chunk) + 1))),
    )(*args)
    return result if gain is not None else result[0]


def regroup_kernel(q_ref, k_ref, v_ref, out_ref):
    split = q_ref.shape[1]
    out_ref[:, :split] = q_ref[...]
    out_ref[:, split:split + HEAD_DIM] = k_ref[...]
    out_ref[:, split + HEAD_DIM:] = v_ref[...]


def regroup(w_query, w_key, w_value):
    rows = w_query.shape[0]
    groups = w_key.shape[1] // HEAD_DIM
    split = w_query.shape[1] // groups
    spec = lambda columns: pl.BlockSpec((rows, columns), lambda g: (0, g))
    out = jax.ShapeDtypeStruct((rows, groups * (split + 2 * HEAD_DIM)), w_query.dtype)
    return pl.pallas_call(
        regroup_kernel,
        out_shape=out,
        grid=(groups,),
        in_specs=[spec(split), spec(HEAD_DIM), spec(HEAD_DIM)],
        out_specs=spec(split + 2 * HEAD_DIM),
        cost_estimate=cost(rows * out.shape[1] * 400, 0, out, out),
        name="regroup",
    )(w_query, w_key, w_value)


def ungroup_kernel(*refs):
    q_ref, k_ref, v_ref = refs[-3:]
    split = q_ref.shape[1]
    for group in range(len(refs) // 2 - 1):

        @pl.when(pl.program_id(1) == group)
        def _(group=group):
            block = refs[2 * group][...] + refs[2 * group + 1][...]
            q_ref[...] = block[:, :split]
            k_ref[...] = block[:, split:split + HEAD_DIM]
            v_ref[...] = block[:, split + HEAD_DIM:]


def ungroup(terms, row_block=96):
    groups = len(terms)
    rows, block = terms[0][0].shape
    split = block - 2 * HEAD_DIM
    row_block = min(row_block, rows)
    spec = lambda columns: pl.BlockSpec((row_block, columns), lambda r, g: (r, g))
    shape = lambda columns: jax.ShapeDtypeStruct((rows, groups * columns), F32)
    flat = [term for pair in terms for term in pair]
    return pl.pallas_call(
        ungroup_kernel,
        out_shape=(shape(split), shape(HEAD_DIM), shape(HEAD_DIM)),
        grid=(rows // row_block, groups),
        in_specs=[pl.BlockSpec((row_block, block), lambda r, g: (r, 0))] * len(flat),
        out_specs=(spec(split), spec(HEAD_DIM), spec(HEAD_DIM)),
        compiler_params=pltpu.CompilerParams(vmem_limit_bytes=32 * 2**20),
        cost_estimate=cost(rows * block * groups * 400, 0, *flat, *flat[:groups]),
        name="ungroup",
    )(*flat)


CHUNKS = 2


def after(value, *others):
    return lax.optimization_barrier((value, *others))[0]


def solution(mesh):
    swap = [(0, 1), (1, 0)]

    def exchange(values):
        return lax.ppermute(values, "tp", swap)

    def mm(eq, a, b):
        return jnp.einsum(eq, a, b, preferred_element_type=F32)

    def local_block(hidden, norm_gain, w_query, w_key, w_value, w_out, grad_out):
        batch, half, _ = hidden.shape
        rows_loc = w_query.shape[0]
        groups = w_key.shape[1] // HEAD_DIM
        group_size = w_query.shape[1] // w_key.shape[1]
        block = (group_size + 2) * HEAD_DIM
        tp_index = lax.axis_index("tp").astype(jnp.int32).reshape(1)
        tables = rope_tables(2 * half)

        step = batch // CHUNKS
        hidden_rec, grad_rec = [], []
        source = hidden
        for i in range(CHUNKS):
            piece = lax.optimization_barrier(source[i * step:(i + 1) * step])
            source = after(hidden, piece)
            hidden_rec.append(exchange(piece))
        pieces = [(0, 2), (2, 1), (3, 1)]
        for start, count in pieces:
            grad_rec.append(exchange(grad_out[start:start + count]))

        w_qkv = regroup(w_query, w_key, w_value)
        w_qkv = lax.all_gather(w_qkv, "dp", axis=0, tiled=True)
        w_o = lax.all_gather(w_out, "dp", axis=1, tiled=True)
        gain = lax.all_gather(norm_gain, "dp", axis=0, tiled=True).astype(F32)

        def norm(values):
            values = values.astype(F32)
            inv_rms = lax.rsqrt(jnp.mean(values * values, axis=-1, keepdims=True) + NORM_EPS)
            return (values * inv_rms * gain).astype(BF16)

        normed_own = norm(hidden)
        qkv_own = mm("bsd,de->bse", normed_own, w_qkv).astype(BF16)
        qkv_rec = []
        attn = None
        before = qkv_own
        for i in range(CHUNKS):
            rec = norm(after(hidden_rec[i], before))
            qkv_rec.append(mm("bsd,de->bse", rec, w_qkv).astype(BF16))
            attn = attention_fwd(tp_index, qkv_own, qkv_rec[i], tables, i * step, attn, groups, group_size)
            before = attn[0]
        attn_own, attn_rec = attn

        out_send = []
        for i in range(CHUNKS):
            out_send.append(lax.optimization_barrier(mm("bse,ed->bsd", attn_rec[i * step:(i + 1) * step], w_o).astype(BF16)))

        ga_own = mm("bsd,ed->bse", after(grad_out, *out_send), w_o).astype(BF16)
        place = lax.axis_index("dp").astype(jnp.uint32)
        core, along_x, along_y = place & 1, (place >> 1) & 1, place >> 2
        core_index = core.astype(jnp.int32).reshape(1)
        normed_mine, normed_sent = split_norm(core_index, gain, hidden, hidden_rec[0], after(hidden_rec[1], ga_own))

        gqkv = None
        before = ga_own
        for i, (start, count) in enumerate(pieces):
            if i == len(pieces) - 1:
                grad_wo = mm("bse,bsd->ed", attn_own, after(grad_out, gqkv)) + mm("bse,bsd->ed", attn_rec, jnp.concatenate(grad_rec, axis=0))
                before = grad_wo
            ga_rec = mm("bsd,ed->bse", after(grad_rec[i], before), w_o).astype(BF16)
            gqkv = attention_bwd(tp_index, qkv_own, qkv_rec[start // step], tables, ga_own, ga_rec, start, start % step, gqkv, groups, group_size)
            before = gqkv
        grad_wo = lax.psum_scatter(grad_wo, "dp", scatter_dimension=1, tiled=True)

        cut = groups // 2 * block

        def pick(values, axis, coordinate, columns=0):
            at = [jnp.uint32(0)] * values.ndim
            at[axis], at[-1] = coordinate, jnp.uint32(columns)
            size = [*values.shape[:-1], block]
            size[axis] = 1
            return lax.squeeze(lax.dynamic_slice(values, at, size), [axis])

        def pass_on(values, bit):
            return lax.ppermute(values, "dp", [(i, i ^ bit) for i in range(8)])

        def weight_grad(normed, columns, before):
            return mm("hbsd,hbse->de", normed, after(gqkv, *before)[..., columns])

        late, early = slice(cut, 2 * cut), slice(0, cut)
        late_sent = weight_grad(normed_sent, late, [])
        late_far = pass_on(late_sent, 1)
        early_sent = weight_grad(normed_sent, early, [late_sent])
        early_far = pass_on(early_sent, 1)

        def first_stage(mine, far):
            total = (mine + far).reshape(2, 2, rows_loc, cut)
            sent = pick(total, 1, along_x ^ 1), pick(total, 0, along_y ^ 1, block)
            sent, total = lax.optimization_barrier((sent, total))
            mine = pick(total, 1, along_x), pick(total, 0, along_y, block)
            return sent, mine, (pass_on(sent[0], 2), pass_on(sent[1], 4))

        def second_stage(mine, far, before):
            far = after(far, *before)
            total = mine[0] + far[0], mine[1] + far[1]
            sent = pick(total[0], 0, along_y ^ 1), pick(total[1], 0, along_x ^ 1)
            sent, total = lax.optimization_barrier((sent, total))
            mine = pick(total[0], 0, along_y), pick(total[1], 0, along_x)
            return sent, [(mine[0], pass_on(sent[0], 4)), (mine[1], pass_on(sent[1], 2))]

        late_sent, late_mine, late_far = first_stage(weight_grad(normed_mine, late, [early_sent]), late_far)
        early_sent, early_mine, early_far = first_stage(weight_grad(normed_mine, early, late_sent), early_far)

        gqkv_rec = after(gqkv, *early_sent)[1]
        dn_send = []
        for i in range(CHUNKS):
            dn_send.append(lax.optimization_barrier(mm("bse,de->bsd", gqkv_rec[i * step:(i + 1) * step], w_qkv).astype(BF16)))

        out_far, dn_far = [], []
        out_far.append(exchange(out_send[0]))
        out_far.append(exchange(out_send[1][:1]))
        out_far.append(exchange(out_send[1][1:]))
        dn_sent = [dn_send[0], dn_send[1][:1], dn_send[1][1:]]
        for i in range(3):
            dn_far.append(exchange(dn_sent[i]))

        attn_own, gqkv = after((attn_own, gqkv), *dn_send)
        out_near = lax.optimization_barrier(mm("bse,ed->bsd", attn_own, w_o).astype(BF16))
        dn_near = lax.optimization_barrier(mm("bse,de->bsd", gqkv[0], w_qkv).astype(BF16))
        late_sent, late_terms = second_stage(late_mine, late_far, [out_near, dn_near])
        hidden_out = finish(finish_out_kernel, [hidden, after(out_near, *late_sent)], [out_far[0]], 0, None)
        hidden_out = finish(finish_out_kernel, [hidden, out_near], [after(out_far[1], hidden_out)], 2, hidden_out)
        early_sent, early_terms = second_stage(early_mine, early_far, [hidden_out])
        dn_near = after(dn_near, *early_sent)
        grad_hidden = None
        gain_parts = []
        for i, (start, count) in enumerate(pieces):
            grad_hidden, part = finish(
                finish_grad_kernel, [hidden, grad_out, dn_near], [dn_far[i]], start, grad_hidden, gain
            )
            gain_parts.append(part)
        gain_sum = lax.psum(jnp.sum(sum(gain_parts), axis=0), ("dp", "tp"))
        grad_gain = lax.dynamic_slice(gain_sum, (lax.axis_index("dp") * rows_loc,), (rows_loc,))
        grad_wq, grad_wk, grad_wv = w_grads = ungroup([(mine, after(far, gain_sum)) for mine, far in early_terms + late_terms])
        hidden_out = finish(finish_out_kernel, [hidden, out_near], [after(out_far[2], *w_grads)], 3, hidden_out)
        return hidden_out, grad_hidden, grad_gain, grad_wq, grad_wk, grad_wv, grad_wo

    act_spec = P("dp", "tp", None)
    col_spec = P("dp", "tp")
    row_spec = P("tp", "dp")
    return jax.shard_map(
        local_block,
        mesh=mesh,
        in_specs=(act_spec, P("dp"), col_spec, col_spec, col_spec, row_spec, act_spec),
        out_specs=(act_spec, act_spec, P("dp"), col_spec, col_spec, col_spec, row_spec),
        check_vma=False,
    )
```

```python
import functools

import jax
import jax.numpy as jnp
from jax import lax
from jax.experimental import pallas as pl
from jax.experimental.pallas import tpu as pltpu
from jax.sharding import PartitionSpec as P


HEAD_DIM = 128
NORM_EPS = 1e-5
ROPE_BASE = 500000.0
SCORE_SCALE = HEAD_DIM ** -0.5
MASK_VALUE = -1e30
F32 = jnp.float32
BF16 = jnp.bfloat16
NT = (((1,), (1,)), ((), ()))
NN = (((1,), (0,)), ((), ()))
TN = (((0,), (0,)), ((), ()))


def rope_tables(seq_len):
    half_dim = HEAD_DIM // 2
    inv_freq = ROPE_BASE ** (-jnp.arange(half_dim, dtype=F32) * 2.0 / HEAD_DIM)
    angles = jnp.arange(seq_len, dtype=F32)[:, None] * inv_freq[None, :]
    cos_t, sin_t = jnp.cos(angles), jnp.sin(angles)
    return jnp.concatenate([cos_t, cos_t], axis=1), jnp.concatenate([-sin_t, sin_t], axis=1)


def dot(lhs, rhs, dims):
    return lax.dot_general(lhs, rhs, dims, preferred_element_type=F32)


def turn(values, cos_t, sin_t):
    return values * cos_t + pltpu.roll(values, HEAD_DIM // 2, 1) * sin_t


def pick_halves(first, own, rec):
    own, rec = own.astype(F32), rec.astype(F32)
    return jnp.where(first, own, rec), jnp.where(first, rec, own)


def heads_of(group_size, block, cos_t, sin_t):
    cut = [block[:, i * HEAD_DIM:(i + 1) * HEAD_DIM] for i in range(group_size + 2)]
    queries = jnp.concatenate([turn(cut[i], cos_t, sin_t).astype(BF16) for i in range(group_size)], axis=0)
    return queries, turn(cut[group_size], cos_t, sin_t).astype(BF16), cut[group_size + 1].astype(BF16)


def store_halves(first, own_ref, rec_ref, columns, lower, upper):
    own_ref[0, :, columns] = jnp.where(first, lower, upper).astype(own_ref.dtype)
    rec_ref[0, :, columns] = jnp.where(first, upper, lower).astype(rec_ref.dtype)


def attention_fwd_kernel(group_size, tp_ref, own_ref, rec_ref, cos_ref, sin_ref, *rest):
    out_own_ref, out_rec_ref = rest[-2:]
    half = own_ref.shape[1]
    first = tp_ref[0] == 0
    lower, upper = pick_halves(first, own_ref[0], rec_ref[0])
    q_lo, k_lo, v_lo = heads_of(group_size, lower, cos_ref[:half], sin_ref[:half])
    q_up, k_up, v_up = heads_of(group_size, upper, cos_ref[half:], sin_ref[half:])
    rows = lax.broadcasted_iota(jnp.int32, (group_size, half, half), 1).reshape(group_size * half, half)
    cols = lax.broadcasted_iota(jnp.int32, (group_size * half, half), 1)
    causal = rows >= cols

    s_lo = jnp.where(causal, dot(q_lo, k_lo, NT), MASK_VALUE)
    p_lo = jnp.exp((s_lo - jnp.max(s_lo, axis=1, keepdims=True)) * SCORE_SCALE)
    p_lo = (p_lo * (1.0 / jnp.sum(p_lo, axis=1, keepdims=True))).astype(BF16)
    a_lo = dot(p_lo, v_lo, NN)

    s_a = dot(q_up, k_lo, NT)
    s_b = jnp.where(causal, dot(q_up, k_up, NT), MASK_VALUE)
    top = jnp.maximum(jnp.max(s_a, axis=1, keepdims=True), jnp.max(s_b, axis=1, keepdims=True))
    p_a = jnp.exp((s_a - top) * SCORE_SCALE)
    p_b = jnp.exp((s_b - top) * SCORE_SCALE)
    inv = 1.0 / (jnp.sum(p_a, axis=1, keepdims=True) + jnp.sum(p_b, axis=1, keepdims=True))
    a_up = dot((p_a * inv).astype(BF16), v_lo, NN) + dot((p_b * inv).astype(BF16), v_up, NN)
    for i in range(group_size):
        part = slice(i * half, (i + 1) * half)
        store_halves(first, out_own_ref, out_rec_ref, slice(i * HEAD_DIM, (i + 1) * HEAD_DIM), a_lo[part], a_up[part])


def attention_bwd_kernel(group_size, tp_ref, own_ref, rec_ref, cos_ref, sin_ref, ga_own_ref, ga_rec_ref, *rest):
    out_ref = rest[-1]
    half = own_ref.shape[1]
    first = tp_ref[0] == 0
    lower, upper = pick_halves(first, own_ref[0], rec_ref[0])
    cos_lo, sin_lo, cos_up, sin_up = cos_ref[:half], sin_ref[:half], cos_ref[half:], sin_ref[half:]
    q_lo, k_lo, v_lo = heads_of(group_size, lower, cos_lo, sin_lo)
    q_up, k_up, v_up = heads_of(group_size, upper, cos_up, sin_up)
    ga_lower, ga_upper = pick_halves(first, ga_own_ref[0], ga_rec_ref[0])

    def stacked(block):
        return jnp.concatenate([block[:, i * HEAD_DIM:(i + 1) * HEAD_DIM].astype(BF16) for i in range(group_size)], axis=0)

    ga_lo, ga_up = stacked(ga_lower), stacked(ga_upper)
    keys = lax.broadcasted_iota(jnp.int32, (half, half), 0)
    spots = lax.broadcasted_iota(jnp.int32, (half, half), 1)
    causal = jnp.concatenate([spots >= keys] * group_size, axis=1)

    s_lo = jnp.where(causal, dot(k_lo, q_lo, NT), MASK_VALUE)
    p_lo = jnp.exp((s_lo - jnp.max(s_lo, axis=0, keepdims=True)) * SCORE_SCALE)
    p_lo = p_lo * (1.0 / jnp.sum(p_lo, axis=0, keepdims=True))
    gp_lo = dot(v_lo, ga_lo, NT).astype(BF16).astype(F32)
    gs_lo = (p_lo * (gp_lo - jnp.sum(gp_lo * p_lo, axis=0, keepdims=True)) * SCORE_SCALE).astype(BF16)

    s_a = dot(k_lo, q_up, NT)
    s_b = jnp.where(causal, dot(k_up, q_up, NT), MASK_VALUE)
    top = jnp.maximum(jnp.max(s_a, axis=0, keepdims=True), jnp.max(s_b, axis=0, keepdims=True))
    p_a = jnp.exp((s_a - top) * SCORE_SCALE)
    p_b = jnp.exp((s_b - top) * SCORE_SCALE)
    inv = 1.0 / (jnp.sum(p_a, axis=0, keepdims=True) + jnp.sum(p_b, axis=0, keepdims=True))
    p_a = p_a * inv
    p_b = p_b * inv
    gp_a = dot(v_lo, ga_up, NT).astype(BF16).astype(F32)
    gp_b = dot(v_up, ga_up, NT).astype(BF16).astype(F32)
    mean_up = jnp.sum(gp_a * p_a, axis=0, keepdims=True) + jnp.sum(gp_b * p_b, axis=0, keepdims=True)
    gs_a = (p_a * (gp_a - mean_up) * SCORE_SCALE).astype(BF16)
    gs_b = (p_b * (gp_b - mean_up) * SCORE_SCALE).astype(BF16)

    gv_lo = dot(p_lo.astype(BF16), ga_lo, NN) + dot(p_a.astype(BF16), ga_up, NN)
    gv_up = dot(p_b.astype(BF16), ga_up, NN)
    gk_lo = (dot(gs_lo, q_lo, NN) + dot(gs_a, q_up, NN)).astype(BF16).astype(F32)
    gk_up = dot(gs_b, q_up, NN).astype(BF16).astype(F32)
    gq_lo = dot(gs_lo, k_lo, TN).astype(BF16).astype(F32)
    gq_up = (dot(gs_a, k_lo, TN) + dot(gs_b, k_up, TN)).astype(BF16).astype(F32)

    def store(index, lower_part, upper_part):
        store_halves(first, out_ref.at[0], out_ref.at[1], slice(index * HEAD_DIM, (index + 1) * HEAD_DIM), lower_part, upper_part)

    for i in range(group_size):
        part = slice(i * half, (i + 1) * half)
        store(i, turn(gq_lo[part], cos_lo, -sin_lo), turn(gq_up[part], cos_up, -sin_up))
    store(group_size, turn(gk_lo, cos_lo, -sin_lo), turn(gk_up, cos_up, -sin_up))
    store(group_size + 1, gv_lo, gv_up)


def cost(flops, transcendentals, *arrays):
    return pl.CostEstimate(flops=int(flops), transcendentals=int(transcendentals), bytes_accessed=int(sum(a.size * a.dtype.itemsize for a in arrays)))


def attention_fwd(tp_index, qkv_own, qkv_rec, tables, start, held, groups, group_size):
    batch, half, width = qkv_own.shape
    count = qkv_rec.shape[0]
    block = width // groups
    out_block = group_size * HEAD_DIM
    shape = jax.ShapeDtypeStruct((batch, half, groups * out_block), BF16)
    spec = lambda columns, offset: pl.BlockSpec((1, half, columns), lambda b, g, tp: (b + offset, 0, g))
    table = pl.BlockSpec((2 * half, HEAD_DIM), lambda b, g, tp: (0, 0))
    in_specs = [spec(block, start), spec(block, 0), table, table]
    args = [tp_index, qkv_own, qkv_rec, *tables]
    aliases = {}
    if held is not None:
        in_specs += [pl.BlockSpec(memory_space=pl.ANY)] * 2
        aliases = {len(args): 0, len(args) + 1: 1}
        args += list(held)
    work = count * groups * group_size * half * half
    return pl.pallas_call(
        functools.partial(attention_fwd_kernel, group_size),
        out_shape=(shape, shape),
        grid_spec=pltpu.PrefetchScalarGridSpec(
            num_scalar_prefetch=1,
            grid=(count, groups),
            in_specs=in_specs,
            out_specs=(spec(out_block, start), spec(out_block, start)),
        ),
        input_output_aliases=aliases,
        compiler_params=pltpu.CompilerParams(vmem_limit_bytes=48 * 2**20),
        cost_estimate=cost(work * HEAD_DIM * 12, work * 3, qkv_rec, qkv_rec),
        name="attention_fwd",
    )(*args)


def attention_bwd(tp_index, qkv_own, qkv_rec, tables, ga_own, ga_rec, start, rec_start, held, groups, group_size):
    batch, half, width = qkv_own.shape
    count = ga_rec.shape[0]
    block = width // groups
    ga_block = group_size * HEAD_DIM
    shape = jax.ShapeDtypeStruct((2, batch, half, width), BF16)
    spec = lambda columns, offset: pl.BlockSpec((1, half, columns), lambda b, g, tp: (b + offset, 0, g))
    table = pl.BlockSpec((2 * half, HEAD_DIM), lambda b, g, tp: (0, 0))
    in_specs = [spec(block, start), spec(block, rec_start), table, table, spec(ga_block, start), spec(ga_block, 0)]
    args = [tp_index, qkv_own, qkv_rec, *tables, ga_own, ga_rec]
    aliases = {}
    if held is not None:
        in_specs.append(pl.BlockSpec(memory_space=pl.ANY))
        aliases = {len(args): 0}
        args.append(held)
    work = count * groups * group_size * half * half
    return pl.pallas_call(
        functools.partial(attention_bwd_kernel, group_size),
        out_shape=shape,
        grid_spec=pltpu.PrefetchScalarGridSpec(
            num_scalar_prefetch=1,
            grid=(count, groups),
            in_specs=in_specs,
            out_specs=pl.BlockSpec((2, 1, half, block), lambda b, g, tp: (0, b + start, 0, g)),
        ),
        input_output_aliases=aliases,
        compiler_params=pltpu.CompilerParams(vmem_limit_bytes=48 * 2**20),
        cost_estimate=cost(work * HEAD_DIM * 30, work * 3, ga_rec, ga_rec, ga_rec, ga_rec),
        name="attention_bwd",
    )(*args)


def split_norm_kernel(core_ref, gain_ref, source_ref, *rest):
    mine_ref, sent_ref = rest[-2:]
    first = core_ref[0] == 0
    values = source_ref[0].astype(F32)
    inv_rms = lax.rsqrt(jnp.mean(values * values, axis=-1, keepdims=True) + NORM_EPS)
    normed = values * inv_rms * gain_ref[...]
    rows = normed.shape[1] // 8
    for i in range(4):
        even = normed[:, 2 * i * rows:(2 * i + 1) * rows]
        odd = normed[:, (2 * i + 1) * rows:(2 * i + 2) * rows]
        mine_ref[0, 0, :, i * rows:(i + 1) * rows] = jnp.where(first, even, odd).astype(BF16)
        sent_ref[0, 0, :, i * rows:(i + 1) * rows] = jnp.where(first, odd, even).astype(BF16)


def split_norm(core_index, gain, source, kind, start, batch, held, row_block=128):
    count, half, width = source.shape
    row_block = min(row_block, half)
    out = jax.ShapeDtypeStruct((2, batch, half, width // 2), BF16)
    out_spec = pl.BlockSpec((1, 1, row_block, width // 2), lambda b, r, c: (kind, b + start, r, 0))
    in_specs = [pl.BlockSpec((1, width), lambda b, r, c: (0, 0)), pl.BlockSpec((1, row_block, width), lambda b, r, c: (b, r, 0))]
    args = [core_index, gain.reshape(1, width), source]
    aliases = {}
    if held is not None:
        in_specs += [pl.BlockSpec(memory_space=pl.ANY)] * 2
        aliases = {len(args): 0, len(args) + 1: 1}
        args += list(held)
    return pl.pallas_call(
        split_norm_kernel,
        out_shape=(out, out),
        grid_spec=pltpu.PrefetchScalarGridSpec(
            num_scalar_prefetch=1, grid=(count, half // row_block), in_specs=in_specs, out_specs=(out_spec, out_spec)
        ),
        input_output_aliases=aliases,
        compiler_params=pltpu.CompilerParams(vmem_limit_bytes=32 * 2**20),
        cost_estimate=cost(count * half * width * 400, 0, source, source),
        name="split_norm",
    )(*args)


def gain_sum_kernel(tp_size, dp_size, part_ref, out_ref, slots, send_sem, recv_sem):
    total = tp_size * dp_size
    me_dp = lax.axis_index("dp")
    me = lax.axis_index("tp") * dp_size + me_dp

    def place(index):
        return (index // dp_size, lax.rem(index, dp_size))

    barrier = pltpu.get_barrier_semaphore()
    for offset in range(1, total):
        pl.semaphore_signal(barrier, inc=1, device_id=place(lax.rem(me + offset, total)), device_id_type=pl.DeviceIdType.MESH)
    pl.semaphore_wait(barrier, total - 1)

    def copy(offset, slot, target):
        return pltpu.make_async_remote_copy(
            src_ref=part_ref.at[place(target)[1]],
            dst_ref=slots.at[slot],
            send_sem=send_sem.at[offset],
            recv_sem=recv_sem.at[slot],
            device_id=place(target),
            device_id_type=pl.DeviceIdType.MESH,
        )

    for offset in range(1, total):
        copy(offset, me, lax.rem(me + offset, total)).start()
    slots[me] = part_ref[me_dp]
    for offset in range(1, total):
        copy(offset, me, lax.rem(me + offset, total)).wait_send()
        copy(offset, lax.rem(me + total - offset, total), me).wait_recv()
    result = slots[0]
    for i in range(1, total):
        result = result + slots[i]
    out_ref[...] = result


def gain_sum(part, tp_size, dp_size):
    rows = part.shape[0] // dp_size
    tile = 8 * HEAD_DIM
    padded = jnp.pad(part.reshape(dp_size, rows), ((0, 0), (0, -rows % tile))).reshape(dp_size, -1, HEAD_DIM)
    sublanes = padded.shape[1]
    total = tp_size * dp_size
    result = pl.pallas_call(
        functools.partial(gain_sum_kernel, tp_size, dp_size),
        out_shape=jax.ShapeDtypeStruct((sublanes, HEAD_DIM), F32),
        in_specs=[pl.BlockSpec(memory_space=pltpu.VMEM)],
        out_specs=pl.BlockSpec(memory_space=pltpu.VMEM),
        scratch_shapes=[
            pltpu.VMEM((total, sublanes, HEAD_DIM), F32),
            pltpu.SemaphoreType.DMA((total,)),
            pltpu.SemaphoreType.DMA((total,)),
        ],
        compiler_params=pltpu.CompilerParams(collective_id=0, has_side_effects=True),
        name="gain_sum",
    )(padded)
    return result.reshape(-1)[:rows]


def finish_out_kernel(x_ref, near_ref, far_ref, *rest):
    out_sum = (near_ref[0].astype(F32) + far_ref[0].astype(F32)).astype(BF16).astype(F32)
    rest[-1][0] = (x_ref[0].astype(F32) + out_sum).astype(BF16)


def finish_grad_kernel(x_ref, dy_ref, near_ref, gain_ref, far_ref, *rest):
    out_ref, gain_out_ref = rest[-2:]
    values = x_ref[0].astype(F32)
    inv_rms = lax.rsqrt(jnp.mean(values * values, axis=-1, keepdims=True) + NORM_EPS)
    x_hat = values * inv_rms
    grad_normed = (near_ref[0].astype(F32) + far_ref[0].astype(F32)).astype(BF16).astype(F32)
    scaled = grad_normed * gain_ref[...]
    mean = jnp.mean(scaled * x_hat, axis=-1, keepdims=True)
    out_ref[0] = (dy_ref[0].astype(F32) + inv_rms * (scaled - x_hat * mean)).astype(BF16)

    @pl.when((pl.program_id(0) == 0) & (pl.program_id(1) == 0))
    def _():
        gain_out_ref[...] = jnp.zeros_like(gain_out_ref)

    gain_out_ref[...] += jnp.sum((grad_normed * x_hat).reshape(-1, 8, x_hat.shape[-1]), axis=0)


def finish(kernel, full, chunk, start, held, gain=None, row_block=64):
    batch, half, width = full[0].shape
    count = chunk[0].shape[0]
    row_block = min(row_block, half)
    spec = lambda offset: pl.BlockSpec((1, row_block, width), lambda b, r: (b + offset, r, 0))
    in_specs = [spec(start)] * len(full)
    args = list(full)
    out_shape = [jax.ShapeDtypeStruct((batch, half, width), BF16)]
    out_specs = [spec(start)]
    if gain is not None:
        in_specs.append(pl.BlockSpec((1, width), lambda b, r: (0, 0)))
        args.append(gain.reshape(1, width))
        out_shape.append(jax.ShapeDtypeStruct((8, width), F32))
        out_specs.append(pl.BlockSpec((8, width), lambda b, r: (0, 0)))
    in_specs += [spec(0)] * len(chunk)
    args += list(chunk)
    aliases = {}
    if held is not None:
        aliases = {len(args): 0}
        in_specs.append(pl.BlockSpec(memory_space=pl.ANY))
        args.append(held)
    result = pl.pallas_call(
        kernel,
        out_shape=out_shape,
        grid=(count, half // row_block),
        in_specs=in_specs,
        out_specs=out_specs,
        input_output_aliases=aliases,
        compiler_params=pltpu.CompilerParams(vmem_limit_bytes=32 * 2**20),
        cost_estimate=cost(count * half * width * 400, 0, *([chunk[0]] * (len(full) + len(chunk) + 1))),
    )(*args)
    return result if gain is not None else result[0]


def regroup_kernel(q_ref, k_ref, v_ref, out_ref):
    split = q_ref.shape[1]
    out_ref[:, :split] = q_ref[...]
    out_ref[:, split:split + HEAD_DIM] = k_ref[...]
    out_ref[:, split + HEAD_DIM:] = v_ref[...]


def regroup(w_query, w_key, w_value):
    rows = w_query.shape[0]
    groups = w_key.shape[1] // HEAD_DIM
    split = w_query.shape[1] // groups
    spec = lambda columns: pl.BlockSpec((rows, columns), lambda g: (0, g))
    out = jax.ShapeDtypeStruct((rows, groups * (split + 2 * HEAD_DIM)), w_query.dtype)
    return pl.pallas_call(
        regroup_kernel,
        out_shape=out,
        grid=(groups,),
        in_specs=[spec(split), spec(HEAD_DIM), spec(HEAD_DIM)],
        out_specs=spec(split + 2 * HEAD_DIM),
        cost_estimate=cost(rows * out.shape[1] * 400, 0, out, out),
        name="regroup",
    )(w_query, w_key, w_value)


def ungroup_kernel(count, *refs):
    q_ref, k_ref, v_ref = refs[-3:]
    split = q_ref.shape[1]
    for group in range(count):

        @pl.when(pl.program_id(1) == group)
        def _(group=group):
            block = refs[2 * group][...] + refs[2 * group + 1][...]
            q_ref[...] = block[:, :split]
            k_ref[...] = block[:, split:split + HEAD_DIM]
            v_ref[...] = block[:, split + HEAD_DIM:]


def ungroup(terms, start, groups, held, row_block=192):
    rows, block = terms[0][0].shape
    split = block - 2 * HEAD_DIM
    row_block = min(row_block, rows)
    spec = lambda columns: pl.BlockSpec((row_block, columns), lambda r, g: (r, g + start))
    shape = lambda columns: jax.ShapeDtypeStruct((rows, groups * columns), F32)
    args = [term for pair in terms for term in pair]
    in_specs = [pl.BlockSpec((row_block, block), lambda r, g: (r, 0))] * len(args)
    estimate = cost(rows * block * len(terms) * 400, 0, *args, *args[:len(terms)])
    aliases = {}
    if held is not None:
        in_specs += [pl.BlockSpec(memory_space=pl.ANY)] * 3
        aliases = {len(args) + i: i for i in range(3)}
        args += list(held)
    return pl.pallas_call(
        functools.partial(ungroup_kernel, len(terms)),
        out_shape=(shape(split), shape(HEAD_DIM), shape(HEAD_DIM)),
        grid=(rows // row_block, len(terms)),
        in_specs=in_specs,
        out_specs=(spec(split), spec(HEAD_DIM), spec(HEAD_DIM)),
        input_output_aliases=aliases,
        compiler_params=pltpu.CompilerParams(vmem_limit_bytes=32 * 2**20),
        cost_estimate=estimate,
        name="ungroup",
    )(*args)


CHUNKS = 2


def after(value, *others):
    return lax.optimization_barrier((value, *others))[0]


def solution(mesh):
    swap = [(0, 1), (1, 0)]

    def exchange(values):
        return lax.ppermute(values, "tp", swap)

    def mm(eq, a, b):
        return jnp.einsum(eq, a, b, preferred_element_type=F32)

    def local_block(hidden, norm_gain, w_query, w_key, w_value, w_out, grad_out):
        batch, half, _ = hidden.shape
        rows_loc = w_query.shape[0]
        groups = w_key.shape[1] // HEAD_DIM
        group_size = w_query.shape[1] // w_key.shape[1]
        block = (group_size + 2) * HEAD_DIM
        tp_index = lax.axis_index("tp").astype(jnp.int32).reshape(1)
        tables = rope_tables(2 * half)

        step = batch // CHUNKS
        hidden_rec, grad_rec = [], []
        source = hidden
        for i in range(CHUNKS):
            piece = lax.optimization_barrier(source[i * step:(i + 1) * step])
            source = after(hidden, piece)
            hidden_rec.append(exchange(piece))
        pieces = [(0, 2), (2, 1), (3, 1)]
        for start, count in pieces:
            grad_rec.append(exchange(grad_out[start:start + count]))

        w_qkv = regroup(w_query, w_key, w_value)
        w_qkv = lax.all_gather(w_qkv, "dp", axis=0, tiled=True)
        w_o = lax.all_gather(w_out, "dp", axis=1, tiled=True)
        gain = lax.all_gather(norm_gain, "dp", axis=0, tiled=True).astype(F32)

        def norm(values):
            values = values.astype(F32)
            inv_rms = lax.rsqrt(jnp.mean(values * values, axis=-1, keepdims=True) + NORM_EPS)
            return (values * inv_rms * gain).astype(BF16)

        place = lax.axis_index("dp").astype(jnp.uint32)
        core, along_x, along_y = place & 1, (place >> 1) & 1, place >> 2
        core_index = core.astype(jnp.int32).reshape(1)
        split = split_norm(core_index, gain, hidden, 0, 0, batch, None)
        for i in range(CHUNKS):
            split = split_norm(core_index, gain, hidden_rec[i], 1, i * step, batch, split)
        normed_mine, normed_sent = split

        normed_own = norm(hidden)
        qkv_own = mm("bsd,de->bse", normed_own, w_qkv).astype(BF16)
        qkv_rec = []
        attn = None
        before = qkv_own
        for i in range(CHUNKS):
            rec = norm(after(hidden_rec[i], before))
            qkv_rec.append(mm("bsd,de->bse", rec, w_qkv).astype(BF16))
            attn = attention_fwd(tp_index, qkv_own, qkv_rec[i], tables, i * step, attn, groups, group_size)
            before = attn[0]
        attn_own, attn_rec = attn

        out_send = []
        for i in range(CHUNKS):
            out_send.append(lax.optimization_barrier(mm("bse,ed->bsd", attn_rec[i * step:(i + 1) * step], w_o).astype(BF16)))

        ga_own = mm("bsd,ed->bse", after(grad_out, *out_send), w_o).astype(BF16)
        gqkv = None
        before = ga_own
        for i, (start, count) in enumerate(pieces):
            if i == len(pieces) - 1:
                grad_wo = mm("bse,bsd->ed", attn_own, after(grad_out, gqkv)) + mm("bse,bsd->ed", attn_rec, jnp.concatenate(grad_rec, axis=0))
                before = grad_wo
            ga_rec = mm("bsd,ed->bse", after(grad_rec[i], before), w_o).astype(BF16)
            gqkv = attention_bwd(tp_index, qkv_own, qkv_rec[start // step], tables, ga_own, ga_rec, start, start % step, gqkv, groups, group_size)
            before = gqkv
        grad_wo = lax.psum_scatter(grad_wo, "dp", scatter_dimension=1, tiled=True)

        cut = groups // 2 * block

        def pick(values, axis, coordinate, columns=0):
            at = [jnp.uint32(0)] * values.ndim
            at[axis], at[-1] = coordinate, jnp.uint32(columns)
            size = [*values.shape[:-1], block]
            size[axis] = 1
            return lax.squeeze(lax.dynamic_slice(values, at, size), [axis])

        def pass_on(values, bit):
            return lax.ppermute(values, "dp", [(i, i ^ bit) for i in range(8)])

        def weight_grad(normed, columns, before):
            return mm("hbsd,hbse->de", normed, after(gqkv, *before)[..., columns])

        late, early = slice(cut, 2 * cut), slice(0, cut)
        late_sent = weight_grad(normed_sent, late, [])
        late_far = pass_on(late_sent, 1)
        early_sent = weight_grad(normed_sent, early, [late_sent])
        early_far = pass_on(early_sent, 1)

        def first_stage(mine, far):
            total = (mine + far).reshape(2, 2, rows_loc, cut)
            sent = pick(total, 1, along_x ^ 1), pick(total, 0, along_y ^ 1, block)
            sent, total = lax.optimization_barrier((sent, total))
            mine = pick(total, 1, along_x), pick(total, 0, along_y, block)
            return sent, mine, (pass_on(sent[0], 2), pass_on(sent[1], 4))

        def second_stage(mine, far, before):
            far = after(far, *before)
            total = mine[0] + far[0], mine[1] + far[1]
            sent = pick(total[0], 0, along_y ^ 1), pick(total[1], 0, along_x ^ 1)
            sent, total = lax.optimization_barrier((sent, total))
            mine = pick(total[0], 0, along_y), pick(total[1], 0, along_x)
            return sent, [(mine[0], pass_on(sent[0], 4)), (mine[1], pass_on(sent[1], 2))]

        gqkv_rec = after(gqkv, early_sent)[1]
        dn_send = []
        for i in range(CHUNKS):
            dn_send.append(lax.optimization_barrier(mm("bse,de->bsd", gqkv_rec[i * step:(i + 1) * step], w_qkv).astype(BF16)))

        out_far, dn_far = [], []
        for i in range(CHUNKS):
            out_far.append(exchange(out_send[i]))
        dn_sent = [dn_send[0], dn_send[1][:1], dn_send[1][1:]]
        for i in range(3):
            dn_far.append(exchange(dn_sent[i]))

        late_sent, late_mine, late_far = first_stage(weight_grad(normed_mine, late, dn_send), late_far)
        early_sent, early_mine, early_far = first_stage(weight_grad(normed_mine, early, late_sent), early_far)

        attn_own, gqkv = after((attn_own, gqkv), *early_sent)
        out_near = lax.optimization_barrier(mm("bse,ed->bsd", attn_own, w_o).astype(BF16))
        dn_near = lax.optimization_barrier(mm("bse,de->bsd", gqkv[0], w_qkv).astype(BF16))
        late_sent, late_terms = second_stage(late_mine, late_far, [out_near, dn_near])
        hidden_out = None
        for i in range(CHUNKS):
            hidden_out = finish(finish_out_kernel, [hidden, after(out_near, *late_sent)], [out_far[i]], i * step, hidden_out)
        early_sent, early_terms = second_stage(early_mine, early_far, [hidden_out])
        dn_near = after(dn_near, *early_sent)
        grad_hidden = None
        gain_parts = []
        w_grads = None
        for i, (start, count) in enumerate(pieces):
            grad_hidden, part = finish(
                finish_grad_kernel, [hidden, grad_out, dn_near], [dn_far[i]], start, grad_hidden, gain
            )
            gain_parts.append(part)
            if i == 0:
                w_grads = ungroup([(mine, after(far, grad_hidden)) for mine, far in late_terms], groups // 2, groups, None)
                dn_near = after(dn_near, *w_grads)
        grad_gain = gain_sum(jnp.sum(sum(gain_parts), axis=0), mesh.shape["tp"], mesh.shape["dp"])
        grad_wq, grad_wk, grad_wv = ungroup([(mine, after(far, grad_gain)) for mine, far in early_terms], 0, groups, w_grads)
        return hidden_out, grad_hidden, grad_gain, grad_wq, grad_wk, grad_wv, grad_wo

    act_spec = P("dp", "tp", None)
    col_spec = P("dp", "tp")
    row_spec = P("tp", "dp")
    return jax.shard_map(
        local_block,
        mesh=mesh,
        in_specs=(act_spec, P("dp"), col_spec, col_spec, col_spec, row_spec, act_spec),
        out_specs=(act_spec, act_spec, P("dp"), col_spec, col_spec, col_spec, row_spec),
        check_vma=False,
    )
```

```python
import functools

import jax
import jax.numpy as jnp
from jax import lax
from jax.experimental import pallas as pl
from jax.experimental.pallas import tpu as pltpu
from jax.sharding import PartitionSpec as P


HEAD_DIM = 128
NORM_EPS = 1e-5
ROPE_BASE = 500000.0
SCORE_SCALE = HEAD_DIM ** -0.5
MASK_VALUE = -1e30
F32 = jnp.float32
BF16 = jnp.bfloat16
NT = (((1,), (1,)), ((), ()))
NN = (((1,), (0,)), ((), ()))
TN = (((0,), (0,)), ((), ()))


def rope_tables(seq_len):
    half_dim = HEAD_DIM // 2
    inv_freq = ROPE_BASE ** (-jnp.arange(half_dim, dtype=F32) * 2.0 / HEAD_DIM)
    angles = jnp.arange(seq_len, dtype=F32)[:, None] * inv_freq[None, :]
    cos_t, sin_t = jnp.cos(angles), jnp.sin(angles)
    return jnp.concatenate([cos_t, cos_t], axis=1), jnp.concatenate([-sin_t, sin_t], axis=1)


def dot(lhs, rhs, dims):
    return lax.dot_general(lhs, rhs, dims, preferred_element_type=F32)


def turn(values, cos_t, sin_t):
    return values * cos_t + pltpu.roll(values, HEAD_DIM // 2, 1) * sin_t


def pick_halves(first, own, rec):
    own, rec = own.astype(F32), rec.astype(F32)
    return jnp.where(first, own, rec), jnp.where(first, rec, own)


def heads_of(group_size, block, cos_t, sin_t):
    cut = [block[:, i * HEAD_DIM:(i + 1) * HEAD_DIM] for i in range(group_size + 2)]
    queries = jnp.concatenate([turn(cut[i], cos_t, sin_t).astype(BF16) for i in range(group_size)], axis=0)
    return queries, turn(cut[group_size], cos_t, sin_t).astype(BF16), cut[group_size + 1].astype(BF16)


def store_halves(first, own_ref, rec_ref, columns, lower, upper):
    own_ref[0, :, columns] = jnp.where(first, lower, upper).astype(own_ref.dtype)
    rec_ref[0, :, columns] = jnp.where(first, upper, lower).astype(rec_ref.dtype)


def attention_fwd_kernel(group_size, tp_ref, own_ref, rec_ref, cos_ref, sin_ref, *rest):
    out_ref = rest[-1]
    half = own_ref.shape[1]
    first = tp_ref[0] == 0
    lower, upper = pick_halves(first, own_ref[0], rec_ref[0])
    q_lo, k_lo, v_lo = heads_of(group_size, lower, cos_ref[:half], sin_ref[:half])
    q_up, k_up, v_up = heads_of(group_size, upper, cos_ref[half:], sin_ref[half:])
    rows = lax.broadcasted_iota(jnp.int32, (group_size, half, half), 1).reshape(group_size * half, half)
    cols = lax.broadcasted_iota(jnp.int32, (group_size * half, half), 1)
    causal = rows >= cols

    s_lo = jnp.where(causal, dot(q_lo, k_lo, NT), MASK_VALUE)
    p_lo = jnp.exp((s_lo - jnp.max(s_lo, axis=1, keepdims=True)) * SCORE_SCALE)
    p_lo = (p_lo * (1.0 / jnp.sum(p_lo, axis=1, keepdims=True))).astype(BF16)
    a_lo = dot(p_lo, v_lo, NN)

    s_a = dot(q_up, k_lo, NT)
    s_b = jnp.where(causal, dot(q_up, k_up, NT), MASK_VALUE)
    top = jnp.maximum(jnp.max(s_a, axis=1, keepdims=True), jnp.max(s_b, axis=1, keepdims=True))
    p_a = jnp.exp((s_a - top) * SCORE_SCALE)
    p_b = jnp.exp((s_b - top) * SCORE_SCALE)
    inv = 1.0 / (jnp.sum(p_a, axis=1, keepdims=True) + jnp.sum(p_b, axis=1, keepdims=True))
    a_up = dot((p_a * inv).astype(BF16), v_lo, NN) + dot((p_b * inv).astype(BF16), v_up, NN)
    for i in range(group_size):
        part = slice(i * half, (i + 1) * half)
        store_halves(first, out_ref.at[0], out_ref.at[1], slice(i * HEAD_DIM, (i + 1) * HEAD_DIM), a_lo[part], a_up[part])


def attention_bwd_kernel(group_size, tp_ref, own_ref, rec_ref, cos_ref, sin_ref, ga_own_ref, ga_rec_ref, *rest):
    out_ref = rest[-1]
    half = own_ref.shape[1]
    first = tp_ref[0] == 0
    lower, upper = pick_halves(first, own_ref[0], rec_ref[0])
    cos_lo, sin_lo, cos_up, sin_up = cos_ref[:half], sin_ref[:half], cos_ref[half:], sin_ref[half:]
    q_lo, k_lo, v_lo = heads_of(group_size, lower, cos_lo, sin_lo)
    q_up, k_up, v_up = heads_of(group_size, upper, cos_up, sin_up)
    ga_lower, ga_upper = pick_halves(first, ga_own_ref[0], ga_rec_ref[0])

    def stacked(block):
        return jnp.concatenate([block[:, i * HEAD_DIM:(i + 1) * HEAD_DIM].astype(BF16) for i in range(group_size)], axis=0)

    ga_lo, ga_up = stacked(ga_lower), stacked(ga_upper)
    keys = lax.broadcasted_iota(jnp.int32, (half, half), 0)
    spots = lax.broadcasted_iota(jnp.int32, (half, half), 1)
    causal = jnp.concatenate([spots >= keys] * group_size, axis=1)

    s_lo = jnp.where(causal, dot(k_lo, q_lo, NT), MASK_VALUE)
    p_lo = jnp.exp((s_lo - jnp.max(s_lo, axis=0, keepdims=True)) * SCORE_SCALE)
    p_lo = p_lo * (1.0 / jnp.sum(p_lo, axis=0, keepdims=True))
    gp_lo = dot(v_lo, ga_lo, NT).astype(BF16).astype(F32)
    gs_lo = (p_lo * (gp_lo - jnp.sum(gp_lo * p_lo, axis=0, keepdims=True)) * SCORE_SCALE).astype(BF16)

    s_a = dot(k_lo, q_up, NT)
    s_b = jnp.where(causal, dot(k_up, q_up, NT), MASK_VALUE)
    top = jnp.maximum(jnp.max(s_a, axis=0, keepdims=True), jnp.max(s_b, axis=0, keepdims=True))
    p_a = jnp.exp((s_a - top) * SCORE_SCALE)
    p_b = jnp.exp((s_b - top) * SCORE_SCALE)
    inv = 1.0 / (jnp.sum(p_a, axis=0, keepdims=True) + jnp.sum(p_b, axis=0, keepdims=True))
    p_a = p_a * inv
    p_b = p_b * inv
    gp_a = dot(v_lo, ga_up, NT).astype(BF16).astype(F32)
    gp_b = dot(v_up, ga_up, NT).astype(BF16).astype(F32)
    mean_up = jnp.sum(gp_a * p_a, axis=0, keepdims=True) + jnp.sum(gp_b * p_b, axis=0, keepdims=True)
    gs_a = (p_a * (gp_a - mean_up) * SCORE_SCALE).astype(BF16)
    gs_b = (p_b * (gp_b - mean_up) * SCORE_SCALE).astype(BF16)

    gv_lo = dot(p_lo.astype(BF16), ga_lo, NN) + dot(p_a.astype(BF16), ga_up, NN)
    gv_up = dot(p_b.astype(BF16), ga_up, NN)
    gk_lo = (dot(gs_lo, q_lo, NN) + dot(gs_a, q_up, NN)).astype(BF16).astype(F32)
    gk_up = dot(gs_b, q_up, NN).astype(BF16).astype(F32)
    gq_lo = dot(gs_lo, k_lo, TN).astype(BF16).astype(F32)
    gq_up = (dot(gs_a, k_lo, TN) + dot(gs_b, k_up, TN)).astype(BF16).astype(F32)

    def store(index, lower_part, upper_part):
        store_halves(first, out_ref.at[0], out_ref.at[1], slice(index * HEAD_DIM, (index + 1) * HEAD_DIM), lower_part, upper_part)

    for i in range(group_size):
        part = slice(i * half, (i + 1) * half)
        store(i, turn(gq_lo[part], cos_lo, -sin_lo), turn(gq_up[part], cos_up, -sin_up))
    store(group_size, turn(gk_lo, cos_lo, -sin_lo), turn(gk_up, cos_up, -sin_up))
    store(group_size + 1, gv_lo, gv_up)


def cost(flops, transcendentals, *arrays):
    return pl.CostEstimate(flops=int(flops), transcendentals=int(transcendentals), bytes_accessed=int(sum(a.size * a.dtype.itemsize for a in arrays)))


def attention_fwd(tp_index, qkv_own, qkv_rec, tables, start, held, groups, group_size):
    batch, half, width = qkv_own.shape
    count = qkv_rec.shape[0]
    block = width // groups
    out_block = group_size * HEAD_DIM
    shape = jax.ShapeDtypeStruct((2, batch, half, groups * out_block), BF16)
    spec = lambda columns, offset: pl.BlockSpec((1, half, columns), lambda b, g, tp: (b + offset, 0, g))
    table = pl.BlockSpec((2 * half, HEAD_DIM), lambda b, g, tp: (0, 0))
    in_specs = [spec(block, start), spec(block, 0), table, table]
    args = [tp_index, qkv_own, qkv_rec, *tables]
    aliases = {}
    if held is not None:
        in_specs.append(pl.BlockSpec(memory_space=pl.ANY))
        aliases = {len(args): 0}
        args.append(held)
    work = count * groups * group_size * half * half
    return pl.pallas_call(
        functools.partial(attention_fwd_kernel, group_size),
        out_shape=shape,
        grid_spec=pltpu.PrefetchScalarGridSpec(
            num_scalar_prefetch=1,
            grid=(count, groups),
            in_specs=in_specs,
            out_specs=pl.BlockSpec((2, 1, half, out_block), lambda b, g, tp: (0, b + start, 0, g)),
        ),
        input_output_aliases=aliases,
        compiler_params=pltpu.CompilerParams(vmem_limit_bytes=48 * 2**20),
        cost_estimate=cost(work * HEAD_DIM * 12, work * 3, qkv_rec, qkv_rec),
        name="attention_fwd",
    )(*args)


def attention_bwd(tp_index, qkv_own, qkv_rec, tables, ga_own, ga_rec, start, rec_start, held, groups, group_size):
    batch, half, width = qkv_own.shape
    count = ga_rec.shape[0]
    block = width // groups
    ga_block = group_size * HEAD_DIM
    shape = jax.ShapeDtypeStruct((2, batch, half, width), BF16)
    spec = lambda columns, offset: pl.BlockSpec((1, half, columns), lambda b, g, tp: (b + offset, 0, g))
    table = pl.BlockSpec((2 * half, HEAD_DIM), lambda b, g, tp: (0, 0))
    in_specs = [spec(block, start), spec(block, rec_start), table, table, spec(ga_block, start), spec(ga_block, 0)]
    args = [tp_index, qkv_own, qkv_rec, *tables, ga_own, ga_rec]
    aliases = {}
    if held is not None:
        in_specs.append(pl.BlockSpec(memory_space=pl.ANY))
        aliases = {len(args): 0}
        args.append(held)
    work = count * groups * group_size * half * half
    return pl.pallas_call(
        functools.partial(attention_bwd_kernel, group_size),
        out_shape=shape,
        grid_spec=pltpu.PrefetchScalarGridSpec(
            num_scalar_prefetch=1,
            grid=(count, groups),
            in_specs=in_specs,
            out_specs=pl.BlockSpec((2, 1, half, block), lambda b, g, tp: (0, b + start, 0, g)),
        ),
        input_output_aliases=aliases,
        compiler_params=pltpu.CompilerParams(vmem_limit_bytes=48 * 2**20),
        cost_estimate=cost(work * HEAD_DIM * 30, work * 3, ga_rec, ga_rec, ga_rec, ga_rec),
        name="attention_bwd",
    )(*args)


def split_kernel(normalise, core_ref, gain_ref, source_ref, *rest):
    mine_ref, sent_ref = rest[-2:]
    first = core_ref[0] == 0
    normed = source_ref[0].astype(F32)
    if normalise:
        inv_rms = lax.rsqrt(jnp.mean(normed * normed, axis=-1, keepdims=True) + NORM_EPS)
        normed = normed * inv_rms * gain_ref[...]
    rows = normed.shape[1] // 8
    for i in range(4):
        even = normed[:, 2 * i * rows:(2 * i + 1) * rows]
        odd = normed[:, (2 * i + 1) * rows:(2 * i + 2) * rows]
        mine_ref[0, 0, :, i * rows:(i + 1) * rows] = jnp.where(first, even, odd).astype(BF16)
        sent_ref[0, 0, :, i * rows:(i + 1) * rows] = jnp.where(first, odd, even).astype(BF16)


def split_columns(core_index, gain, source, kind, start, batch, held, normalise, row_block=128):
    count, half, width = source.shape
    row_block = min(row_block, half)
    out = jax.ShapeDtypeStruct((2, batch, half, width // 2), BF16)
    out_spec = pl.BlockSpec((1, 1, row_block, width // 2), lambda b, r, c: (kind, b + start, r, 0))
    in_specs = [pl.BlockSpec((1, width), lambda b, r, c: (0, 0)), pl.BlockSpec((1, row_block, width), lambda b, r, c: (b, r, 0))]
    args = [core_index, gain.reshape(1, width), source]
    aliases = {}
    if held is not None:
        in_specs += [pl.BlockSpec(memory_space=pl.ANY)] * 2
        aliases = {len(args): 0, len(args) + 1: 1}
        args += list(held)
    return pl.pallas_call(
        functools.partial(split_kernel, normalise),
        out_shape=(out, out),
        grid_spec=pltpu.PrefetchScalarGridSpec(
            num_scalar_prefetch=1, grid=(count, half // row_block), in_specs=in_specs, out_specs=(out_spec, out_spec)
        ),
        input_output_aliases=aliases,
        compiler_params=pltpu.CompilerParams(vmem_limit_bytes=32 * 2**20),
        cost_estimate=cost(count * half * width * 400, 0, source, source),
        name="split_norm" if normalise else "split_plain",
    )(*args)


def join_kernel(axis, place_ref, *refs):
    out_ref = refs[-1]
    relative = pl.program_id(0) ^ place_ref[0]
    own = pl.program_id(1) == place_ref[1]

    def put(values):
        out_ref[...] = values.reshape(out_ref.shape)

    for side, here in ((refs[:5], own), (refs[5:10], jnp.logical_not(own))):
        for index, source in ((0, 0), (1, 2), (2, 1)):

            @pl.when(here & (relative == index))
            def _(source=source, side=side):
                put(side[source][...])

        @pl.when(here & (relative == 3))
        def _(side=side):
            put(jnp.concatenate([side[3][...], side[4][...]], axis=axis))


def join(place, near, far, axis):
    rows, columns = near[0].shape
    whole = lambda array: pl.BlockSpec(array.shape, lambda j, c, place: (0, 0))
    if axis == 1:
        out, out_spec = (8 * rows, columns), pl.BlockSpec((rows, columns), lambda j, c, place: (2 * j + c, 0))
    else:
        out, out_spec = (rows, 8 * columns), pl.BlockSpec((rows, columns), lambda j, c, place: (0, 2 * j + c))
    out = jax.ShapeDtypeStruct(out, BF16)
    return pl.pallas_call(
        functools.partial(join_kernel, axis),
        out_shape=out,
        grid_spec=pltpu.PrefetchScalarGridSpec(
            num_scalar_prefetch=1, grid=(4, 2), in_specs=[whole(array) for array in (*near, *far)], out_specs=out_spec
        ),
        compiler_params=pltpu.CompilerParams(vmem_limit_bytes=48 * 2**20),
        cost_estimate=cost(out.size * 400, 0, out, out),
        name="join",
    )(place, *near, *far)


def gain_sum_kernel(tp_size, dp_size, part_ref, out_ref, slots, send_sem, recv_sem):
    total = tp_size * dp_size
    me_dp = lax.axis_index("dp")
    me = lax.axis_index("tp") * dp_size + me_dp

    def place(index):
        return (index // dp_size, lax.rem(index, dp_size))

    barrier = pltpu.get_barrier_semaphore()
    for offset in range(1, total):
        pl.semaphore_signal(barrier, inc=1, device_id=place(lax.rem(me + offset, total)), device_id_type=pl.DeviceIdType.MESH)
    pl.semaphore_wait(barrier, total - 1)

    def copy(offset, slot, target):
        return pltpu.make_async_remote_copy(
            src_ref=part_ref.at[place(target)[1]],
            dst_ref=slots.at[slot],
            send_sem=send_sem.at[offset],
            recv_sem=recv_sem.at[slot],
            device_id=place(target),
            device_id_type=pl.DeviceIdType.MESH,
        )

    for offset in range(1, total):
        copy(offset, me, lax.rem(me + offset, total)).start()
    slots[me] = part_ref[me_dp]
    for offset in range(1, total):
        copy(offset, me, lax.rem(me + offset, total)).wait_send()
        copy(offset, lax.rem(me + total - offset, total), me).wait_recv()
    result = slots[0]
    for i in range(1, total):
        result = result + slots[i]
    out_ref[...] = result


def gain_sum(part, tp_size, dp_size):
    rows = part.shape[0] // dp_size
    tile = 8 * HEAD_DIM
    padded = jnp.pad(part.reshape(dp_size, rows), ((0, 0), (0, -rows % tile))).reshape(dp_size, -1, HEAD_DIM)
    sublanes = padded.shape[1]
    total = tp_size * dp_size
    result = pl.pallas_call(
        functools.partial(gain_sum_kernel, tp_size, dp_size),
        out_shape=jax.ShapeDtypeStruct((sublanes, HEAD_DIM), F32),
        in_specs=[pl.BlockSpec(memory_space=pltpu.VMEM)],
        out_specs=pl.BlockSpec(memory_space=pltpu.VMEM),
        scratch_shapes=[
            pltpu.VMEM((total, sublanes, HEAD_DIM), F32),
            pltpu.SemaphoreType.DMA((total,)),
            pltpu.SemaphoreType.DMA((total,)),
        ],
        compiler_params=pltpu.CompilerParams(collective_id=0, has_side_effects=True),
        name="gain_sum",
    )(padded)
    return result.reshape(-1)[:rows]


def finish_out_kernel(x_ref, near_ref, far_ref, *rest):
    out_sum = (near_ref[0].astype(F32) + far_ref[0].astype(F32)).astype(BF16).astype(F32)
    rest[-1][0] = (x_ref[0].astype(F32) + out_sum).astype(BF16)


def finish_grad_kernel(x_ref, dy_ref, near_ref, gain_ref, far_ref, *rest):
    out_ref, gain_out_ref = rest[-2:]
    values = x_ref[0].astype(F32)
    inv_rms = lax.rsqrt(jnp.mean(values * values, axis=-1, keepdims=True) + NORM_EPS)
    x_hat = values * inv_rms
    grad_normed = (near_ref[0].astype(F32) + far_ref[0].astype(F32)).astype(BF16).astype(F32)
    scaled = grad_normed * gain_ref[...]
    mean = jnp.mean(scaled * x_hat, axis=-1, keepdims=True)
    out_ref[0] = (dy_ref[0].astype(F32) + inv_rms * (scaled - x_hat * mean)).astype(BF16)

    @pl.when((pl.program_id(0) == 0) & (pl.program_id(1) == 0))
    def _():
        gain_out_ref[...] = jnp.zeros_like(gain_out_ref)

    gain_out_ref[...] += jnp.sum((grad_normed * x_hat).reshape(-1, 8, x_hat.shape[-1]), axis=0)


def finish(kernel, full, chunk, start, held, gain=None, row_block=64):
    batch, half, width = full[0].shape
    count = chunk[0].shape[0]
    row_block = min(row_block, half)
    spec = lambda offset: pl.BlockSpec((1, row_block, width), lambda b, r: (b + offset, r, 0))
    in_specs = [spec(start)] * len(full)
    args = list(full)
    out_shape = [jax.ShapeDtypeStruct((batch, half, width), BF16)]
    out_specs = [spec(start)]
    if gain is not None:
        in_specs.append(pl.BlockSpec((1, width), lambda b, r: (0, 0)))
        args.append(gain.reshape(1, width))
        out_shape.append(jax.ShapeDtypeStruct((8, width), F32))
        out_specs.append(pl.BlockSpec((8, width), lambda b, r: (0, 0)))
    in_specs += [spec(0)] * len(chunk)
    args += list(chunk)
    aliases = {}
    if held is not None:
        aliases = {len(args): 0}
        in_specs.append(pl.BlockSpec(memory_space=pl.ANY))
        args.append(held)
    result = pl.pallas_call(
        kernel,
        out_shape=out_shape,
        grid=(count, half // row_block),
        in_specs=in_specs,
        out_specs=out_specs,
        input_output_aliases=aliases,
        compiler_params=pltpu.CompilerParams(vmem_limit_bytes=32 * 2**20),
        cost_estimate=cost(count * half * width * 400, 0, *([chunk[0]] * (len(full) + len(chunk) + 1))),
    )(*args)
    return result if gain is not None else result[0]


def regroup_kernel(q_ref, k_ref, v_ref, out_ref):
    split = q_ref.shape[1]
    out_ref[:, :split] = q_ref[...]
    out_ref[:, split:split + HEAD_DIM] = k_ref[...]
    out_ref[:, split + HEAD_DIM:] = v_ref[...]


def regroup(w_query, w_key, w_value):
    rows = w_query.shape[0]
    groups = w_key.shape[1] // HEAD_DIM
    split = w_query.shape[1] // groups
    spec = lambda columns: pl.BlockSpec((rows, columns), lambda g: (0, g))
    out = jax.ShapeDtypeStruct((rows, groups * (split + 2 * HEAD_DIM)), w_query.dtype)
    return pl.pallas_call(
        regroup_kernel,
        out_shape=out,
        grid=(groups,),
        in_specs=[spec(split), spec(HEAD_DIM), spec(HEAD_DIM)],
        out_specs=spec(split + 2 * HEAD_DIM),
        cost_estimate=cost(rows * out.shape[1] * 400, 0, out, out),
        name="regroup",
    )(w_query, w_key, w_value)


def ungroup_kernel(count, *refs):
    q_ref, k_ref, v_ref = refs[-3:]
    split = q_ref.shape[1]
    for group in range(count):

        @pl.when(pl.program_id(1) == group)
        def _(group=group):
            block = refs[2 * group][...] + refs[2 * group + 1][...]
            q_ref[...] = block[:, :split]
            k_ref[...] = block[:, split:split + HEAD_DIM]
            v_ref[...] = block[:, split + HEAD_DIM:]


def ungroup(terms, start, groups, held, row_block=192):
    rows, block = terms[0][0].shape
    split = block - 2 * HEAD_DIM
    row_block = min(row_block, rows)
    spec = lambda columns: pl.BlockSpec((row_block, columns), lambda r, g: (r, g + start))
    shape = lambda columns: jax.ShapeDtypeStruct((rows, groups * columns), F32)
    args = [term for pair in terms for term in pair]
    in_specs = [pl.BlockSpec((row_block, block), lambda r, g: (r, 0))] * len(args)
    estimate = cost(rows * block * len(terms) * 400, 0, *args, *args[:len(terms)])
    aliases = {}
    if held is not None:
        in_specs += [pl.BlockSpec(memory_space=pl.ANY)] * 3
        aliases = {len(args) + i: i for i in range(3)}
        args += list(held)
    return pl.pallas_call(
        functools.partial(ungroup_kernel, len(terms)),
        out_shape=(shape(split), shape(HEAD_DIM), shape(HEAD_DIM)),
        grid=(rows // row_block, len(terms)),
        in_specs=in_specs,
        out_specs=(spec(split), spec(HEAD_DIM), spec(HEAD_DIM)),
        input_output_aliases=aliases,
        compiler_params=pltpu.CompilerParams(vmem_limit_bytes=32 * 2**20),
        cost_estimate=estimate,
        name="ungroup",
    )(*args)


CHUNKS = 2


def after(value, *others):
    return lax.optimization_barrier((value, *others))[0]


def solution(mesh):
    swap = [(0, 1), (1, 0)]

    def exchange(values):
        return lax.ppermute(values, "tp", swap)

    def mm(eq, a, b):
        return jnp.einsum(eq, a, b, preferred_element_type=F32)

    def local_block(hidden, norm_gain, w_query, w_key, w_value, w_out, grad_out):
        batch, half, _ = hidden.shape
        rows_loc = w_query.shape[0]
        groups = w_key.shape[1] // HEAD_DIM
        group_size = w_query.shape[1] // w_key.shape[1]
        block = (group_size + 2) * HEAD_DIM
        tp_index = lax.axis_index("tp").astype(jnp.int32).reshape(1)
        tables = rope_tables(2 * half)

        step = batch // CHUNKS
        hidden_rec, grad_rec = [], []
        source = hidden
        for i in range(CHUNKS):
            piece = lax.optimization_barrier(source[i * step:(i + 1) * step])
            source = after(hidden, piece)
            hidden_rec.append(exchange(piece))
        pieces = [(0, 2), (2, 1), (3, 1)]
        for start, count in pieces:
            grad_rec.append(exchange(grad_out[start:start + count]))

        place = lax.axis_index("dp").astype(jnp.uint32)
        core, along_x, along_y = place & 1, (place >> 1) & 1, place >> 2
        core_index = core.astype(jnp.int32).reshape(1)

        def pass_on(values, bit):
            return lax.ppermute(values, "dp", [(i, i ^ bit) for i in range(8)])

        cut, cut_o = groups // 2 * block, w_out.shape[0] // 2
        chip_core = jnp.stack([place >> 1, core]).astype(jnp.int32)

        def gather(piece, axis, before=()):
            from_y = pass_on(piece, 4)
            from_x = pass_on(piece, 2)
            from_y, from_x = after((from_y, from_x), *before)
            middle = piece.shape[axis] // 2
            diagonal = (
                pass_on(lax.slice_in_dim(from_y, 0, middle, axis=axis), 2),
                pass_on(lax.slice_in_dim(from_x, middle, None, axis=axis), 4),
            )
            near = (piece, from_y, from_x, *diagonal)
            far = [pass_on(part, 1) for part in near]
            return join(chip_core, near, far, axis)

        w_qkv = regroup(w_query, w_key, w_value)
        w_qkv = gather(w_qkv, 1)
        w_o = gather(w_out, 0, [w_qkv])
        gain = lax.all_gather(norm_gain, "dp", axis=0, tiled=True).astype(F32)

        def norm(values):
            values = values.astype(F32)
            inv_rms = lax.rsqrt(jnp.mean(values * values, axis=-1, keepdims=True) + NORM_EPS)
            return (values * inv_rms * gain).astype(BF16)

        split = split_columns(core_index, gain, hidden, 0, 0, batch, None, True)
        for i in range(CHUNKS):
            split = split_columns(core_index, gain, hidden_rec[i], 1, i * step, batch, split, True)
        normed_mine, normed_sent = split
        split = split_columns(core_index, gain, grad_out, 0, 0, batch, None, False)
        for i, (start, _) in enumerate(pieces):
            split = split_columns(core_index, gain, grad_rec[i], 1, start, batch, split, False)
        dy_mine, dy_sent = split

        normed_own = norm(hidden)
        qkv_own = mm("bsd,de->bse", normed_own, w_qkv).astype(BF16)
        qkv_rec = []
        attn = None
        before = qkv_own
        for i in range(CHUNKS):
            rec = norm(after(hidden_rec[i], before))
            qkv_rec.append(mm("bsd,de->bse", rec, w_qkv).astype(BF16))
            attn = attention_fwd(tp_index, qkv_own, qkv_rec[i], tables, i * step, attn, groups, group_size)
            before = attn

        out_send = []
        for i in range(CHUNKS):
            out_send.append(lax.optimization_barrier(mm("bse,ed->bsd", attn[1][i * step:(i + 1) * step], w_o).astype(BF16)))

        ga_own = mm("bsd,ed->bse", after(grad_out, *out_send), w_o).astype(BF16)
        gqkv = None
        before = ga_own
        for i, (start, count) in enumerate(pieces):
            if i == len(pieces) - 1:
                out_grad_sent = mm("hbse,hbsd->ed", after(attn, gqkv), dy_sent)
                out_grad_far = pass_on(out_grad_sent, 1)
                before = out_grad_sent
            ga_rec = mm("bsd,ed->bse", after(grad_rec[i], before), w_o).astype(BF16)
            gqkv = attention_bwd(tp_index, qkv_own, qkv_rec[start // step], tables, ga_own, ga_rec, start, start % step, gqkv, groups, group_size)
            before = gqkv

        def column_pick(values, pieces_at, row=0, wide=1):
            cuts = [lax.dynamic_slice(values, (jnp.uint32(row), at * rows_loc), (cut_o, wide * rows_loc)) for at in pieces_at]
            return cuts[0] if len(cuts) == 1 else jnp.concatenate(cuts, axis=1)

        total = mm("hbse,hbsd->ed", after(attn, gqkv), dy_mine) + out_grad_far
        o_sent = column_pick(total, [along_x ^ 1, 2 + (along_x ^ 1)]), column_pick(total, [2 * (along_y ^ 1)], cut_o, 2)
        o_sent, total = lax.optimization_barrier((o_sent, total))
        o_mine = column_pick(total, [along_x, 2 + along_x]), column_pick(total, [2 * along_y], cut_o, 2)
        o_far = pass_on(o_sent[0], 2), pass_on(o_sent[1], 4)

        def second_stage_o(before):
            far = after(o_far, *before)
            total = o_mine[0] + far[0], o_mine[1] + far[1]
            sent = column_pick(total[0], [along_y ^ 1]), column_pick(total[1], [along_x ^ 1])
            sent, total = lax.optimization_barrier((sent, total))
            mine = column_pick(total[0], [along_y]), column_pick(total[1], [along_x])
            return sent, mine, (pass_on(sent[0], 4), pass_on(sent[1], 2))

        def pick(values, axis, coordinate, columns=0):
            at = [jnp.uint32(0)] * values.ndim
            at[axis], at[-1] = coordinate, jnp.uint32(columns)
            size = [*values.shape[:-1], block]
            size[axis] = 1
            return lax.squeeze(lax.dynamic_slice(values, at, size), [axis])

        def weight_grad(normed, columns, before):
            return mm("hbsd,hbse->de", normed, after(gqkv, *before)[..., columns])

        late, early = slice(cut, 2 * cut), slice(0, cut)
        late_sent = weight_grad(normed_sent, late, o_sent)
        late_far = pass_on(late_sent, 1)
        early_sent = weight_grad(normed_sent, early, [late_sent])
        early_far = pass_on(early_sent, 1)

        def first_stage(mine, far):
            total = (mine + far).reshape(2, 2, rows_loc, cut)
            sent = pick(total, 1, along_x ^ 1), pick(total, 0, along_y ^ 1, block)
            sent, total = lax.optimization_barrier((sent, total))
            mine = pick(total, 1, along_x), pick(total, 0, along_y, block)
            return sent, mine, (pass_on(sent[0], 2), pass_on(sent[1], 4))

        def second_stage(mine, far, before):
            far = after(far, *before)
            total = mine[0] + far[0], mine[1] + far[1]
            sent = pick(total[0], 0, along_y ^ 1), pick(total[1], 0, along_x ^ 1)
            sent, total = lax.optimization_barrier((sent, total))
            mine = pick(total[0], 0, along_y), pick(total[1], 0, along_x)
            return sent, [(mine[0], pass_on(sent[0], 4)), (mine[1], pass_on(sent[1], 2))]

        gqkv_rec = after(gqkv, early_sent)[1]
        dn_send = []
        for i in range(CHUNKS):
            dn_send.append(lax.optimization_barrier(mm("bse,de->bsd", gqkv_rec[i * step:(i + 1) * step], w_qkv).astype(BF16)))

        out_far, dn_far = [], []
        for i in range(CHUNKS):
            out_far.append(exchange(out_send[i]))
        dn_sent = [dn_send[0], dn_send[1][:1], dn_send[1][1:]]
        for i in range(3):
            dn_far.append(exchange(dn_sent[i]))

        o_sent, o_mine, o_far = second_stage_o(dn_send)
        late_sent, late_mine, late_far = first_stage(weight_grad(normed_mine, late, o_sent), late_far)
        early_sent, early_mine, early_far = first_stage(weight_grad(normed_mine, early, late_sent), early_far)

        attn, gqkv = after((attn, gqkv), *early_sent)
        out_near = lax.optimization_barrier(mm("bse,ed->bsd", attn[0], w_o).astype(BF16))
        dn_near = lax.optimization_barrier(mm("bse,de->bsd", gqkv[0], w_qkv).astype(BF16))
        late_sent, late_terms = second_stage(late_mine, late_far, [out_near, dn_near])
        hidden_out = None
        for i in range(CHUNKS):
            hidden_out = finish(finish_out_kernel, [hidden, after(out_near, *late_sent)], [out_far[i]], i * step, hidden_out)
        early_sent, early_terms = second_stage(early_mine, early_far, [hidden_out])
        dn_near = after(dn_near, *early_sent)
        grad_hidden = None
        gain_parts = []
        w_grads = None
        for i, (start, count) in enumerate(pieces):
            grad_hidden, part = finish(
                finish_grad_kernel, [hidden, grad_out, dn_near], [dn_far[i]], start, grad_hidden, gain
            )
            gain_parts.append(part)
            if i == 1:
                w_grads = ungroup([(mine, after(far, grad_hidden)) for mine, far in early_terms], 0, groups, w_grads)
                dn_near = after(dn_near, *w_grads)
            if i == 0:
                w_grads = ungroup([(mine, after(far, grad_hidden)) for mine, far in late_terms], groups // 2, groups, None)
                dn_near = after(dn_near, *w_grads)
        grad_gain = gain_sum(jnp.sum(sum(gain_parts), axis=0), mesh.shape["tp"], mesh.shape["dp"])
        grad_wq, grad_wk, grad_wv = w_grads
        grad_wo = jnp.concatenate([o_mine[0] + after(o_far[0], hidden_out), o_mine[1] + after(o_far[1], hidden_out)], axis=0)
        return hidden_out, grad_hidden, grad_gain, grad_wq, grad_wk, grad_wv, grad_wo

    act_spec = P("dp", "tp", None)
    col_spec = P("dp", "tp")
    row_spec = P("tp", "dp")
    return jax.shard_map(
        local_block,
        mesh=mesh,
        in_specs=(act_spec, P("dp"), col_spec, col_spec, col_spec, row_spec, act_spec),
        out_specs=(act_spec, act_spec, P("dp"), col_spec, col_spec, col_spec, row_spec),
        check_vma=False,
    )
```

```python
import functools

import jax
import jax.numpy as jnp
from jax import lax
from jax.experimental import pallas as pl
from jax.experimental.pallas import tpu as pltpu
from jax.sharding import PartitionSpec as P


HEAD_DIM = 128
NORM_EPS = 1e-5
ROPE_BASE = 500000.0
SCORE_SCALE = HEAD_DIM ** -0.5
MASK_VALUE = -1e30
F32 = jnp.float32
BF16 = jnp.bfloat16
NT = (((1,), (1,)), ((), ()))
NN = (((1,), (0,)), ((), ()))
TN = (((0,), (0,)), ((), ()))


def rope_tables(seq_len):
    half_dim = HEAD_DIM // 2
    inv_freq = ROPE_BASE ** (-jnp.arange(half_dim, dtype=F32) * 2.0 / HEAD_DIM)
    angles = jnp.arange(seq_len, dtype=F32)[:, None] * inv_freq[None, :]
    cos_t, sin_t = jnp.cos(angles), jnp.sin(angles)
    return jnp.concatenate([cos_t, cos_t], axis=1), jnp.concatenate([-sin_t, sin_t], axis=1)


def dot(lhs, rhs, dims):
    return lax.dot_general(lhs, rhs, dims, preferred_element_type=F32)


def turn(values, cos_t, sin_t):
    return values * cos_t + pltpu.roll(values, HEAD_DIM // 2, 1) * sin_t


def pick_halves(first, own, rec):
    own, rec = own.astype(F32), rec.astype(F32)
    return jnp.where(first, own, rec), jnp.where(first, rec, own)


def heads_of(group_size, block, cos_t, sin_t):
    cut = [block[:, i * HEAD_DIM:(i + 1) * HEAD_DIM] for i in range(group_size + 2)]
    queries = jnp.concatenate([turn(cut[i], cos_t, sin_t).astype(BF16) for i in range(group_size)], axis=0)
    return queries, turn(cut[group_size], cos_t, sin_t).astype(BF16), cut[group_size + 1].astype(BF16)


def store_halves(first, own_ref, rec_ref, columns, lower, upper):
    own_ref[0, :, columns] = jnp.where(first, lower, upper).astype(own_ref.dtype)
    rec_ref[0, :, columns] = jnp.where(first, upper, lower).astype(rec_ref.dtype)


def attention_fwd_kernel(group_size, tp_ref, own_ref, rec_ref, cos_ref, sin_ref, *rest):
    out_own_ref, out_rec_ref = rest[-2:]
    half = own_ref.shape[1]
    first = tp_ref[0] == 0
    lower, upper = pick_halves(first, own_ref[0], rec_ref[0])
    q_lo, k_lo, v_lo = heads_of(group_size, lower, cos_ref[:half], sin_ref[:half])
    q_up, k_up, v_up = heads_of(group_size, upper, cos_ref[half:], sin_ref[half:])
    rows = lax.broadcasted_iota(jnp.int32, (group_size, half, half), 1).reshape(group_size * half, half)
    cols = lax.broadcasted_iota(jnp.int32, (group_size * half, half), 1)
    causal = rows >= cols

    s_lo = jnp.where(causal, dot(q_lo, k_lo, NT), MASK_VALUE)
    p_lo = jnp.exp((s_lo - jnp.max(s_lo, axis=1, keepdims=True)) * SCORE_SCALE)
    p_lo = (p_lo * (1.0 / jnp.sum(p_lo, axis=1, keepdims=True))).astype(BF16)
    a_lo = dot(p_lo, v_lo, NN)

    s_a = dot(q_up, k_lo, NT)
    s_b = jnp.where(causal, dot(q_up, k_up, NT), MASK_VALUE)
    top = jnp.maximum(jnp.max(s_a, axis=1, keepdims=True), jnp.max(s_b, axis=1, keepdims=True))
    p_a = jnp.exp((s_a - top) * SCORE_SCALE)
    p_b = jnp.exp((s_b - top) * SCORE_SCALE)
    inv = 1.0 / (jnp.sum(p_a, axis=1, keepdims=True) + jnp.sum(p_b, axis=1, keepdims=True))
    a_up = dot((p_a * inv).astype(BF16), v_lo, NN) + dot((p_b * inv).astype(BF16), v_up, NN)
    for i in range(group_size):
        part = slice(i * half, (i + 1) * half)
        store_halves(first, out_own_ref, out_rec_ref, slice(i * HEAD_DIM, (i + 1) * HEAD_DIM), a_lo[part], a_up[part])


def attention_bwd_kernel(group_size, tp_ref, own_ref, rec_ref, cos_ref, sin_ref, ga_own_ref, ga_rec_ref, *rest):
    out_ref = rest[-1]
    half = own_ref.shape[1]
    first = tp_ref[0] == 0
    lower, upper = pick_halves(first, own_ref[0], rec_ref[0])
    cos_lo, sin_lo, cos_up, sin_up = cos_ref[:half], sin_ref[:half], cos_ref[half:], sin_ref[half:]
    q_lo, k_lo, v_lo = heads_of(group_size, lower, cos_lo, sin_lo)
    q_up, k_up, v_up = heads_of(group_size, upper, cos_up, sin_up)
    ga_lower, ga_upper = pick_halves(first, ga_own_ref[0], ga_rec_ref[0])

    def stacked(block):
        return jnp.concatenate([block[:, i * HEAD_DIM:(i + 1) * HEAD_DIM].astype(BF16) for i in range(group_size)], axis=0)

    ga_lo, ga_up = stacked(ga_lower), stacked(ga_upper)
    keys = lax.broadcasted_iota(jnp.int32, (half, half), 0)
    spots = lax.broadcasted_iota(jnp.int32, (half, half), 1)
    causal = jnp.concatenate([spots >= keys] * group_size, axis=1)

    s_lo = jnp.where(causal, dot(k_lo, q_lo, NT), MASK_VALUE)
    p_lo = jnp.exp((s_lo - jnp.max(s_lo, axis=0, keepdims=True)) * SCORE_SCALE)
    p_lo = p_lo * (1.0 / jnp.sum(p_lo, axis=0, keepdims=True))
    gp_lo = dot(v_lo, ga_lo, NT).astype(BF16).astype(F32)
    gs_lo = (p_lo * (gp_lo - jnp.sum(gp_lo * p_lo, axis=0, keepdims=True)) * SCORE_SCALE).astype(BF16)

    s_a = dot(k_lo, q_up, NT)
    s_b = jnp.where(causal, dot(k_up, q_up, NT), MASK_VALUE)
    top = jnp.maximum(jnp.max(s_a, axis=0, keepdims=True), jnp.max(s_b, axis=0, keepdims=True))
    p_a = jnp.exp((s_a - top) * SCORE_SCALE)
    p_b = jnp.exp((s_b - top) * SCORE_SCALE)
    inv = 1.0 / (jnp.sum(p_a, axis=0, keepdims=True) + jnp.sum(p_b, axis=0, keepdims=True))
    p_a = p_a * inv
    p_b = p_b * inv
    gp_a = dot(v_lo, ga_up, NT).astype(BF16).astype(F32)
    gp_b = dot(v_up, ga_up, NT).astype(BF16).astype(F32)
    mean_up = jnp.sum(gp_a * p_a, axis=0, keepdims=True) + jnp.sum(gp_b * p_b, axis=0, keepdims=True)
    gs_a = (p_a * (gp_a - mean_up) * SCORE_SCALE).astype(BF16)
    gs_b = (p_b * (gp_b - mean_up) * SCORE_SCALE).astype(BF16)

    gv_lo = dot(p_lo.astype(BF16), ga_lo, NN) + dot(p_a.astype(BF16), ga_up, NN)
    gv_up = dot(p_b.astype(BF16), ga_up, NN)
    gk_lo = (dot(gs_lo, q_lo, NN) + dot(gs_a, q_up, NN)).astype(BF16).astype(F32)
    gk_up = dot(gs_b, q_up, NN).astype(BF16).astype(F32)
    gq_lo = dot(gs_lo, k_lo, TN).astype(BF16).astype(F32)
    gq_up = (dot(gs_a, k_lo, TN) + dot(gs_b, k_up, TN)).astype(BF16).astype(F32)

    def store(index, lower_part, upper_part):
        store_halves(first, out_ref.at[0], out_ref.at[1], slice(index * HEAD_DIM, (index + 1) * HEAD_DIM), lower_part, upper_part)

    for i in range(group_size):
        part = slice(i * half, (i + 1) * half)
        store(i, turn(gq_lo[part], cos_lo, -sin_lo), turn(gq_up[part], cos_up, -sin_up))
    store(group_size, turn(gk_lo, cos_lo, -sin_lo), turn(gk_up, cos_up, -sin_up))
    store(group_size + 1, gv_lo, gv_up)


def cost(flops, transcendentals, *arrays):
    return pl.CostEstimate(flops=int(flops), transcendentals=int(transcendentals), bytes_accessed=int(sum(a.size * a.dtype.itemsize for a in arrays)))


def attention_fwd(tp_index, qkv_own, qkv_rec, tables, start, held, groups, group_size):
    batch, half, width = qkv_own.shape
    count = qkv_rec.shape[0]
    block = width // groups
    out_block = group_size * HEAD_DIM
    shape = jax.ShapeDtypeStruct((batch, half, groups * out_block), BF16)
    spec = lambda columns, offset: pl.BlockSpec((1, half, columns), lambda b, g, tp: (b + offset, 0, g))
    table = pl.BlockSpec((2 * half, HEAD_DIM), lambda b, g, tp: (0, 0))
    in_specs = [spec(block, start), spec(block, 0), table, table]
    args = [tp_index, qkv_own, qkv_rec, *tables]
    aliases = {}
    if held is not None:
        in_specs += [pl.BlockSpec(memory_space=pl.ANY)] * 2
        aliases = {len(args): 0, len(args) + 1: 1}
        args += list(held)
    work = count * groups * group_size * half * half
    return pl.pallas_call(
        functools.partial(attention_fwd_kernel, group_size),
        out_shape=(shape, shape),
        grid_spec=pltpu.PrefetchScalarGridSpec(
            num_scalar_prefetch=1,
            grid=(count, groups),
            in_specs=in_specs,
            out_specs=(spec(out_block, start), spec(out_block, start)),
        ),
        input_output_aliases=aliases,
        compiler_params=pltpu.CompilerParams(vmem_limit_bytes=48 * 2**20),
        cost_estimate=cost(work * HEAD_DIM * 12, work * 3, qkv_rec, qkv_rec),
        name="attention_fwd",
    )(*args)


def attention_bwd(tp_index, qkv_own, qkv_rec, tables, ga_own, ga_rec, start, rec_start, held, groups, group_size):
    batch, half, width = qkv_own.shape
    count = ga_rec.shape[0]
    block = width // groups
    ga_block = group_size * HEAD_DIM
    shape = jax.ShapeDtypeStruct((2, batch, half, width), BF16)
    spec = lambda columns, offset: pl.BlockSpec((1, half, columns), lambda b, g, tp: (b + offset, 0, g))
    table = pl.BlockSpec((2 * half, HEAD_DIM), lambda b, g, tp: (0, 0))
    in_specs = [spec(block, start), spec(block, rec_start), table, table, spec(ga_block, start), spec(ga_block, 0)]
    args = [tp_index, qkv_own, qkv_rec, *tables, ga_own, ga_rec]
    aliases = {}
    if held is not None:
        in_specs.append(pl.BlockSpec(memory_space=pl.ANY))
        aliases = {len(args): 0}
        args.append(held)
    work = count * groups * group_size * half * half
    return pl.pallas_call(
        functools.partial(attention_bwd_kernel, group_size),
        out_shape=shape,
        grid_spec=pltpu.PrefetchScalarGridSpec(
            num_scalar_prefetch=1,
            grid=(count, groups),
            in_specs=in_specs,
            out_specs=pl.BlockSpec((2, 1, half, block), lambda b, g, tp: (0, b + start, 0, g)),
        ),
        input_output_aliases=aliases,
        compiler_params=pltpu.CompilerParams(vmem_limit_bytes=48 * 2**20),
        cost_estimate=cost(work * HEAD_DIM * 30, work * 3, ga_rec, ga_rec, ga_rec, ga_rec),
        name="attention_bwd",
    )(*args)


def split_norm_kernel(core_ref, gain_ref, source_ref, *rest):
    mine_ref, sent_ref = rest[-2:]
    first = core_ref[0] == 0
    values = source_ref[0].astype(F32)
    inv_rms = lax.rsqrt(jnp.mean(values * values, axis=-1, keepdims=True) + NORM_EPS)
    normed = values * inv_rms * gain_ref[...]
    rows = normed.shape[1] // 8
    for i in range(4):
        even = normed[:, 2 * i * rows:(2 * i + 1) * rows]
        odd = normed[:, (2 * i + 1) * rows:(2 * i + 2) * rows]
        mine_ref[0, 0, :, i * rows:(i + 1) * rows] = jnp.where(first, even, odd).astype(BF16)
        sent_ref[0, 0, :, i * rows:(i + 1) * rows] = jnp.where(first, odd, even).astype(BF16)


def split_norm(core_index, gain, source, kind, start, batch, held, row_block=128):
    count, half, width = source.shape
    row_block = min(row_block, half)
    out = jax.ShapeDtypeStruct((2, batch, half, width // 2), BF16)
    out_spec = pl.BlockSpec((1, 1, row_block, width // 2), lambda b, r, c: (kind, b + start, r, 0))
    in_specs = [pl.BlockSpec((1, width), lambda b, r, c: (0, 0)), pl.BlockSpec((1, row_block, width), lambda b, r, c: (b, r, 0))]
    args = [core_index, gain.reshape(1, width), source]
    aliases = {}
    if held is not None:
        in_specs += [pl.BlockSpec(memory_space=pl.ANY)] * 2
        aliases = {len(args): 0, len(args) + 1: 1}
        args += list(held)
    return pl.pallas_call(
        split_norm_kernel,
        out_shape=(out, out),
        grid_spec=pltpu.PrefetchScalarGridSpec(
            num_scalar_prefetch=1, grid=(count, half // row_block), in_specs=in_specs, out_specs=(out_spec, out_spec)
        ),
        input_output_aliases=aliases,
        compiler_params=pltpu.CompilerParams(vmem_limit_bytes=32 * 2**20),
        cost_estimate=cost(count * half * width * 400, 0, source, source),
        name="split_norm",
    )(*args)


def gain_sum_kernel(tp_size, dp_size, part_ref, out_ref, slots, send_sem, recv_sem):
    total = tp_size * dp_size
    me_dp = lax.axis_index("dp")
    me = lax.axis_index("tp") * dp_size + me_dp

    def place(index):
        return (index // dp_size, lax.rem(index, dp_size))

    barrier = pltpu.get_barrier_semaphore()
    for offset in range(1, total):
        pl.semaphore_signal(barrier, inc=1, device_id=place(lax.rem(me + offset, total)), device_id_type=pl.DeviceIdType.MESH)
    pl.semaphore_wait(barrier, total - 1)

    def copy(offset, slot, target):
        return pltpu.make_async_remote_copy(
            src_ref=part_ref.at[place(target)[1]],
            dst_ref=slots.at[slot],
            send_sem=send_sem.at[offset],
            recv_sem=recv_sem.at[slot],
            device_id=place(target),
            device_id_type=pl.DeviceIdType.MESH,
        )

    for offset in range(1, total):
        copy(offset, me, lax.rem(me + offset, total)).start()
    slots[me] = part_ref[me_dp]
    for offset in range(1, total):
        copy(offset, me, lax.rem(me + offset, total)).wait_send()
        copy(offset, lax.rem(me + total - offset, total), me).wait_recv()
    result = slots[0]
    for i in range(1, total):
        result = result + slots[i]
    for i in range(out_ref.shape[1] // HEAD_DIM):
        out_ref[:, i * HEAD_DIM:(i + 1) * HEAD_DIM] = result[i:i + 1]


def gain_sum(part, tp_size, dp_size):
    rows = part.shape[0] // dp_size
    tile = 8 * HEAD_DIM
    padded = jnp.pad(part.reshape(dp_size, rows), ((0, 0), (0, -rows % tile))).reshape(dp_size, -1, HEAD_DIM)
    sublanes = padded.shape[1]
    total = tp_size * dp_size
    result = pl.pallas_call(
        functools.partial(gain_sum_kernel, tp_size, dp_size),
        out_shape=jax.ShapeDtypeStruct((1, rows), F32),
        in_specs=[pl.BlockSpec(memory_space=pltpu.VMEM)],
        out_specs=pl.BlockSpec(memory_space=pltpu.VMEM),
        scratch_shapes=[
            pltpu.VMEM((total, sublanes, HEAD_DIM), F32),
            pltpu.SemaphoreType.DMA((total,)),
            pltpu.SemaphoreType.DMA((total,)),
        ],
        compiler_params=pltpu.CompilerParams(collective_id=0, has_side_effects=True),
        name="gain_sum",
    )(padded)
    return result.reshape(rows)


def finish_out_kernel(x_ref, near_ref, far_ref, *rest):
    out_sum = (near_ref[0].astype(F32) + far_ref[0].astype(F32)).astype(BF16).astype(F32)
    rest[-1][0] = (x_ref[0].astype(F32) + out_sum).astype(BF16)


def finish_grad_kernel(x_ref, dy_ref, near_ref, gain_ref, far_ref, *rest):
    out_ref, gain_out_ref = rest[-2:]
    values = x_ref[0].astype(F32)
    inv_rms = lax.rsqrt(jnp.mean(values * values, axis=-1, keepdims=True) + NORM_EPS)
    x_hat = values * inv_rms
    grad_normed = (near_ref[0].astype(F32) + far_ref[0].astype(F32)).astype(BF16).astype(F32)
    scaled = grad_normed * gain_ref[...]
    mean = jnp.mean(scaled * x_hat, axis=-1, keepdims=True)
    out_ref[0] = (dy_ref[0].astype(F32) + inv_rms * (scaled - x_hat * mean)).astype(BF16)

    @pl.when((pl.program_id(0) == 0) & (pl.program_id(1) == 0))
    def _():
        gain_out_ref[...] = jnp.zeros_like(gain_out_ref)

    gain_out_ref[...] += jnp.sum((grad_normed * x_hat).reshape(-1, 8, x_hat.shape[-1]), axis=0)


def finish(kernel, full, chunk, start, held, gain=None, row_block=64):
    batch, half, width = full[0].shape
    count = chunk[0].shape[0]
    row_block = min(row_block, half)
    spec = lambda offset: pl.BlockSpec((1, row_block, width), lambda b, r: (b + offset, r, 0))
    in_specs = [spec(start)] * len(full)
    args = list(full)
    out_shape = [jax.ShapeDtypeStruct((batch, half, width), BF16)]
    out_specs = [spec(start)]
    if gain is not None:
        in_specs.append(pl.BlockSpec((1, width), lambda b, r: (0, 0)))
        args.append(gain.reshape(1, width))
        out_shape.append(jax.ShapeDtypeStruct((8, width), F32))
        out_specs.append(pl.BlockSpec((8, width), lambda b, r: (0, 0)))
    in_specs += [spec(0)] * len(chunk)
    args += list(chunk)
    aliases = {}
    if held is not None:
        aliases = {len(args): 0}
        in_specs.append(pl.BlockSpec(memory_space=pl.ANY))
        args.append(held)
    result = pl.pallas_call(
        kernel,
        out_shape=out_shape,
        grid=(count, half // row_block),
        in_specs=in_specs,
        out_specs=out_specs,
        input_output_aliases=aliases,
        compiler_params=pltpu.CompilerParams(vmem_limit_bytes=32 * 2**20),
        cost_estimate=cost(count * half * width * 400, 0, *([chunk[0]] * (len(full) + len(chunk) + 1))),
    )(*args)
    return result if gain is not None else result[0]


def regroup_kernel(q_ref, k_ref, v_ref, out_ref):
    split = q_ref.shape[1]
    out_ref[:, :split] = q_ref[...]
    out_ref[:, split:split + HEAD_DIM] = k_ref[...]
    out_ref[:, split + HEAD_DIM:] = v_ref[...]


def regroup(w_query, w_key, w_value):
    rows = w_query.shape[0]
    groups = w_key.shape[1] // HEAD_DIM
    split = w_query.shape[1] // groups
    spec = lambda columns: pl.BlockSpec((rows, columns), lambda g: (0, g))
    out = jax.ShapeDtypeStruct((rows, groups * (split + 2 * HEAD_DIM)), w_query.dtype)
    return pl.pallas_call(
        regroup_kernel,
        out_shape=out,
        grid=(groups,),
        in_specs=[spec(split), spec(HEAD_DIM), spec(HEAD_DIM)],
        out_specs=spec(split + 2 * HEAD_DIM),
        cost_estimate=cost(rows * out.shape[1] * 400, 0, out, out),
        name="regroup",
    )(w_query, w_key, w_value)


def ungroup_kernel(count, *refs):
    q_ref, k_ref, v_ref = refs[-3:]
    split = q_ref.shape[1]
    for group in range(count):

        @pl.when(pl.program_id(1) == group)
        def _(group=group):
            block = refs[2 * group][...] + refs[2 * group + 1][...]
            q_ref[...] = block[:, :split]
            k_ref[...] = block[:, split:split + HEAD_DIM]
            v_ref[...] = block[:, split + HEAD_DIM:]


def ungroup(terms, start, groups, held, row_block=192):
    rows, block = terms[0][0].shape
    split = block - 2 * HEAD_DIM
    row_block = min(row_block, rows)
    spec = lambda columns: pl.BlockSpec((row_block, columns), lambda r, g: (r, g + start))
    shape = lambda columns: jax.ShapeDtypeStruct((rows, groups * columns), F32)
    args = [term for pair in terms for term in pair]
    in_specs = [pl.BlockSpec((row_block, block), lambda r, g: (r, 0))] * len(args)
    estimate = cost(rows * block * len(terms) * 400, 0, *args, *args[:len(terms)])
    aliases = {}
    if held is not None:
        in_specs += [pl.BlockSpec(memory_space=pl.ANY)] * 3
        aliases = {len(args) + i: i for i in range(3)}
        args += list(held)
    return pl.pallas_call(
        functools.partial(ungroup_kernel, len(terms)),
        out_shape=(shape(split), shape(HEAD_DIM), shape(HEAD_DIM)),
        grid=(rows // row_block, len(terms)),
        in_specs=in_specs,
        out_specs=(spec(split), spec(HEAD_DIM), spec(HEAD_DIM)),
        input_output_aliases=aliases,
        compiler_params=pltpu.CompilerParams(vmem_limit_bytes=32 * 2**20),
        cost_estimate=estimate,
        name="ungroup",
    )(*args)


CHUNKS = 2


def after(value, *others):
    return lax.optimization_barrier((value, *others))[0]


def solution(mesh):
    swap = [(0, 1), (1, 0)]

    def exchange(values):
        return lax.ppermute(values, "tp", swap)

    def mm(eq, a, b):
        return jnp.einsum(eq, a, b, preferred_element_type=F32)

    def local_block(hidden, norm_gain, w_query, w_key, w_value, w_out, grad_out):
        batch, half, _ = hidden.shape
        rows_loc = w_query.shape[0]
        groups = w_key.shape[1] // HEAD_DIM
        group_size = w_query.shape[1] // w_key.shape[1]
        block = (group_size + 2) * HEAD_DIM
        tp_index = lax.axis_index("tp").astype(jnp.int32).reshape(1)
        tables = rope_tables(2 * half)

        step = batch // CHUNKS
        hidden_rec, grad_rec = [], []
        source = hidden
        for start, count in [(0, 1), (1, 1), (2, 2)]:
            piece = lax.optimization_barrier(source[start:start + count])
            source = after(hidden, piece)
            hidden_rec.append(exchange(piece))
        hidden_rec = [jnp.concatenate(hidden_rec[:2], axis=0), hidden_rec[2]]
        pieces = [(0, 2), (2, 1), (3, 1)]
        for start, count in pieces:
            grad_rec.append(exchange(grad_out[start:start + count]))

        w_qkv = regroup(w_query, w_key, w_value)
        w_qkv = lax.all_gather(w_qkv, "dp", axis=0, tiled=True)
        w_o = lax.all_gather(w_out, "dp", axis=1, tiled=True)
        gain = lax.all_gather(norm_gain, "dp", axis=0, tiled=True).astype(F32)

        def norm(values):
            values = values.astype(F32)
            inv_rms = lax.rsqrt(jnp.mean(values * values, axis=-1, keepdims=True) + NORM_EPS)
            return (values * inv_rms * gain).astype(BF16)

        place = lax.axis_index("dp").astype(jnp.uint32)
        core, along_x, along_y = place & 1, (place >> 1) & 1, place >> 2
        core_index = core.astype(jnp.int32).reshape(1)
        split = split_norm(core_index, gain, hidden, 0, 0, batch, None)
        for i in range(CHUNKS):
            split = split_norm(core_index, gain, hidden_rec[i], 1, i * step, batch, split)
        normed_mine, normed_sent = split

        normed_own = norm(hidden)
        qkv_own = mm("bsd,de->bse", normed_own, w_qkv).astype(BF16)
        qkv_rec = []
        attn = None
        before = qkv_own
        for i in range(CHUNKS):
            rec = norm(after(hidden_rec[i], before))
            qkv_rec.append(mm("bsd,de->bse", rec, w_qkv).astype(BF16))
            attn = attention_fwd(tp_index, qkv_own, qkv_rec[i], tables, i * step, attn, groups, group_size)
            before = attn[0]
        attn_own, attn_rec = attn

        out_send = []
        for i in range(CHUNKS):
            out_send.append(lax.optimization_barrier(mm("bse,ed->bsd", attn_rec[i * step:(i + 1) * step], w_o).astype(BF16)))

        ga_own = mm("bsd,ed->bse", after(grad_out, *out_send), w_o).astype(BF16)
        gqkv = None
        before = ga_own
        for i, (start, count) in enumerate(pieces):
            if i == len(pieces) - 1:
                grad_wo = mm("bse,bsd->ed", attn_own, after(grad_out, gqkv)) + mm("bse,bsd->ed", attn_rec, jnp.concatenate(grad_rec, axis=0))
                before = grad_wo
            ga_rec = mm("bsd,ed->bse", after(grad_rec[i], before), w_o).astype(BF16)
            gqkv = attention_bwd(tp_index, qkv_own, qkv_rec[start // step], tables, ga_own, ga_rec, start, start % step, gqkv, groups, group_size)
            before = gqkv
        grad_wo = lax.psum_scatter(grad_wo, "dp", scatter_dimension=1, tiled=True)

        cut = groups // 2 * block

        def pick(values, axis, coordinate, columns=0):
            at = [jnp.uint32(0)] * values.ndim
            at[axis], at[-1] = coordinate, jnp.uint32(columns)
            size = [*values.shape[:-1], block]
            size[axis] = 1
            return lax.squeeze(lax.dynamic_slice(values, at, size), [axis])

        def pass_on(values, bit):
            return lax.ppermute(values, "dp", [(i, i ^ bit) for i in range(8)])

        def weight_grad(normed, columns, before):
            return mm("hbsd,hbse->de", normed, after(gqkv, *before)[..., columns])

        late, early = slice(cut, 2 * cut), slice(0, cut)
        late_sent = weight_grad(normed_sent, late, [])
        late_far = pass_on(late_sent, 1)
        early_sent = weight_grad(normed_sent, early, [late_sent])
        early_far = pass_on(early_sent, 1)

        def first_stage(mine, far):
            total = (mine + far).reshape(2, 2, rows_loc, cut)
            sent = pick(total, 1, along_x ^ 1), pick(total, 0, along_y ^ 1, block)
            sent, total = lax.optimization_barrier((sent, total))
            mine = pick(total, 1, along_x), pick(total, 0, along_y, block)
            return sent, mine, (pass_on(sent[0], 2), pass_on(sent[1], 4))

        def second_stage(mine, far, before):
            far = after(far, *before)
            total = mine[0] + far[0], mine[1] + far[1]
            sent = pick(total[0], 0, along_y ^ 1), pick(total[1], 0, along_x ^ 1)
            sent, total = lax.optimization_barrier((sent, total))
            mine = pick(total[0], 0, along_y), pick(total[1], 0, along_x)
            return sent, [(mine[0], pass_on(sent[0], 4)), (mine[1], pass_on(sent[1], 2))]

        gqkv_rec = after(gqkv, early_sent)[1]
        dn_send = []
        for i in range(CHUNKS):
            dn_send.append(lax.optimization_barrier(mm("bse,de->bsd", gqkv_rec[i * step:(i + 1) * step], w_qkv).astype(BF16)))

        out_far, dn_far = [], []
        for i in range(CHUNKS):
            out_far.append(exchange(out_send[i]))
        dn_sent = [dn_send[0], dn_send[1][:1], dn_send[1][1:]]
        for i in range(3):
            dn_far.append(exchange(dn_sent[i]))

        late_sent, late_mine, late_far = first_stage(weight_grad(normed_mine, late, dn_send), late_far)
        early_sent, early_mine, early_far = first_stage(weight_grad(normed_mine, early, late_sent), early_far)

        attn_own, gqkv = after((attn_own, gqkv), *early_sent)
        out_near = lax.optimization_barrier(mm("bse,ed->bsd", attn_own, w_o).astype(BF16))
        dn_near = lax.optimization_barrier(mm("bse,de->bsd", gqkv[0], w_qkv).astype(BF16))
        late_sent, late_terms = second_stage(late_mine, late_far, [out_near, dn_near])
        hidden_out = None
        for i in range(CHUNKS):
            hidden_out = finish(finish_out_kernel, [hidden, after(out_near, *late_sent)], [out_far[i]], i * step, hidden_out)
        gain_parts = []

        def finish_piece(index, dn_near, grad_hidden):
            grad_hidden, part = finish(
                finish_grad_kernel, [hidden, grad_out, dn_near], [dn_far[index]], pieces[index][0], grad_hidden, gain
            )
            gain_parts.append(part)
            return grad_hidden

        dn_near = after(dn_near, hidden_out)
        grad_hidden = finish_piece(0, dn_near, None)
        early_sent, early_terms = second_stage(early_mine, early_far, [grad_hidden])
        dn_near = after(dn_near, *early_sent)
        grad_hidden = finish_piece(1, dn_near, grad_hidden)
        w_grads = ungroup([(mine, after(far, grad_hidden)) for mine, far in late_terms], groups // 2, groups, None)
        w_grads = ungroup([(mine, after(far, *w_grads)) for mine, far in early_terms], 0, groups, w_grads)
        grad_wq, grad_wk, grad_wv = w_grads
        grad_hidden = finish_piece(2, after(dn_near, *w_grads), grad_hidden)
        grad_gain = gain_sum(jnp.sum(sum(gain_parts), axis=0), mesh.shape["tp"], mesh.shape["dp"])
        return hidden_out, grad_hidden, grad_gain, grad_wq, grad_wk, grad_wv, grad_wo

    act_spec = P("dp", "tp", None)
    col_spec = P("dp", "tp")
    row_spec = P("tp", "dp")
    return jax.shard_map(
        local_block,
        mesh=mesh,
        in_specs=(act_spec, P("dp"), col_spec, col_spec, col_spec, row_spec, act_spec),
        out_specs=(act_spec, act_spec, P("dp"), col_spec, col_spec, col_spec, row_spec),
        check_vma=False,
    )
```

```python
import functools

import jax
import jax.numpy as jnp
from jax import lax
from jax.experimental import pallas as pl
from jax.experimental.pallas import tpu as pltpu
from jax.sharding import PartitionSpec as P


HEAD_DIM = 128
NORM_EPS = 1e-5
ROPE_BASE = 500000.0
SCORE_SCALE = HEAD_DIM ** -0.5
MASK_VALUE = -1e30
F32 = jnp.float32
BF16 = jnp.bfloat16
NT = (((1,), (1,)), ((), ()))
NN = (((1,), (0,)), ((), ()))
TN = (((0,), (0,)), ((), ()))


def rope_tables(seq_len):
    half_dim = HEAD_DIM // 2
    inv_freq = ROPE_BASE ** (-jnp.arange(half_dim, dtype=F32) * 2.0 / HEAD_DIM)
    angles = jnp.arange(seq_len, dtype=F32)[:, None] * inv_freq[None, :]
    cos_t, sin_t = jnp.cos(angles), jnp.sin(angles)
    return jnp.concatenate([cos_t, cos_t], axis=1), jnp.concatenate([-sin_t, sin_t], axis=1)


def dot(lhs, rhs, dims):
    return lax.dot_general(lhs, rhs, dims, preferred_element_type=F32)


def turn(values, cos_t, sin_t):
    return values * cos_t + pltpu.roll(values, HEAD_DIM // 2, 1) * sin_t


def pick_halves(first, own, rec):
    own, rec = own.astype(F32), rec.astype(F32)
    return jnp.where(first, own, rec), jnp.where(first, rec, own)


def heads_of(group_size, block, cos_t, sin_t):
    cut = [block[:, i * HEAD_DIM:(i + 1) * HEAD_DIM] for i in range(group_size + 2)]
    queries = jnp.concatenate([turn(cut[i], cos_t, sin_t).astype(BF16) for i in range(group_size)], axis=0)
    return queries, turn(cut[group_size], cos_t, sin_t).astype(BF16), cut[group_size + 1].astype(BF16)


def store_halves(first, own_ref, rec_ref, columns, lower, upper):
    own_ref[0, :, columns] = jnp.where(first, lower, upper).astype(own_ref.dtype)
    rec_ref[0, :, columns] = jnp.where(first, upper, lower).astype(rec_ref.dtype)


def attention_fwd_kernel(group_size, tp_ref, own_ref, rec_ref, cos_ref, sin_ref, *rest):
    out_own_ref, out_rec_ref = rest[-2:]
    half = own_ref.shape[1]
    first = tp_ref[0] == 0
    lower, upper = pick_halves(first, own_ref[0], rec_ref[0])
    q_lo, k_lo, v_lo = heads_of(group_size, lower, cos_ref[:half], sin_ref[:half])
    q_up, k_up, v_up = heads_of(group_size, upper, cos_ref[half:], sin_ref[half:])
    rows = lax.broadcasted_iota(jnp.int32, (group_size, half, half), 1).reshape(group_size * half, half)
    cols = lax.broadcasted_iota(jnp.int32, (group_size * half, half), 1)
    causal = rows >= cols

    s_lo = jnp.where(causal, dot(q_lo, k_lo, NT), MASK_VALUE)
    p_lo = jnp.exp((s_lo - jnp.max(s_lo, axis=1, keepdims=True)) * SCORE_SCALE)
    p_lo = (p_lo * (1.0 / jnp.sum(p_lo, axis=1, keepdims=True))).astype(BF16)
    a_lo = dot(p_lo, v_lo, NN)

    s_a = dot(q_up, k_lo, NT)
    s_b = jnp.where(causal, dot(q_up, k_up, NT), MASK_VALUE)
    top = jnp.maximum(jnp.max(s_a, axis=1, keepdims=True), jnp.max(s_b, axis=1, keepdims=True))
    p_a = jnp.exp((s_a - top) * SCORE_SCALE)
    p_b = jnp.exp((s_b - top) * SCORE_SCALE)
    inv = 1.0 / (jnp.sum(p_a, axis=1, keepdims=True) + jnp.sum(p_b, axis=1, keepdims=True))
    a_up = dot((p_a * inv).astype(BF16), v_lo, NN) + dot((p_b * inv).astype(BF16), v_up, NN)
    for i in range(group_size):
        part = slice(i * half, (i + 1) * half)
        store_halves(first, out_own_ref, out_rec_ref, slice(i * HEAD_DIM, (i + 1) * HEAD_DIM), a_lo[part], a_up[part])


def attention_bwd_kernel(group_size, tp_ref, own_ref, rec_ref, cos_ref, sin_ref, ga_own_ref, ga_rec_ref, *rest):
    out_ref = rest[-1]
    half = own_ref.shape[1]
    first = tp_ref[0] == 0
    lower, upper = pick_halves(first, own_ref[0], rec_ref[0])
    cos_lo, sin_lo, cos_up, sin_up = cos_ref[:half], sin_ref[:half], cos_ref[half:], sin_ref[half:]
    q_lo, k_lo, v_lo = heads_of(group_size, lower, cos_lo, sin_lo)
    q_up, k_up, v_up = heads_of(group_size, upper, cos_up, sin_up)
    ga_lower, ga_upper = pick_halves(first, ga_own_ref[0], ga_rec_ref[0])

    def stacked(block):
        return jnp.concatenate([block[:, i * HEAD_DIM:(i + 1) * HEAD_DIM].astype(BF16) for i in range(group_size)], axis=0)

    ga_lo, ga_up = stacked(ga_lower), stacked(ga_upper)
    keys = lax.broadcasted_iota(jnp.int32, (half, half), 0)
    spots = lax.broadcasted_iota(jnp.int32, (half, half), 1)
    causal = jnp.concatenate([spots >= keys] * group_size, axis=1)

    s_lo = jnp.where(causal, dot(k_lo, q_lo, NT), MASK_VALUE)
    p_lo = jnp.exp((s_lo - jnp.max(s_lo, axis=0, keepdims=True)) * SCORE_SCALE)
    p_lo = p_lo * (1.0 / jnp.sum(p_lo, axis=0, keepdims=True))
    gp_lo = dot(v_lo, ga_lo, NT).astype(BF16).astype(F32)
    gs_lo = (p_lo * (gp_lo - jnp.sum(gp_lo * p_lo, axis=0, keepdims=True)) * SCORE_SCALE).astype(BF16)

    s_a = dot(k_lo, q_up, NT)
    s_b = jnp.where(causal, dot(k_up, q_up, NT), MASK_VALUE)
    top = jnp.maximum(jnp.max(s_a, axis=0, keepdims=True), jnp.max(s_b, axis=0, keepdims=True))
    p_a = jnp.exp((s_a - top) * SCORE_SCALE)
    p_b = jnp.exp((s_b - top) * SCORE_SCALE)
    inv = 1.0 / (jnp.sum(p_a, axis=0, keepdims=True) + jnp.sum(p_b, axis=0, keepdims=True))
    p_a = p_a * inv
    p_b = p_b * inv
    gp_a = dot(v_lo, ga_up, NT).astype(BF16).astype(F32)
    gp_b = dot(v_up, ga_up, NT).astype(BF16).astype(F32)
    mean_up = jnp.sum(gp_a * p_a, axis=0, keepdims=True) + jnp.sum(gp_b * p_b, axis=0, keepdims=True)
    gs_a = (p_a * (gp_a - mean_up) * SCORE_SCALE).astype(BF16)
    gs_b = (p_b * (gp_b - mean_up) * SCORE_SCALE).astype(BF16)

    gv_lo = dot(p_lo.astype(BF16), ga_lo, NN) + dot(p_a.astype(BF16), ga_up, NN)
    gv_up = dot(p_b.astype(BF16), ga_up, NN)
    gk_lo = (dot(gs_lo, q_lo, NN) + dot(gs_a, q_up, NN)).astype(BF16).astype(F32)
    gk_up = dot(gs_b, q_up, NN).astype(BF16).astype(F32)
    gq_lo = dot(gs_lo, k_lo, TN).astype(BF16).astype(F32)
    gq_up = (dot(gs_a, k_lo, TN) + dot(gs_b, k_up, TN)).astype(BF16).astype(F32)

    def store(index, lower_part, upper_part):
        store_halves(first, out_ref.at[0], out_ref.at[1], slice(index * HEAD_DIM, (index + 1) * HEAD_DIM), lower_part, upper_part)

    for i in range(group_size):
        part = slice(i * half, (i + 1) * half)
        store(i, turn(gq_lo[part], cos_lo, -sin_lo), turn(gq_up[part], cos_up, -sin_up))
    store(group_size, turn(gk_lo, cos_lo, -sin_lo), turn(gk_up, cos_up, -sin_up))
    store(group_size + 1, gv_lo, gv_up)


def cost(flops, transcendentals, *arrays):
    return pl.CostEstimate(flops=int(flops), transcendentals=int(transcendentals), bytes_accessed=int(sum(a.size * a.dtype.itemsize for a in arrays)))


def attention_fwd(tp_index, qkv_own, qkv_rec, tables, start, held, groups, group_size):
    batch, half, width = qkv_own.shape
    count = qkv_rec.shape[0]
    block = width // groups
    out_block = group_size * HEAD_DIM
    shape = jax.ShapeDtypeStruct((batch, half, groups * out_block), BF16)
    spec = lambda columns, offset: pl.BlockSpec((1, half, columns), lambda b, g, tp: (b + offset, 0, g))
    table = pl.BlockSpec((2 * half, HEAD_DIM), lambda b, g, tp: (0, 0))
    in_specs = [spec(block, start), spec(block, 0), table, table]
    args = [tp_index, qkv_own, qkv_rec, *tables]
    aliases = {}
    if held is not None:
        in_specs += [pl.BlockSpec(memory_space=pl.ANY)] * 2
        aliases = {len(args): 0, len(args) + 1: 1}
        args += list(held)
    work = count * groups * group_size * half * half
    return pl.pallas_call(
        functools.partial(attention_fwd_kernel, group_size),
        out_shape=(shape, shape),
        grid_spec=pltpu.PrefetchScalarGridSpec(
            num_scalar_prefetch=1,
            grid=(count, groups),
            in_specs=in_specs,
            out_specs=(spec(out_block, start), spec(out_block, start)),
        ),
        input_output_aliases=aliases,
        compiler_params=pltpu.CompilerParams(vmem_limit_bytes=48 * 2**20),
        cost_estimate=cost(work * HEAD_DIM * 12, work * 3, qkv_rec, qkv_rec),
        name="attention_fwd",
    )(*args)


def attention_bwd(tp_index, qkv_own, qkv_rec, tables, ga_own, ga_rec, start, rec_start, held, groups, group_size):
    batch, half, width = qkv_own.shape
    count = ga_rec.shape[0]
    block = width // groups
    ga_block = group_size * HEAD_DIM
    shape = jax.ShapeDtypeStruct((2, batch, half, width), BF16)
    spec = lambda columns, offset: pl.BlockSpec((1, half, columns), lambda b, g, tp: (b + offset, 0, g))
    table = pl.BlockSpec((2 * half, HEAD_DIM), lambda b, g, tp: (0, 0))
    in_specs = [spec(block, start), spec(block, rec_start), table, table, spec(ga_block, start), spec(ga_block, 0)]
    args = [tp_index, qkv_own, qkv_rec, *tables, ga_own, ga_rec]
    aliases = {}
    if held is not None:
        in_specs.append(pl.BlockSpec(memory_space=pl.ANY))
        aliases = {len(args): 0}
        args.append(held)
    work = count * groups * group_size * half * half
    return pl.pallas_call(
        functools.partial(attention_bwd_kernel, group_size),
        out_shape=shape,
        grid_spec=pltpu.PrefetchScalarGridSpec(
            num_scalar_prefetch=1,
            grid=(count, groups),
            in_specs=in_specs,
            out_specs=pl.BlockSpec((2, 1, half, block), lambda b, g, tp: (0, b + start, 0, g)),
        ),
        input_output_aliases=aliases,
        compiler_params=pltpu.CompilerParams(vmem_limit_bytes=48 * 2**20),
        cost_estimate=cost(work * HEAD_DIM * 30, work * 3, ga_rec, ga_rec, ga_rec, ga_rec),
        name="attention_bwd",
    )(*args)


def split_norm_kernel(core_ref, gain_ref, source_ref, *rest):
    mine_ref, sent_ref = rest[-2:]
    first = core_ref[0] == 0
    values = source_ref[0].astype(F32)
    inv_rms = lax.rsqrt(jnp.mean(values * values, axis=-1, keepdims=True) + NORM_EPS)
    normed = values * inv_rms * gain_ref[...]
    rows = normed.shape[1] // 8
    for i in range(4):
        even = normed[:, 2 * i * rows:(2 * i + 1) * rows]
        odd = normed[:, (2 * i + 1) * rows:(2 * i + 2) * rows]
        mine_ref[0, 0, :, i * rows:(i + 1) * rows] = jnp.where(first, even, odd).astype(BF16)
        sent_ref[0, 0, :, i * rows:(i + 1) * rows] = jnp.where(first, odd, even).astype(BF16)


def split_norm(core_index, gain, source, kind, start, batch, held, row_block=128):
    count, half, width = source.shape
    row_block = min(row_block, half)
    out = jax.ShapeDtypeStruct((2, batch, half, width // 2), BF16)
    out_spec = pl.BlockSpec((1, 1, row_block, width // 2), lambda b, r, c: (kind, b + start, r, 0))
    in_specs = [pl.BlockSpec((1, width), lambda b, r, c: (0, 0)), pl.BlockSpec((1, row_block, width), lambda b, r, c: (b, r, 0))]
    args = [core_index, gain.reshape(1, width), source]
    aliases = {}
    if held is not None:
        in_specs += [pl.BlockSpec(memory_space=pl.ANY)] * 2
        aliases = {len(args): 0, len(args) + 1: 1}
        args += list(held)
    return pl.pallas_call(
        split_norm_kernel,
        out_shape=(out, out),
        grid_spec=pltpu.PrefetchScalarGridSpec(
            num_scalar_prefetch=1, grid=(count, half // row_block), in_specs=in_specs, out_specs=(out_spec, out_spec)
        ),
        input_output_aliases=aliases,
        compiler_params=pltpu.CompilerParams(vmem_limit_bytes=32 * 2**20),
        cost_estimate=cost(count * half * width * 400, 0, source, source),
        name="split_norm",
    )(*args)


def gain_sum_kernel(tp_size, dp_size, part_ref, out_ref, slots, send_sem, recv_sem):
    total = tp_size * dp_size
    me_dp = lax.axis_index("dp")
    me = lax.axis_index("tp") * dp_size + me_dp

    def place(index):
        return (index // dp_size, lax.rem(index, dp_size))

    barrier = pltpu.get_barrier_semaphore()
    for offset in range(1, total):
        pl.semaphore_signal(barrier, inc=1, device_id=place(lax.rem(me + offset, total)), device_id_type=pl.DeviceIdType.MESH)
    pl.semaphore_wait(barrier, total - 1)

    def copy(offset, slot, target):
        return pltpu.make_async_remote_copy(
            src_ref=part_ref.at[place(target)[1]],
            dst_ref=slots.at[slot],
            send_sem=send_sem.at[offset],
            recv_sem=recv_sem.at[slot],
            device_id=place(target),
            device_id_type=pl.DeviceIdType.MESH,
        )

    for offset in range(1, total):
        copy(offset, me, lax.rem(me + offset, total)).start()
    slots[me] = part_ref[me_dp]
    for offset in range(1, total):
        copy(offset, me, lax.rem(me + offset, total)).wait_send()
        copy(offset, lax.rem(me + total - offset, total), me).wait_recv()
    result = slots[0]
    for i in range(1, total):
        result = result + slots[i]
    for i in range(out_ref.shape[1] // HEAD_DIM):
        out_ref[:, i * HEAD_DIM:(i + 1) * HEAD_DIM] = result[i:i + 1]


def gain_sum(part, tp_size, dp_size):
    rows = part.shape[0] // dp_size
    tile = 8 * HEAD_DIM
    padded = jnp.pad(part.reshape(dp_size, rows), ((0, 0), (0, -rows % tile))).reshape(dp_size, -1, HEAD_DIM)
    sublanes = padded.shape[1]
    total = tp_size * dp_size
    result = pl.pallas_call(
        functools.partial(gain_sum_kernel, tp_size, dp_size),
        out_shape=jax.ShapeDtypeStruct((1, rows), F32),
        in_specs=[pl.BlockSpec(memory_space=pltpu.VMEM)],
        out_specs=pl.BlockSpec(memory_space=pltpu.VMEM),
        scratch_shapes=[
            pltpu.VMEM((total, sublanes, HEAD_DIM), F32),
            pltpu.SemaphoreType.DMA((total,)),
            pltpu.SemaphoreType.DMA((total,)),
        ],
        compiler_params=pltpu.CompilerParams(collective_id=0, has_side_effects=True),
        name="gain_sum",
    )(padded)
    return result.reshape(rows)


def finish_out_kernel(x_ref, near_ref, far_ref, *rest):
    out_sum = (near_ref[0].astype(F32) + far_ref[0].astype(F32)).astype(BF16).astype(F32)
    rest[-1][0] = (x_ref[0].astype(F32) + out_sum).astype(BF16)


def finish_grad_kernel(x_ref, dy_ref, near_ref, gain_ref, far_ref, *rest):
    out_ref, gain_out_ref = rest[-2:]
    values = x_ref[0].astype(F32)
    inv_rms = lax.rsqrt(jnp.mean(values * values, axis=-1, keepdims=True) + NORM_EPS)
    x_hat = values * inv_rms
    grad_normed = (near_ref[0].astype(F32) + far_ref[0].astype(F32)).astype(BF16).astype(F32)
    scaled = grad_normed * gain_ref[...]
    mean = jnp.mean(scaled * x_hat, axis=-1, keepdims=True)
    out_ref[0] = (dy_ref[0].astype(F32) + inv_rms * (scaled - x_hat * mean)).astype(BF16)

    @pl.when((pl.program_id(0) == 0) & (pl.program_id(1) == 0))
    def _():
        gain_out_ref[...] = jnp.zeros_like(gain_out_ref)

    gain_out_ref[...] += jnp.sum((grad_normed * x_hat).reshape(-1, 8, x_hat.shape[-1]), axis=0)


def finish(kernel, full, chunk, start, held, gain=None, row_block=64):
    batch, half, width = full[0].shape
    count = chunk[0].shape[0]
    row_block = min(row_block, half)
    spec = lambda offset: pl.BlockSpec((1, row_block, width), lambda b, r: (b + offset, r, 0))
    in_specs = [spec(start)] * len(full)
    args = list(full)
    out_shape = [jax.ShapeDtypeStruct((batch, half, width), BF16)]
    out_specs = [spec(start)]
    if gain is not None:
        in_specs.append(pl.BlockSpec((1, width), lambda b, r: (0, 0)))
        args.append(gain.reshape(1, width))
        out_shape.append(jax.ShapeDtypeStruct((8, width), F32))
        out_specs.append(pl.BlockSpec((8, width), lambda b, r: (0, 0)))
    in_specs += [spec(0)] * len(chunk)
    args += list(chunk)
    aliases = {}
    if held is not None:
        aliases = {len(args): 0}
        in_specs.append(pl.BlockSpec(memory_space=pl.ANY))
        args.append(held)
    result = pl.pallas_call(
        kernel,
        out_shape=out_shape,
        grid=(count, half // row_block),
        in_specs=in_specs,
        out_specs=out_specs,
        input_output_aliases=aliases,
        compiler_params=pltpu.CompilerParams(vmem_limit_bytes=32 * 2**20),
        cost_estimate=cost(count * half * width * 400, 0, *([chunk[0]] * (len(full) + len(chunk) + 1))),
    )(*args)
    return result if gain is not None else result[0]


def regroup_kernel(q_ref, k_ref, v_ref, out_ref):
    split = q_ref.shape[1]
    out_ref[:, :split] = q_ref[...]
    out_ref[:, split:split + HEAD_DIM] = k_ref[...]
    out_ref[:, split + HEAD_DIM:] = v_ref[...]


def regroup(w_query, w_key, w_value):
    rows = w_query.shape[0]
    groups = w_key.shape[1] // HEAD_DIM
    split = w_query.shape[1] // groups
    spec = lambda columns: pl.BlockSpec((rows, columns), lambda g: (0, g))
    out = jax.ShapeDtypeStruct((rows, groups * (split + 2 * HEAD_DIM)), w_query.dtype)
    return pl.pallas_call(
        regroup_kernel,
        out_shape=out,
        grid=(groups,),
        in_specs=[spec(split), spec(HEAD_DIM), spec(HEAD_DIM)],
        out_specs=spec(split + 2 * HEAD_DIM),
        cost_estimate=cost(rows * out.shape[1] * 400, 0, out, out),
        name="regroup",
    )(w_query, w_key, w_value)


def ungroup_kernel(count, *refs):
    q_ref, k_ref, v_ref = refs[-3:]
    split = q_ref.shape[1]
    for group in range(count):

        @pl.when(pl.program_id(1) == group)
        def _(group=group):
            block = refs[2 * group][...] + refs[2 * group + 1][...]
            q_ref[...] = block[:, :split]
            k_ref[...] = block[:, split:split + HEAD_DIM]
            v_ref[...] = block[:, split + HEAD_DIM:]


def ungroup(terms, start, groups, held, row_block=192):
    rows, block = terms[0][0].shape
    split = block - 2 * HEAD_DIM
    row_block = min(row_block, rows)
    spec = lambda columns: pl.BlockSpec((row_block, columns), lambda r, g: (r, g + start))
    shape = lambda columns: jax.ShapeDtypeStruct((rows, groups * columns), F32)
    args = [term for pair in terms for term in pair]
    in_specs = [pl.BlockSpec((row_block, block), lambda r, g: (r, 0))] * len(args)
    estimate = cost(rows * block * len(terms) * 400, 0, *args, *args[:len(terms)])
    aliases = {}
    if held is not None:
        in_specs += [pl.BlockSpec(memory_space=pl.ANY)] * 3
        aliases = {len(args) + i: i for i in range(3)}
        args += list(held)
    return pl.pallas_call(
        functools.partial(ungroup_kernel, len(terms)),
        out_shape=(shape(split), shape(HEAD_DIM), shape(HEAD_DIM)),
        grid=(rows // row_block, len(terms)),
        in_specs=in_specs,
        out_specs=(spec(split), spec(HEAD_DIM), spec(HEAD_DIM)),
        input_output_aliases=aliases,
        compiler_params=pltpu.CompilerParams(vmem_limit_bytes=32 * 2**20),
        cost_estimate=estimate,
        name="ungroup",
    )(*args)


CHUNKS = 2


def after(value, *others):
    return lax.optimization_barrier((value, *others))[0]


def solution(mesh):
    swap = [(0, 1), (1, 0)]

    def exchange(values):
        return lax.ppermute(values, "tp", swap)

    def mm(eq, a, b):
        return jnp.einsum(eq, a, b, preferred_element_type=F32)

    def local_block(hidden, norm_gain, w_query, w_key, w_value, w_out, grad_out):
        batch, half, _ = hidden.shape
        rows_loc = w_query.shape[0]
        groups = w_key.shape[1] // HEAD_DIM
        group_size = w_query.shape[1] // w_key.shape[1]
        block = (group_size + 2) * HEAD_DIM
        tp_index = lax.axis_index("tp").astype(jnp.int32).reshape(1)
        tables = rope_tables(2 * half)

        step = batch // CHUNKS
        hidden_rec, grad_rec = [], []
        source = hidden
        for start, count in [(0, 1), (1, 1), (2, 2)]:
            piece = lax.optimization_barrier(source[start:start + count])
            source = after(hidden, piece)
            hidden_rec.append(exchange(piece))
        hidden_rec = [jnp.concatenate(hidden_rec[:2], axis=0), hidden_rec[2]]
        pieces = [(0, 2), (2, 1), (3, 1)]
        for start, count in pieces:
            grad_rec.append(exchange(grad_out[start:start + count]))

        w_qkv = regroup(w_query, w_key, w_value)
        w_qkv = lax.all_gather(w_qkv, "dp", axis=0, tiled=True)
        w_o = lax.all_gather(w_out, "dp", axis=1, tiled=True)
        gain = lax.all_gather(norm_gain, "dp", axis=0, tiled=True).astype(F32)

        def norm(values):
            values = values.astype(F32)
            inv_rms = lax.rsqrt(jnp.mean(values * values, axis=-1, keepdims=True) + NORM_EPS)
            return (values * inv_rms * gain).astype(BF16)

        place = lax.axis_index("dp").astype(jnp.uint32)
        core, along_x, along_y = place & 1, (place >> 1) & 1, place >> 2
        core_index = core.astype(jnp.int32).reshape(1)
        split = split_norm(core_index, gain, hidden, 0, 0, batch, None)
        for i in range(CHUNKS):
            split = split_norm(core_index, gain, hidden_rec[i], 1, i * step, batch, split)
        normed_mine, normed_sent = split

        normed_own = norm(hidden)
        qkv_own = mm("bsd,de->bse", normed_own, w_qkv).astype(BF16)
        qkv_rec = []
        attn = None
        before = qkv_own
        for i in range(CHUNKS):
            rec = norm(after(hidden_rec[i], before))
            qkv_rec.append(mm("bsd,de->bse", rec, w_qkv).astype(BF16))
            attn = attention_fwd(tp_index, qkv_own, qkv_rec[i], tables, i * step, attn, groups, group_size)
            before = attn[0]
        attn_own, attn_rec = attn

        out_send = []
        for i in range(CHUNKS):
            out_send.append(lax.optimization_barrier(mm("bse,ed->bsd", attn_rec[i * step:(i + 1) * step], w_o).astype(BF16)))

        ga_own = mm("bsd,ed->bse", after(grad_out, *out_send), w_o).astype(BF16)
        gqkv = None
        before = ga_own
        for i, (start, count) in enumerate(pieces):
            if i == len(pieces) - 1:
                grad_wo = mm("bse,bsd->ed", attn_own, after(grad_out, gqkv)) + mm("bse,bsd->ed", attn_rec, jnp.concatenate(grad_rec, axis=0))
                before = grad_wo
            ga_rec = mm("bsd,ed->bse", after(grad_rec[i], before), w_o).astype(BF16)
            gqkv = attention_bwd(tp_index, qkv_own, qkv_rec[start // step], tables, ga_own, ga_rec, start, start % step, gqkv, groups, group_size)
            before = gqkv
        grad_wo = lax.psum_scatter(grad_wo, "dp", scatter_dimension=1, tiled=True)

        cut = groups // 2 * block

        def pick(values, axis, coordinate, columns=0):
            at = [jnp.uint32(0)] * values.ndim
            at[axis], at[-1] = coordinate, jnp.uint32(columns)
            size = [*values.shape[:-1], block]
            size[axis] = 1
            return lax.squeeze(lax.dynamic_slice(values, at, size), [axis])

        def pass_on(values, bit):
            return lax.ppermute(values, "dp", [(i, i ^ bit) for i in range(8)])

        def weight_grad(normed, columns, before):
            return mm("hbsd,hbse->de", normed, after(gqkv, *before)[..., columns])

        late, early = slice(cut, 2 * cut), slice(0, cut)
        late_sent = weight_grad(normed_sent, late, [])
        late_far = pass_on(late_sent, 1)
        early_sent = weight_grad(normed_sent, early, [late_sent])
        early_far = pass_on(early_sent, 1)

        def first_stage(mine, far):
            total = (mine + far).reshape(2, 2, rows_loc, cut)
            sent = pick(total, 1, along_x ^ 1), pick(total, 0, along_y ^ 1, block)
            sent, total = lax.optimization_barrier((sent, total))
            mine = pick(total, 1, along_x), pick(total, 0, along_y, block)
            return sent, mine, (pass_on(sent[0], 2), pass_on(sent[1], 4))

        def second_stage(mine, far, before):
            far = after(far, *before)
            total = mine[0] + far[0], mine[1] + far[1]
            sent = pick(total[0], 0, along_y ^ 1), pick(total[1], 0, along_x ^ 1)
            sent, total = lax.optimization_barrier((sent, total))
            mine = pick(total[0], 0, along_y), pick(total[1], 0, along_x)
            return sent, [(mine[0], pass_on(sent[0], 4)), (mine[1], pass_on(sent[1], 2))]

        late_sent, late_mine, late_far = first_stage(weight_grad(normed_mine, late, [early_sent]), late_far)
        gqkv_rec = after(gqkv, *late_sent)[1]
        dn_send = []
        for i in range(CHUNKS):
            dn_send.append(lax.optimization_barrier(mm("bse,de->bsd", gqkv_rec[i * step:(i + 1) * step], w_qkv).astype(BF16)))

        out_far, dn_far = [], []
        for i in range(CHUNKS):
            out_far.append(exchange(out_send[i]))
        dn_sent = [dn_send[0], dn_send[1][:1], dn_send[1][1:]]
        for i in range(3):
            dn_far.append(exchange(dn_sent[i]))

        early_sent, early_mine, early_far = first_stage(weight_grad(normed_mine, early, dn_send), early_far)

        attn_own, gqkv = after((attn_own, gqkv), *early_sent)
        out_near = lax.optimization_barrier(mm("bse,ed->bsd", attn_own, w_o).astype(BF16))
        dn_near = lax.optimization_barrier(mm("bse,de->bsd", gqkv[0], w_qkv).astype(BF16))
        late_sent, late_terms = second_stage(late_mine, late_far, [out_near, dn_near])
        hidden_out = None
        for i in range(CHUNKS):
            hidden_out = finish(finish_out_kernel, [hidden, after(out_near, *late_sent)], [out_far[i]], i * step, hidden_out)
        gain_parts = []

        def finish_piece(index, dn_near, grad_hidden):
            grad_hidden, part = finish(
                finish_grad_kernel, [hidden, grad_out, dn_near], [dn_far[index]], pieces[index][0], grad_hidden, gain
            )
            gain_parts.append(part)
            return grad_hidden

        dn_near = after(dn_near, hidden_out)
        grad_hidden = finish_piece(0, dn_near, None)
        early_sent, early_terms = second_stage(early_mine, early_far, [grad_hidden])
        dn_near = after(dn_near, *early_sent)
        grad_hidden = finish_piece(1, dn_near, grad_hidden)
        w_grads = ungroup([(mine, after(far, grad_hidden)) for mine, far in late_terms], groups // 2, groups, None)
        w_grads = ungroup([(mine, after(far, *w_grads)) for mine, far in early_terms], 0, groups, w_grads)
        grad_wq, grad_wk, grad_wv = w_grads
        grad_hidden = finish_piece(2, after(dn_near, *w_grads), grad_hidden)
        grad_gain = gain_sum(jnp.sum(sum(gain_parts), axis=0), mesh.shape["tp"], mesh.shape["dp"])
        return hidden_out, grad_hidden, grad_gain, grad_wq, grad_wk, grad_wv, grad_wo

    act_spec = P("dp", "tp", None)
    col_spec = P("dp", "tp")
    row_spec = P("tp", "dp")
    return jax.shard_map(
        local_block,
        mesh=mesh,
        in_specs=(act_spec, P("dp"), col_spec, col_spec, col_spec, row_spec, act_spec),
        out_specs=(act_spec, act_spec, P("dp"), col_spec, col_spec, col_spec, row_spec),
        check_vma=False,
    )
```
